8 devices in a mesh: dp: 1 (over z), yz: 2 (over y), x: 4 (over x, core).
Axes of the slice: x: 2, y: 2, z: 1, core: 2. Of those that a mesh axis runs over, the one named last changes fastest.
Arguments:
- x_in: bfloat16 [128, 6144], P('dp', ('x', 'yz'))
- ln_gain: bfloat16 [6144], P(('x', 'yz'))
- w_qkv: bfloat16 [6144, 6400], P('x', 'yz')
- w_gate: bfloat16 [6144, 24576], P('x', 'yz')
- w_up: bfloat16 [6144, 24576], P('x', 'yz')
- w_attn_out: bfloat16 [6144, 6144], P('yz', 'x')
- w_mlp_out: bfloat16 [24576, 6144], P('yz', 'x')
- k_cache: bfloat16 [128, 4096, 128], P(('dp', 'x', 'yz'))
- v_cache: bfloat16 [128, 4096, 128], P(('dp', 'x', 'yz'))
- ctx_len: int32 [128], P(('dp', 'x', 'yz'))
Outputs:
- output 1: bfloat16 [128, 6144], P('dp', ('x', 'yz'))
- output 2: bfloat16 [128, 4096, 128], P(('dp', 'x', 'yz'))
- output 3: bfloat16 [128, 4096, 128], P(('dp', 'x', 'yz'))
All inputs are finite; a program needn't handle non-finite values.
Results may differ from the reference program's by a relative error of at most 0.00713931.
Values are sent between devices in bfloat16 or wider.
A program may use at most 1 GiB of HBM per device.

```python
import jax
import jax.numpy as jnp
from jax import lax

BATCH_SIZE = 128
D_MODEL = 6144
NUM_HEADS = 48
HEAD_DIM = 128
FF_DIM = 24576
CACHE_LEN = 4096


def setup_inputs(seed: int = 0, part: int = 0) -> dict:
    part_key = jax.random.fold_in(jax.random.key(seed), part)
    shared_key = jax.random.key(seed + 1)
    x_key, kc_key, vc_key, vm_key, len_key = jax.random.split(part_key, 5)
    g_key, qkv_key, gate_key, up_key, ao_key, mo_key = jax.random.split(shared_key, 6)
    qkv_cols = (NUM_HEADS + 2) * HEAD_DIM
    attn_cols = NUM_HEADS * HEAD_DIM
    x_in = jax.random.normal(x_key, (BATCH_SIZE, D_MODEL), jnp.float32)
    ln_gain = jax.random.uniform(g_key, (D_MODEL,), jnp.float32, 0.5, 1.5)
    w_qkv = jax.random.normal(qkv_key, (D_MODEL, qkv_cols), jnp.float32) * D_MODEL ** -0.5
    w_gate = jax.random.normal(gate_key, (D_MODEL, FF_DIM), jnp.float32) * D_MODEL ** -0.5
    w_up = jax.random.normal(up_key, (D_MODEL, FF_DIM), jnp.float32) * D_MODEL ** -0.5
    w_attn_out = jax.random.normal(ao_key, (attn_cols, D_MODEL), jnp.float32) * attn_cols ** -0.5
    w_mlp_out = jax.random.normal(mo_key, (FF_DIM, D_MODEL), jnp.float32) * FF_DIM ** -0.5
    k_cache = jax.random.normal(kc_key, (BATCH_SIZE, CACHE_LEN, HEAD_DIM), jnp.float32)
    v_mean = jax.random.normal(vm_key, (BATCH_SIZE, 1, HEAD_DIM), jnp.float32)
    v_cache = v_mean + 0.7 * jax.random.normal(vc_key, (BATCH_SIZE, CACHE_LEN, HEAD_DIM), jnp.float32)
    ctx_len = jax.random.randint(len_key, (BATCH_SIZE,), CACHE_LEN // 8, CACHE_LEN, jnp.int32)
    ctx_len = ctx_len.at[0].set(CACHE_LEN - 1).at[1].set(CACHE_LEN // 8)
    return {
        "x_in": x_in.astype(jnp.bfloat16),
        "ln_gain": ln_gain.astype(jnp.bfloat16),
        "w_qkv": w_qkv.astype(jnp.bfloat16),
        "w_gate": w_gate.astype(jnp.bfloat16),
        "w_up": w_up.astype(jnp.bfloat16),
        "w_attn_out": w_attn_out.astype(jnp.bfloat16),
        "w_mlp_out": w_mlp_out.astype(jnp.bfloat16),
        "k_cache": k_cache.astype(jnp.bfloat16),
        "v_cache": v_cache.astype(jnp.bfloat16),
        "ctx_len": ctx_len,
    }


def apply_rope(vecs, positions):
    half_dim = vecs.shape[-1] // 2
    inv_freq = 10000.0 ** (-jnp.arange(half_dim, dtype=jnp.float32) / half_dim)
    angles = positions.astype(jnp.float32)[..., None] * inv_freq
    cos_t = jnp.cos(angles)
    sin_t = jnp.sin(angles)
    first_half = vecs[..., :half_dim]
    second_half = vecs[..., half_dim:]
    return jnp.concatenate([first_half * cos_t - second_half * sin_t, second_half * cos_t + first_half * sin_t], axis=-1)


def layer_norm(x_in, ln_gain):
    x_f32 = x_in.astype(jnp.float32)
    row_mean = jnp.sum(x_f32, axis=-1, keepdims=True) / D_MODEL
    row_var = jnp.sum(x_f32 * x_f32, axis=-1, keepdims=True) / D_MODEL - row_mean * row_mean
    normed = (x_f32 - row_mean) * lax.rsqrt(row_var + 1e-6) * ln_gain.astype(jnp.float32)
    return normed.astype(jnp.bfloat16)


def reference(x_in, ln_gain, w_qkv, w_gate, w_up, w_attn_out, w_mlp_out, k_cache, v_cache, ctx_len):
    normed = layer_norm(x_in, ln_gain)
    qkv_proj = jnp.dot(normed, w_qkv, preferred_element_type=jnp.float32).astype(jnp.bfloat16)
    gate_proj = jnp.dot(normed, w_gate, preferred_element_type=jnp.float32).astype(jnp.bfloat16)
    up_proj = jnp.dot(normed, w_up, preferred_element_type=jnp.float32).astype(jnp.bfloat16)
    mlp_act = (jax.nn.silu(gate_proj.astype(jnp.float32)) * up_proj.astype(jnp.float32)).astype(jnp.bfloat16)
    attn_cols = NUM_HEADS * HEAD_DIM
    q_heads = qkv_proj[:, :attn_cols].reshape(BATCH_SIZE, NUM_HEADS, HEAD_DIM)
    k_new = qkv_proj[:, attn_cols:attn_cols + HEAD_DIM]
    v_new = qkv_proj[:, attn_cols + HEAD_DIM:]
    q_rot = apply_rope(q_heads.astype(jnp.float32), ctx_len[:, None]).astype(jnp.bfloat16)
    k_rot = apply_rope(k_new.astype(jnp.float32), ctx_len).astype(jnp.bfloat16)
    positions = jnp.arange(CACHE_LEN)
    new_slot = (positions[None, :] == ctx_len[:, None])[:, :, None]
    k_out = jnp.where(new_slot, k_rot[:, None, :], k_cache)
    v_out = jnp.where(new_slot, v_new[:, None, :], v_cache)
    block_rows = 8
    n_blocks = BATCH_SIZE // block_rows

    def attend(block_in):
        q_blk, k_blk, v_blk, len_blk = block_in
        scores = jnp.einsum("bhd,btd->bht", q_blk.astype(jnp.float32), k_blk.astype(jnp.float32)) * HEAD_DIM ** -0.5
        visible = (positions[None, :] <= len_blk[:, None])[:, None, :]
        scores = jnp.where(visible, scores, -1e30)
        attn_probs = jax.nn.softmax(scores, axis=-1).astype(jnp.bfloat16)
        return jnp.einsum("bht,btd->bhd", attn_probs.astype(jnp.float32), v_blk.astype(jnp.float32)).astype(jnp.bfloat16)

    attn_heads = lax.map(attend, (
        q_rot.reshape(n_blocks, block_rows, NUM_HEADS, HEAD_DIM),
        k_out.reshape(n_blocks, block_rows, CACHE_LEN, HEAD_DIM),
        v_out.reshape(n_blocks, block_rows, CACHE_LEN, HEAD_DIM),
        ctx_len.reshape(n_blocks, block_rows),
    ))
    attn_flat = attn_heads.reshape(BATCH_SIZE, attn_cols)
    z_sum = jnp.dot(attn_flat, w_attn_out, preferred_element_type=jnp.float32) + jnp.dot(mlp_act, w_mlp_out, preferred_element_type=jnp.float32)
    y_out = (x_in.astype(jnp.float32) + z_sum).astype(jnp.bfloat16)
    return (y_out, k_out, v_out)
```

```python
import functools

import jax
import jax.numpy as jnp
from jax import lax
from jax.experimental import pallas as pl
from jax.experimental.pallas import tpu as pltpu
from jax.sharding import PartitionSpec as P

MESH = pl.DeviceIdType.MESH
F32 = jnp.float32
BF16 = jnp.bfloat16
VMEM_LIMIT = 66_900_000

C = 768
CQ = 640
SLOTS = 3
N1 = 4
N2 = 9


def remote(src, dst, send_sem, recv_sem, device):
    return pltpu.make_async_remote_copy(
        src_ref=src, dst_ref=dst, send_sem=send_sem, recv_sem=recv_sem, device_id=device, device_id_type=MESH
    )


def places():
    xi = lax.axis_index("x")
    yi = lax.axis_index("yz")
    sib = xi + 1 - 2 * (xi % 2)
    xn = (xi + 2) % 4
    return xi, yi, sib, xn, (sib + 2) % 4, 1 - yi


def activation(total):
    gate = total[:, :C].astype(BF16).astype(F32)
    up = total[:, C:].astype(BF16).astype(F32)
    return (jax.nn.silu(gate) * up).astype(BF16)


def front_kernel(
    d_model, x_ref, g_ref, wq_hbm, wg_hbm, wu_hbm,
    qkv_hbm, a_hbm, perm_hbm, send_hbm, own_hbm,
    stat, xbuf, gbuf, h, wq, wg, wu, pq, rq, xq, qs, qd, p, r, xr, a,
    wq_sem, wg_sem, wu_sem, st_s, st_r, xg_s, xg_r,
    dq_s, dq_r, xq_s, xq_r, yq_s, yq_r, d_s, d_r, x_s, x_r, out_sem, own_sem, q_sem, a_sem,
):
    xi, yi, sib, xn, sibn, yn = places()
    me = yi * 4 + xi
    rows, width = x_ref.shape
    num_q = wq_hbm.shape[1] // CQ
    num_c = wg_hbm.shape[1] // C
    sib_dev, xn_dev, yn_dev = {"x": sib}, {"x": xn}, {"yz": yn}

    def wq_copy(c):
        return pltpu.make_async_copy(wq_hbm.at[:, pl.ds(c * CQ, CQ)], wq.at[c], wq_sem.at[c])

    def w_copies(i, slot):
        start = pl.multiple_of(i * C, C)
        return (
            pltpu.make_async_copy(wg_hbm.at[:, pl.ds(start, C)], wg.at[slot], wg_sem.at[slot]),
            pltpu.make_async_copy(wu_hbm.at[:, pl.ds(start, C)], wu.at[slot], wu_sem.at[slot]),
        )

    for c in range(num_q):
        wq_copy(c).start()
    for i in range(SLOTS):
        for copy in w_copies(i, i):
            copy.start()

    barrier = pltpu.get_barrier_semaphore()
    offsets = [(dy, dx) for dy in range(2) for dx in range(4)][1:]
    for dy, dx in offsets:
        pl.semaphore_signal(barrier, inc=1, device_id={"yz": (yi + dy) % 2, "x": (xi + dx) % 4}, device_id_type=MESH)

    x_f32 = x_ref[...].astype(F32)
    lane = lax.broadcasted_iota(jnp.int32, (rows, rows), 1)
    sums = jnp.where(
        lane == 0,
        jnp.sum(x_f32, axis=1, keepdims=True),
        jnp.where(lane == 1, jnp.sum(x_f32 * x_f32, axis=1, keepdims=True), 0.0),
    )
    stat[me] = sums.T[0:8, :]
    gbuf[yi] = jnp.broadcast_to(g_ref[...].astype(F32), (8, width))
    xbuf[yi] = x_ref[...]
    pl.semaphore_wait(barrier, 7)

    def stat_copy(k, slot):
        dy, dx = offsets[k]
        dev = {"yz": (yi + dy) % 2, "x": (xi + dx) % 4}
        return remote(stat.at[slot], stat.at[slot], st_s.at[k], st_r.at[k], dev)

    def x_copy(slot):
        return remote(x_ref, xbuf.at[slot], xg_s.at[0], xg_r.at[0], yn_dev)

    def g_copy(slot):
        return remote(gbuf.at[slot], gbuf.at[slot], xg_s.at[1], xg_r.at[1], yn_dev)

    for k in range(7):
        stat_copy(k, me).start()
    g_copy(yi).start()
    x_copy(yi).start()
    for k, (dy, dx) in enumerate(offsets):
        stat_copy(k, ((yi + 2 - dy) % 2) * 4 + (xi + 4 - dx) % 4).wait_recv()
    total = stat[0]
    for k in range(1, 8):
        total = total + stat[k]
    cols = jnp.concatenate([total, jnp.zeros((rows - 8, rows), F32)], axis=0).T
    mean = cols[:, 0:1] / d_model
    var = cols[:, 1:2] / d_model - mean * mean
    scale = lax.rsqrt(var + 1e-6)
    g_copy(yn).wait_recv()
    x_copy(yn).wait_recv()
    for b in range(2):
        part = (xbuf[b].astype(F32) - mean) * scale * gbuf[b][0:1, :]
        h[:, b * width:(b + 1) * width] = part.astype(BF16)

    def dq(c, k):
        src = sib if k == 0 else sibn
        return remote(pq.at[c, src], rq.at[c, k], dq_s.at[c, k], dq_r.at[c, k], sib_dev)

    def xq_copy(c):
        return remote(pq.at[c, xn], xq.at[c], xq_s.at[c], xq_r.at[c], xn_dev)

    def q_sum(c):
        dq(c, 1).wait_recv()
        dq(c, 1).wait_send()
        pq[c, xn] = pq[c, xn] + rq[c, 1]
        xq_copy(c).start()
        dq(c, 0).wait_recv()
        dq(c, 0).wait_send()
        pq[c, xi] = pq[c, xi] + rq[c, 0]

    @pl.loop(0, num_q)
    def _(c):
        wq_copy(c).wait()
        prod = jnp.dot(h[...], wq[c], preferred_element_type=F32)
        pq[c] = prod.reshape(4, rows // 4, CQ)
        dq(c, 1).start()
        dq(c, 0).start()

        @pl.when(c >= 1)
        def _():
            q_sum(c - 1)

    def d_copy(i, k):
        src = sib if k == 0 else sibn
        return remote(p.at[i, src], r.at[i, k], d_s.at[i, k], d_r.at[i, k], sib_dev)

    def x_send(i):
        return remote(p.at[i, xn], xr.at[i], x_s.at[i], x_r.at[i], xn_dev)

    def perm_copy(i):
        return pltpu.make_async_copy(p.at[i, xn], perm_hbm.at[i - N1], out_sem.at[i])

    def send_copy(i):
        return pltpu.make_async_copy(p.at[i, xn], send_hbm.at[i - N2], out_sem.at[i])

    def own_copy(i):
        return pltpu.make_async_copy(p.at[i, xi], own_hbm.at[i - N1], own_sem.at[i])

    def chip_sum(i):
        d_copy(i, 1).wait_recv()
        d_copy(i, 1).wait_send()
        p[i, xn] = p[i, xn] + r[i, 1]

        @pl.when(i < N1)
        def _():
            x_send(i).start()

        @pl.when((i >= N1) & (i < N2))
        def _():
            perm_copy(i).start()

        @pl.when(i >= N2)
        def _():
            send_copy(i).start()

        d_copy(i, 0).wait_recv()
        d_copy(i, 0).wait_send()
        p[i, xi] = p[i, xi] + r[i, 0]

        @pl.when(i >= N1)
        def _():
            own_copy(i).start()

    def product(i):
        slot = i % SLOTS
        g_w, u_w = w_copies(i, slot)
        g_w.wait()
        p[i, :, :, :C] = jnp.dot(h[...], wg[slot], preferred_element_type=F32).reshape(4, rows // 4, C)
        u_w.wait()
        p[i, :, :, C:] = jnp.dot(h[...], wu[slot], preferred_element_type=F32).reshape(4, rows // 4, C)
        d_copy(i, 1).start()
        d_copy(i, 0).start()

        @pl.when(i + SLOTS < num_c)
        def _():
            for copy in w_copies(i + SLOTS, slot):
                copy.start()

    product(0)
    q_sum(num_q - 1)

    def step(i):
        product(i)
        chip_sum(i - 1)

    half = num_c // 2 + 1
    pl.loop(1, half)(step)

    @pl.loop(0, num_q)
    def _(c):
        xq_copy(c).wait_recv()
        xq_copy(c).wait_send()
        value = (pq[c, xi] + xq[c]).astype(BF16)
        qs[:, :, pl.ds(pl.multiple_of(c * CQ, CQ), CQ)] = value.reshape(2, rows // 8, CQ)

    def yq_copy(k):
        return remote(qs.at[1 - k], qd.at[k], yq_s, yq_r, yn_dev)

    yq_copy(yi).start()
    qd[yi] = qs[yi]

    pl.loop(half, num_c)(step)
    chip_sum(num_c - 1)
    yq_copy(yn).wait_recv()
    q_out = pltpu.make_async_copy(qd, qkv_hbm, q_sem)
    q_out.start()

    @pl.loop(0, N1)
    def _(i):
        x_send(i).wait_recv()
        x_send(i).wait_send()
        act = activation(p[i, xi] + xr[i])
        a[:, :, pl.ds(pl.multiple_of(i * C, C), C)] = act.reshape(2, rows // 8, C)

    a_out = pltpu.make_async_copy(a, a_hbm, a_sem)
    a_out.start()
    for k in range(7):
        stat_copy(k, me).wait_send()
    g_copy(yi).wait_send()
    x_copy(yi).wait_send()
    yq_copy(yi).wait_send()

    @pl.loop(N1, N2)
    def _(i):
        perm_copy(i).wait()
        own_copy(i).wait()

    @pl.loop(N2, num_c)
    def _(i):
        send_copy(i).wait()
        own_copy(i).wait()

    q_out.wait()
    a_out.wait()


def front(x_loc, gain_loc, wqkv, wgate, wup, d_model):
    rows, width = x_loc.shape
    depth, q_cols = wqkv.shape
    num_q, num_c = q_cols // CQ, wgate.shape[1] // C
    quarter = rows // 4
    dma = pltpu.SemaphoreType.DMA
    any_spec = pl.BlockSpec(memory_space=pl.ANY)
    vmem_spec = pl.BlockSpec(memory_space=pltpu.VMEM)
    return pl.pallas_call(
        functools.partial(front_kernel, d_model),
        name="front",
        out_shape=(
            jax.ShapeDtypeStruct((2, rows // 8, q_cols), BF16),
            jax.ShapeDtypeStruct((2, rows // 8, N1 * C), BF16),
            jax.ShapeDtypeStruct((N2 - N1, quarter, 2 * C), F32),
            jax.ShapeDtypeStruct((num_c - N2, quarter, 2 * C), F32),
            jax.ShapeDtypeStruct((num_c - N1, quarter, 2 * C), F32),
        ),
        in_specs=[vmem_spec, vmem_spec, any_spec, any_spec, any_spec],
        out_specs=(any_spec,) * 5,
        scratch_shapes=[
            pltpu.VMEM((8, 8, rows), F32),
            pltpu.VMEM((2, rows, width), BF16),
            pltpu.VMEM((2, 8, width), F32),
            pltpu.VMEM((rows, depth), BF16),
            pltpu.VMEM((num_q, depth, CQ), BF16),
            pltpu.VMEM((SLOTS, depth, C), BF16),
            pltpu.VMEM((SLOTS, depth, C), BF16),
            pltpu.VMEM((num_q, 4, quarter, CQ), F32),
            pltpu.VMEM((num_q, 2, quarter, CQ), F32),
            pltpu.VMEM((num_q, quarter, CQ), F32),
            pltpu.VMEM((2, rows // 8, q_cols), BF16),
            pltpu.VMEM((2, rows // 8, q_cols), BF16),
            pltpu.VMEM((num_c, 4, quarter, 2 * C), F32),
            pltpu.VMEM((num_c, 2, quarter, 2 * C), F32),
            pltpu.VMEM((N1, quarter, 2 * C), F32),
            pltpu.VMEM((2, rows // 8, N1 * C), BF16),
            dma((num_q,)), dma((SLOTS,)), dma((SLOTS,)), dma((7,)), dma((7,)), dma((2,)), dma((2,)),
            dma((num_q, 2)), dma((num_q, 2)), dma((num_q,)), dma((num_q,)), dma, dma,
            dma((num_c, 2)), dma((num_c, 2)), dma((N1,)), dma((N1,)), dma((num_c,)), dma((num_c,)), dma, dma,
        ],
        compiler_params=pltpu.CompilerParams(collective_id=0, has_side_effects=True, vmem_limit_bytes=VMEM_LIMIT),
        cost_estimate=pl.CostEstimate(
            flops=2 * rows * depth * (q_cols + 2 * wgate.shape[1]),
            bytes_accessed=2 * depth * (q_cols + 2 * wgate.shape[1]),
            transcendentals=0,
        ),
    )(x_loc, gain_loc, wqkv, wgate, wup)


def attend_kernel(len_ref, qkv_ref, cos_ref, sin_ref, k_ref, v_ref, ko_ref, vo_ref, o_ref):
    pos = len_ref[pl.program_id(0)]
    qkv = qkv_ref[0]
    heads, head_dim = qkv.shape[0] - 2, qkv.shape[1]
    wide = qkv.astype(F32)
    turned = (wide * cos_ref[0] + pltpu.roll(wide, head_dim // 2, 1) * sin_ref[0]).astype(BF16)
    query = turned[:heads]
    ko_ref[...] = k_ref[...]
    vo_ref[...] = v_ref[...]
    base = pl.multiple_of((pos // 16) * 16, 16)
    here = lax.broadcasted_iota(jnp.int32, (16, head_dim), 0) == pos - base
    for out, new in ((ko_ref, turned[heads:heads + 1]), (vo_ref, qkv[heads + 1:heads + 2])):
        tile = out[0, pl.ds(base, 16), :].astype(F32)
        out[0, pl.ds(base, 16), :] = jnp.where(here, new.astype(F32), tile).astype(BF16)
    scores = lax.dot_general(query, ko_ref[0], (((1,), (1,)), ((), ())), preferred_element_type=F32)
    scores = scores * head_dim ** -0.5
    at = lax.broadcasted_iota(jnp.int32, scores.shape, 1)
    scores = jnp.where(at <= pos, scores, -1e30)
    weight = jnp.exp(scores - jnp.max(scores, axis=1, keepdims=True))
    probs = (weight / jnp.sum(weight, axis=1, keepdims=True)).astype(BF16)
    o_ref[0] = jnp.dot(probs, vo_ref[0], preferred_element_type=F32).astype(BF16)


def attend(qkv, cos, sin, k_cache, v_cache, ctx_len):
    reqs, length, head_dim = k_cache.shape
    heads = qkv.shape[1] - 2
    cache_spec = pl.BlockSpec((1, length, head_dim), lambda i, lens: (i, 0, 0))
    table_spec = pl.BlockSpec((1, 1, head_dim), lambda i, lens: (i, 0, 0))
    return pl.pallas_call(
        attend_kernel,
        name="attend",
        grid_spec=pltpu.PrefetchScalarGridSpec(
            num_scalar_prefetch=1,
            grid=(reqs,),
            in_specs=[
                pl.BlockSpec((1, heads + 2, head_dim), lambda i, lens: (i, 0, 0)),
                table_spec, table_spec, cache_spec, cache_spec,
            ],
            out_specs=[cache_spec, cache_spec, pl.BlockSpec((1, heads, head_dim), lambda i, lens: (i, 0, 0))],
        ),
        out_shape=(
            jax.ShapeDtypeStruct(k_cache.shape, BF16),
            jax.ShapeDtypeStruct(v_cache.shape, BF16),
            jax.ShapeDtypeStruct((reqs, heads, head_dim), BF16),
        ),
        compiler_params=pltpu.CompilerParams(dimension_semantics=("arbitrary",)),
        cost_estimate=pl.CostEstimate(
            flops=64 * reqs * heads * length * head_dim,
            bytes_accessed=8 * reqs * length * head_dim,
            transcendentals=reqs * heads * length,
        ),
    )(ctx_len, qkv, cos, sin, k_cache, v_cache)


def back_kernel(
    x_ref, o_ref, a1_ref, own_hbm, perm_hbm, send_hbm, wao_hbm, wmo_hbm, y_ref,
    w, own, xr, act, z, zr,
    w_sem, own_sem, x_s, x_r, o_s, o_r, sib_s, sib_r, xn_s, xn_r, fwd_s, fwd_r, z_s, z_r,
):
    xi, yi, sib, xn, _, yn = places()
    sib_dev, xn_dev, yn_dev = {"x": sib}, {"x": xn}, {"yz": yn}
    rows = x_ref.shape[0]
    num_o, num_c = wao_hbm.shape[0] // C, wmo_hbm.shape[0] // C
    num_k = num_o + num_c
    o_cols = wao_hbm.shape[0]
    late = num_c - N1
    here = N2 - N1

    def w_copy(k):
        src = wao_hbm.at[pl.ds(k * C, C), :] if k < num_o else wmo_hbm.at[pl.ds((k - num_o) * C, C), :]
        return pltpu.make_async_copy(src, w.at[k], w_sem.at[k])

    def own_copy(i):
        return pltpu.make_async_copy(own_hbm.at[i], own.at[i], own_sem.at[i])

    def perm_copy(i):
        return pltpu.make_async_copy(perm_hbm.at[i], xr.at[i], x_r.at[i])

    def x_send(i):
        return remote(send_hbm.at[i - here], xr.at[i], x_s.at[i - here], x_r.at[i], xn_dev)

    barrier = pltpu.get_barrier_semaphore()
    for dev in (sib_dev, xn_dev, yn_dev):
        pl.semaphore_signal(barrier, inc=1, device_id=dev, device_id_type=MESH)
    for i in range(here):
        perm_copy(i).start()
        own_copy(i).start()
    for i in range(here, late):
        own_copy(i).start()
    for k in range(num_k):
        w_copy(k).start()
    z[...] = jnp.zeros_like(z)
    act[2 * xi + yi, :, :o_cols] = o_ref[yi]
    act[pl.ds(2 * xi, 2), :, o_cols:o_cols + N1 * C] = a1_ref[...]
    pl.semaphore_wait(barrier, 3)

    def o_copy(half, row):
        return remote(o_ref.at[half], act.at[2 * xi + row, :, 0:o_cols], o_s, o_r, yn_dev)

    def cols_of(e):
        if isinstance(e, int) and e == 0:
            return pl.ds(o_cols, N1 * C)
        if isinstance(e, int) and e == 1:
            return pl.ds(0, o_cols)
        return pl.ds(pl.multiple_of(o_cols + (N1 + e - 2) * C, C), C)

    def gather(e, owner, dev, send_sem, recv_sem):
        block = act.at[pl.ds(2 * owner, 2), :, cols_of(e)]
        return remote(block, block, send_sem.at[e], recv_sem.at[e], dev)

    def to_sib(e, owner):
        return gather(e, owner, sib_dev, sib_s, sib_r)

    def to_xn(e, owner):
        return gather(e, owner, xn_dev, xn_s, xn_r)

    def forward(e, owner):
        return gather(e, owner, sib_dev, fwd_s, fwd_r)

    def send_own(e):
        to_xn(e, xi).start()
        to_sib(e, xi).start()

    def pass_on(e):
        to_xn(e, xn).wait_recv()
        forward(e, xn).start()

    def arrived(e):
        to_sib(e, sib).wait_recv()
        forward(e, (sib + 2) % 4).wait_recv()

    def multiply(k, start):
        lhs = act[:, :, pl.ds(start, C)].reshape(rows, C)
        width = z.shape[2]
        for b in range(2):
            z[b] = z[b] + jnp.dot(lhs, w[k, :, b * width:(b + 1) * width], preferred_element_type=F32)

    def late_multiply(i):
        k = num_o + N1 + i
        pltpu.make_async_copy(wmo_hbm.at[pl.ds(0, C), :], w.at[k], w_sem.at[k]).wait()
        multiply(k, pl.multiple_of(k * C, C))

    def activate(i):
        own_copy(i).wait()
        value = activation(own[i] + xr[i])
        start = pl.multiple_of(o_cols + (N1 + i) * C, C)
        act[pl.ds(2 * xi, 2), :, pl.ds(start, C)] = value.reshape(2, rows // 8, C)

    ahead = 2
    o_copy(yn, yi).start()
    send_own(0)
    for i in range(here, min(here + ahead, late)):
        x_send(i).start()

    @pl.loop(0, here)
    def _(i):
        perm_copy(i).wait()
        activate(i)
        send_own(i + 2)

    o_copy(yi, yn).wait_recv()
    send_own(1)
    pass_on(0)
    pass_on(1)
    arrived(0)
    for k in range(num_o, num_o + N1):
        w_copy(k).wait()
        multiply(k, k * C)
    arrived(1)
    for k in range(num_o):
        w_copy(k).wait()
        multiply(k, k * C)

    @pl.loop(0, here)
    def _(i):
        pass_on(i + 2)

    @pl.loop(here, late)
    def _(i):
        x_send(i).wait_recv()
        activate(i)

        @pl.when(i + ahead < late)
        def _():
            x_send(i + ahead).start()

        send_own(i + 2)
        arrived(i - here + 2)
        late_multiply(i - here)

        @pl.when(i > here)
        def _():
            pass_on(i + 1)

    pass_on(late + 1)

    @pl.loop(late - here, late)
    def _(i):
        arrived(i + 2)
        late_multiply(i)

    z_copy = remote(z.at[yn], zr, z_s, z_r, yn_dev)
    z_copy.start()
    o_copy(yn, yi).wait_send()
    for e in range(2):
        to_xn(e, xi).wait_send()
        to_sib(e, xi).wait_send()
        forward(e, xn).wait_send()

    @pl.loop(2, late + 2)
    def _(e):
        to_xn(e, xi).wait_send()
        to_sib(e, xi).wait_send()
        forward(e, xn).wait_send()

    @pl.loop(here, late)
    def _(i):
        x_send(i).wait_send()

    z_copy.wait()
    y_ref[...] = (x_ref[...].astype(F32) + (z[yi] + zr[...])).astype(BF16)


def back(x_loc, o_halves, a1, own, perm, send, wao, wmo):
    rows, width = x_loc.shape
    num_o, num_c = wao.shape[0] // C, wmo.shape[0] // C
    num_k, late, groups = num_o + num_c, num_c - N1, 2 + num_c - N1
    quarter = rows // 4
    dma = pltpu.SemaphoreType.DMA
    any_spec = pl.BlockSpec(memory_space=pl.ANY)
    vmem_spec = pl.BlockSpec(memory_space=pltpu.VMEM)
    return pl.pallas_call(
        back_kernel,
        name="back",
        out_shape=jax.ShapeDtypeStruct((rows, width), BF16),
        in_specs=[vmem_spec] * 3 + [any_spec] * 5,
        out_specs=vmem_spec,
        scratch_shapes=[
            pltpu.VMEM((num_k, C, 2 * width), BF16),
            pltpu.VMEM((late, quarter, 2 * C), F32),
            pltpu.VMEM((late, quarter, 2 * C), F32),
            pltpu.VMEM((8, rows // 8, num_k * C), BF16),
            pltpu.VMEM((2, rows, width), F32),
            pltpu.VMEM((rows, width), F32),
            dma((num_k,)), dma((late,)), dma((num_c - N2,)), dma((late,)), dma, dma,
            dma((groups,)), dma((groups,)), dma((groups,)), dma((groups,)), dma((groups,)), dma((groups,)), dma, dma,
        ],
        compiler_params=pltpu.CompilerParams(collective_id=1, has_side_effects=True, vmem_limit_bytes=VMEM_LIMIT),
        cost_estimate=pl.CostEstimate(
            flops=4 * rows * num_k * C * width, bytes_accessed=4 * num_k * C * width, transcendentals=0
        ),
    )(x_loc, o_halves, a1, own, perm, send, wao, wmo)


def solution(mesh):
    x_size, yz_size = mesh.shape["x"], mesh.shape["yz"]
    both_axes = ("x", "yz")
    row_spec = P("dp", both_axes)
    in_w_spec = P("x", "yz")
    out_w_spec = P("yz", "x")
    cache_spec = P(("dp", "x", "yz"), None, None)
    len_spec = P(("dp", "x", "yz"))
    across = [(i, (i + 2) % 4) for i in range(4)]

    def local_layer(x_loc, gain_loc, wqkv_loc, wgate_loc, wup_loc, wao_loc, wmo_loc, kc_loc, vc_loc, len_loc):
        d_model = x_loc.shape[1] * x_size * yz_size
        reqs, _, head_dim = kc_loc.shape
        half = head_dim // 2
        inv_freq = 10000.0 ** (-jnp.arange(half, dtype=F32) / half)
        angles = len_loc.astype(F32)[:, None] * inv_freq
        cos, sin = jnp.cos(angles), jnp.sin(angles)
        cos = jnp.concatenate([cos, cos], axis=1)[:, None, :]
        sin = jnp.concatenate([-sin, sin], axis=1)[:, None, :]

        qkv, a1, perm, send, own = front(
            x_loc, gain_loc[None, :], wqkv_loc, wgate_loc, wup_loc, d_model
        )
        perm = lax.ppermute(perm, "x", across)
        qkv = jnp.concatenate([qkv[0], qkv[1]], axis=1).reshape(reqs, -1, head_dim)
        k_all, v_all, attn = attend(qkv, cos, sin, kc_loc, vc_loc, len_loc)
        o_halves = jnp.swapaxes(attn.reshape(reqs, 2, -1), 0, 1)
        y_loc = back(x_loc, o_halves, a1, own, perm, send, wao_loc, wmo_loc)
        return y_loc, k_all, v_all

    in_specs = (row_spec, P(both_axes), in_w_spec, in_w_spec, in_w_spec, out_w_spec, out_w_spec, cache_spec, cache_spec, len_spec)
    out_specs = (row_spec, cache_spec, cache_spec)
    return jax.shard_map(local_layer, mesh=mesh, in_specs=in_specs, out_specs=out_specs, check_vma=False)
```

```python
import functools

import jax
import jax.numpy as jnp
from jax import lax
from jax.experimental import pallas as pl
from jax.experimental.pallas import tpu as pltpu
from jax.sharding import PartitionSpec as P

MESH = pl.DeviceIdType.MESH
F32 = jnp.float32
BF16 = jnp.bfloat16
VMEM_LIMIT = 66_900_000

C = 768
CQ = 640
SLOTS = 3
N1 = 4
N2 = 12


def remote(src, dst, send_sem, recv_sem, device):
    return pltpu.make_async_remote_copy(
        src_ref=src, dst_ref=dst, send_sem=send_sem, recv_sem=recv_sem, device_id=device, device_id_type=MESH
    )


def places():
    xi = lax.axis_index("x")
    yi = lax.axis_index("yz")
    sib = xi + 1 - 2 * (xi % 2)
    xn = (xi + 2) % 4
    return xi, yi, sib, xn, (sib + 2) % 4, 1 - yi


def activation(total):
    gate = total[:, :C].astype(BF16).astype(F32)
    up = total[:, C:].astype(BF16).astype(F32)
    return (jax.nn.silu(gate) * up).astype(BF16)


def front_kernel(
    d_model, x_ref, g_ref, wq_hbm, wg_hbm, wu_hbm,
    qkv_hbm, a_hbm, perm_hbm, send_hbm, own_hbm,
    stat, xbuf, gbuf, h, wq, wg, wu, pq, rq, xq, qs, qd, p, r, xr, a,
    wq_sem, wg_sem, wu_sem, st_s, st_r, xg_s, xg_r,
    dq_s, dq_r, xq_s, xq_r, yq_s, yq_r, d_s, d_r, x_s, x_r, out_sem, own_sem, q_sem, a_sem,
):
    xi, yi, sib, xn, sibn, yn = places()
    me = yi * 4 + xi
    rows, width = x_ref.shape
    num_q = wq_hbm.shape[1] // CQ
    num_c = wg_hbm.shape[1] // C
    sib_dev, xn_dev, yn_dev = {"x": sib}, {"x": xn}, {"yz": yn}

    def wq_copy(c):
        return pltpu.make_async_copy(wq_hbm.at[:, pl.ds(c * CQ, CQ)], wq.at[c], wq_sem.at[c])

    def w_copies(i, slot):
        start = pl.multiple_of(i * C, C)
        return (
            pltpu.make_async_copy(wg_hbm.at[:, pl.ds(start, C)], wg.at[slot], wg_sem.at[slot]),
            pltpu.make_async_copy(wu_hbm.at[:, pl.ds(start, C)], wu.at[slot], wu_sem.at[slot]),
        )

    for c in range(num_q):
        wq_copy(c).start()
    for i in range(SLOTS):
        for copy in w_copies(i, i):
            copy.start()

    barrier = pltpu.get_barrier_semaphore()
    offsets = [(dy, dx) for dy in range(2) for dx in range(4)][1:]
    for dy, dx in offsets:
        pl.semaphore_signal(barrier, inc=1, device_id={"yz": (yi + dy) % 2, "x": (xi + dx) % 4}, device_id_type=MESH)

    x_f32 = x_ref[...].astype(F32)
    lane = lax.broadcasted_iota(jnp.int32, (rows, rows), 1)
    sums = jnp.where(
        lane == 0,
        jnp.sum(x_f32, axis=1, keepdims=True),
        jnp.where(lane == 1, jnp.sum(x_f32 * x_f32, axis=1, keepdims=True), 0.0),
    )
    stat[me] = sums.T[0:8, :]
    gbuf[yi] = jnp.broadcast_to(g_ref[...].astype(F32)[None, :], (8, width))
    xbuf[yi] = x_ref[...]
    pl.semaphore_wait(barrier, 7)

    def stat_copy(k, slot):
        dy, dx = offsets[k]
        dev = {"yz": (yi + dy) % 2, "x": (xi + dx) % 4}
        return remote(stat.at[slot], stat.at[slot], st_s.at[k], st_r.at[k], dev)

    def x_copy(slot):
        return remote(x_ref, xbuf.at[slot], xg_s.at[0], xg_r.at[0], yn_dev)

    def g_copy(slot):
        return remote(gbuf.at[slot], gbuf.at[slot], xg_s.at[1], xg_r.at[1], yn_dev)

    for k in range(7):
        stat_copy(k, me).start()
    g_copy(yi).start()
    x_copy(yi).start()
    for k, (dy, dx) in enumerate(offsets):
        stat_copy(k, ((yi + 2 - dy) % 2) * 4 + (xi + 4 - dx) % 4).wait_recv()
    total = stat[0]
    for k in range(1, 8):
        total = total + stat[k]
    cols = jnp.concatenate([total, jnp.zeros((rows - 8, rows), F32)], axis=0).T
    mean = cols[:, 0:1] / d_model
    var = cols[:, 1:2] / d_model - mean * mean
    scale = lax.rsqrt(var + 1e-6)
    g_copy(yn).wait_recv()
    x_copy(yn).wait_recv()
    for b in range(2):
        part = (xbuf[b].astype(F32) - mean) * scale * gbuf[b][0:1, :]
        h[:, b * width:(b + 1) * width] = part.astype(BF16)

    def dq(c, k):
        src = sib if k == 0 else sibn
        return remote(pq.at[c, src], rq.at[c, k], dq_s.at[c, k], dq_r.at[c, k], sib_dev)

    def xq_copy(c):
        return remote(pq.at[c, xn], xq.at[c], xq_s.at[c], xq_r.at[c], xn_dev)

    def q_sum(c):
        dq(c, 1).wait_recv()
        dq(c, 1).wait_send()
        pq[c, xn] = pq[c, xn] + rq[c, 1]
        xq_copy(c).start()
        dq(c, 0).wait_recv()
        dq(c, 0).wait_send()
        pq[c, xi] = pq[c, xi] + rq[c, 0]

    @pl.loop(0, num_q)
    def _(c):
        wq_copy(c).wait()
        prod = jnp.dot(h[...], wq[c], preferred_element_type=F32)
        pq[c] = prod.reshape(4, rows // 4, CQ)
        dq(c, 1).start()
        dq(c, 0).start()

        @pl.when(c >= 1)
        def _():
            q_sum(c - 1)

    def d_copy(i, k):
        src = sib if k == 0 else sibn
        return remote(p.at[i, src], r.at[i, k], d_s.at[i, k], d_r.at[i, k], sib_dev)

    def x_send(i):
        return remote(p.at[i, xn], xr.at[i], x_s.at[i], x_r.at[i], xn_dev)

    def perm_copy(i):
        return pltpu.make_async_copy(p.at[i, xn], perm_hbm.at[i - N1], out_sem.at[i])

    def send_copy(i):
        return pltpu.make_async_copy(p.at[i, xn], send_hbm.at[i - N2], out_sem.at[i])

    def own_copy(i):
        return pltpu.make_async_copy(p.at[i, xi], own_hbm.at[i - N1], own_sem.at[i])

    def chip_sum(i):
        d_copy(i, 1).wait_recv()
        d_copy(i, 1).wait_send()
        p[i, xn] = p[i, xn] + r[i, 1]

        @pl.when(i < N1)
        def _():
            x_send(i).start()

        @pl.when((i >= N1) & (i < N2))
        def _():
            perm_copy(i).start()

        @pl.when(i >= N2)
        def _():
            send_copy(i).start()

        d_copy(i, 0).wait_recv()
        d_copy(i, 0).wait_send()
        p[i, xi] = p[i, xi] + r[i, 0]

        @pl.when(i >= N1)
        def _():
            own_copy(i).start()

    def product(i):
        slot = i % SLOTS
        g_w, u_w = w_copies(i, slot)
        g_w.wait()
        p[i, :, :, :C] = jnp.dot(h[...], wg[slot], preferred_element_type=F32).reshape(4, rows // 4, C)
        u_w.wait()
        p[i, :, :, C:] = jnp.dot(h[...], wu[slot], preferred_element_type=F32).reshape(4, rows // 4, C)
        d_copy(i, 1).start()
        d_copy(i, 0).start()

        @pl.when(i + SLOTS < num_c)
        def _():
            for copy in w_copies(i + SLOTS, slot):
                copy.start()

    product(0)
    q_sum(num_q - 1)

    def step(i):
        product(i)
        chip_sum(i - 1)

    half = num_c // 2 + 1
    pl.loop(1, half)(step)

    @pl.loop(0, num_q)
    def _(c):
        xq_copy(c).wait_recv()
        xq_copy(c).wait_send()
        value = (pq[c, xi] + xq[c]).astype(BF16)
        qs[:, :, pl.ds(pl.multiple_of(c * CQ, CQ), CQ)] = value.reshape(2, rows // 8, CQ)

    def yq_copy(k):
        return remote(qs.at[1 - k], qd.at[k], yq_s, yq_r, yn_dev)

    yq_copy(yi).start()
    qd[yi] = qs[yi]

    pl.loop(half, num_c)(step)
    chip_sum(num_c - 1)
    yq_copy(yn).wait_recv()
    q_out = pltpu.make_async_copy(qd, qkv_hbm, q_sem)
    q_out.start()

    @pl.loop(0, N1)
    def _(i):
        x_send(i).wait_recv()
        x_send(i).wait_send()
        act = activation(p[i, xi] + xr[i])
        a[:, :, pl.ds(pl.multiple_of(i * C, C), C)] = act.reshape(2, rows // 8, C)

    a_out = pltpu.make_async_copy(a, a_hbm, a_sem)
    a_out.start()
    for k in range(7):
        stat_copy(k, me).wait_send()
    g_copy(yi).wait_send()
    x_copy(yi).wait_send()
    yq_copy(yi).wait_send()

    @pl.loop(N1, N2)
    def _(i):
        perm_copy(i).wait()
        own_copy(i).wait()

    @pl.loop(N2, num_c)
    def _(i):
        send_copy(i).wait()
        own_copy(i).wait()

    q_out.wait()
    a_out.wait()


def front(x_loc, gain_loc, wqkv, wgate, wup, d_model):
    rows, width = x_loc.shape
    depth, q_cols = wqkv.shape
    num_q, num_c = q_cols // CQ, wgate.shape[1] // C
    quarter = rows // 4
    dma = pltpu.SemaphoreType.DMA
    any_spec = pl.BlockSpec(memory_space=pl.ANY)
    vmem_spec = pl.BlockSpec(memory_space=pltpu.VMEM)
    return pl.pallas_call(
        functools.partial(front_kernel, d_model),
        name="front",
        out_shape=(
            jax.ShapeDtypeStruct((2, rows // 8, q_cols), BF16),
            jax.ShapeDtypeStruct((2, rows // 8, N1 * C), BF16),
            jax.ShapeDtypeStruct((N2 - N1, quarter, 2 * C), F32),
            jax.ShapeDtypeStruct((num_c - N2, quarter, 2 * C), F32),
            jax.ShapeDtypeStruct((num_c - N1, quarter, 2 * C), F32),
        ),
        in_specs=[vmem_spec, vmem_spec, any_spec, any_spec, any_spec],
        out_specs=(any_spec,) * 5,
        scratch_shapes=[
            pltpu.VMEM((8, 8, rows), F32),
            pltpu.VMEM((2, rows, width), BF16),
            pltpu.VMEM((2, 8, width), F32),
            pltpu.VMEM((rows, depth), BF16),
            pltpu.VMEM((num_q, depth, CQ), BF16),
            pltpu.VMEM((SLOTS, depth, C), BF16),
            pltpu.VMEM((SLOTS, depth, C), BF16),
            pltpu.VMEM((num_q, 4, quarter, CQ), F32),
            pltpu.VMEM((num_q, 2, quarter, CQ), F32),
            pltpu.VMEM((num_q, quarter, CQ), F32),
            pltpu.VMEM((2, rows // 8, q_cols), BF16),
            pltpu.VMEM((2, rows // 8, q_cols), BF16),
            pltpu.VMEM((num_c, 4, quarter, 2 * C), F32),
            pltpu.VMEM((num_c, 2, quarter, 2 * C), F32),
            pltpu.VMEM((N1, quarter, 2 * C), F32),
            pltpu.VMEM((2, rows // 8, N1 * C), BF16),
            dma((num_q,)), dma((SLOTS,)), dma((SLOTS,)), dma((7,)), dma((7,)), dma((2,)), dma((2,)),
            dma((num_q, 2)), dma((num_q, 2)), dma((num_q,)), dma((num_q,)), dma, dma,
            dma((num_c, 2)), dma((num_c, 2)), dma((N1,)), dma((N1,)), dma((num_c,)), dma((num_c,)), dma, dma,
        ],
        compiler_params=pltpu.CompilerParams(collective_id=0, has_side_effects=True, vmem_limit_bytes=VMEM_LIMIT),
        cost_estimate=pl.CostEstimate(
            flops=2 * rows * depth * (q_cols + 2 * wgate.shape[1]),
            bytes_accessed=2 * depth * (q_cols + 2 * wgate.shape[1]),
            transcendentals=0,
        ),
    )(x_loc, gain_loc, wqkv, wgate, wup)


def attend_kernel(len_ref, qkv_ref, cos_ref, sin_ref, k_ref, v_ref, ko_ref, vo_ref, o_ref):
    pos = len_ref[pl.program_id(0)]
    qkv = qkv_ref[0]
    heads, head_dim = qkv.shape[0] - 2, qkv.shape[1]
    wide = qkv.astype(F32)
    turned = (wide * cos_ref[0] + pltpu.roll(wide, head_dim // 2, 1) * sin_ref[0]).astype(BF16)
    query = turned[:heads]
    ko_ref[...] = k_ref[...]
    vo_ref[...] = v_ref[...]
    base = pl.multiple_of((pos // 16) * 16, 16)
    here = lax.broadcasted_iota(jnp.int32, (16, head_dim), 0) == pos - base
    for out, new in ((ko_ref, turned[heads:heads + 1]), (vo_ref, qkv[heads + 1:heads + 2])):
        tile = out[0, pl.ds(base, 16), :].astype(F32)
        out[0, pl.ds(base, 16), :] = jnp.where(here, new.astype(F32), tile).astype(BF16)
    scores = lax.dot_general(query, ko_ref[0], (((1,), (1,)), ((), ())), preferred_element_type=F32)
    scores = scores * head_dim ** -0.5
    at = lax.broadcasted_iota(jnp.int32, scores.shape, 1)
    scores = jnp.where(at <= pos, scores, -1e30)
    weight = jnp.exp(scores - jnp.max(scores, axis=1, keepdims=True))
    probs = (weight / jnp.sum(weight, axis=1, keepdims=True)).astype(BF16)
    o_ref[0] = jnp.dot(probs, vo_ref[0], preferred_element_type=F32).astype(BF16)


def attend(qkv, cos, sin, k_cache, v_cache, ctx_len):
    reqs, length, head_dim = k_cache.shape
    heads = qkv.shape[1] - 2
    cache_spec = pl.BlockSpec((1, length, head_dim), lambda i, lens: (i, 0, 0))
    table_spec = pl.BlockSpec((1, 1, head_dim), lambda i, lens: (i, 0, 0))
    return pl.pallas_call(
        attend_kernel,
        name="attend",
        grid_spec=pltpu.PrefetchScalarGridSpec(
            num_scalar_prefetch=1,
            grid=(reqs,),
            in_specs=[
                pl.BlockSpec((1, heads + 2, head_dim), lambda i, lens: (i, 0, 0)),
                table_spec, table_spec, cache_spec, cache_spec,
            ],
            out_specs=[cache_spec, cache_spec, pl.BlockSpec((1, heads, head_dim), lambda i, lens: (i, 0, 0))],
        ),
        out_shape=(
            jax.ShapeDtypeStruct(k_cache.shape, BF16),
            jax.ShapeDtypeStruct(v_cache.shape, BF16),
            jax.ShapeDtypeStruct((reqs, heads, head_dim), BF16),
        ),
        compiler_params=pltpu.CompilerParams(dimension_semantics=("arbitrary",)),
        cost_estimate=pl.CostEstimate(
            flops=64 * reqs * heads * length * head_dim,
            bytes_accessed=8 * reqs * length * head_dim,
            transcendentals=reqs * heads * length,
        ),
    )(ctx_len, qkv, cos, sin, k_cache, v_cache)


def back_kernel(
    x_ref, o_ref, a1_ref, own_hbm, perm_hbm, send_hbm, wao_hbm, wmo_hbm, y_ref,
    w, own, xr, act, z, zr,
    w_sem, own_sem, x_s, x_r, o_s, o_r, sib_s, sib_r, xn_s, xn_r, fwd_s, fwd_r, z_s, z_r,
):
    xi, yi, sib, xn, _, yn = places()
    sib_dev, xn_dev, yn_dev = {"x": sib}, {"x": xn}, {"yz": yn}
    rows = x_ref.shape[0]
    num_o, num_c = wao_hbm.shape[0] // C, wmo_hbm.shape[0] // C
    num_k = num_o + num_c
    o_cols = wao_hbm.shape[0]
    late = num_c - N1
    here = N2 - N1

    def w_copy(k):
        src = wao_hbm.at[pl.ds(k * C, C), :] if k < num_o else wmo_hbm.at[pl.ds((k - num_o) * C, C), :]
        return pltpu.make_async_copy(src, w.at[k], w_sem.at[k])

    def own_copy(i):
        return pltpu.make_async_copy(own_hbm.at[i], own.at[i], own_sem.at[i])

    def perm_copy(i):
        return pltpu.make_async_copy(perm_hbm.at[i], xr.at[i], x_r.at[i])

    def x_send(i):
        return remote(send_hbm.at[i - here], xr.at[i], x_s.at[i - here], x_r.at[i], xn_dev)

    barrier = pltpu.get_barrier_semaphore()
    for dev in (sib_dev, xn_dev, yn_dev):
        pl.semaphore_signal(barrier, inc=1, device_id=dev, device_id_type=MESH)
    for i in range(here):
        perm_copy(i).start()
        own_copy(i).start()
    for i in range(here, late):
        own_copy(i).start()
    for k in range(num_k):
        w_copy(k).start()
    z[...] = jnp.zeros_like(z)
    act[2 * xi + yi, :, :o_cols] = o_ref[yi]
    act[pl.ds(2 * xi, 2), :, o_cols:o_cols + N1 * C] = a1_ref[...]
    pl.semaphore_wait(barrier, 3)

    def o_copy(half, row):
        return remote(o_ref.at[half], act.at[2 * xi + row, :, 0:o_cols], o_s, o_r, yn_dev)

    def cols_of(e):
        if isinstance(e, int) and e == 0:
            return pl.ds(o_cols, N1 * C)
        if isinstance(e, int) and e == 1:
            return pl.ds(0, o_cols)
        return pl.ds(pl.multiple_of(o_cols + (N1 + e - 2) * C, C), C)

    def gather(e, owner, dev, send_sem, recv_sem):
        block = act.at[pl.ds(2 * owner, 2), :, cols_of(e)]
        return remote(block, block, send_sem.at[e], recv_sem.at[e], dev)

    def to_sib(e, owner):
        return gather(e, owner, sib_dev, sib_s, sib_r)

    def to_xn(e, owner):
        return gather(e, owner, xn_dev, xn_s, xn_r)

    def forward(e, owner):
        return gather(e, owner, sib_dev, fwd_s, fwd_r)

    def send_own(e):
        to_xn(e, xi).start()
        to_sib(e, xi).start()

    def pass_on(e):
        to_xn(e, xn).wait_recv()
        forward(e, xn).start()

    def arrived(e):
        to_sib(e, sib).wait_recv()
        forward(e, (sib + 2) % 4).wait_recv()

    def multiply(k, start):
        lhs = act[:, :, pl.ds(start, C)].reshape(rows, C)
        width = z.shape[2]
        for b in range(2):
            z[b] = z[b] + jnp.dot(lhs, w[k, :, b * width:(b + 1) * width], preferred_element_type=F32)

    def late_multiply(i):
        k = num_o + N1 + i
        pltpu.make_async_copy(wmo_hbm.at[pl.ds(0, C), :], w.at[k], w_sem.at[k]).wait()
        multiply(k, pl.multiple_of(k * C, C))

    def activate(i):
        own_copy(i).wait()
        value = activation(own[i] + xr[i])
        start = pl.multiple_of(o_cols + (N1 + i) * C, C)
        act[pl.ds(2 * xi, 2), :, pl.ds(start, C)] = value.reshape(2, rows // 8, C)

    ahead = 2
    o_copy(yn, yi).start()
    send_own(0)
    for i in range(here, min(here + ahead, late)):
        x_send(i).start()

    @pl.loop(0, here)
    def _(i):
        perm_copy(i).wait()
        activate(i)
        send_own(i + 2)

    o_copy(yi, yn).wait_recv()
    send_own(1)
    pass_on(0)
    pass_on(1)
    arrived(0)
    for k in range(num_o, num_o + N1):
        w_copy(k).wait()
        multiply(k, k * C)
    arrived(1)
    for k in range(num_o):
        w_copy(k).wait()
        multiply(k, k * C)

    @pl.loop(0, here)
    def _(i):
        pass_on(i + 2)

    @pl.loop(here, late)
    def _(i):
        x_send(i).wait_recv()
        activate(i)

        @pl.when(i + ahead < late)
        def _():
            x_send(i + ahead).start()

        send_own(i + 2)
        arrived(i - here + 2)
        late_multiply(i - here)

        @pl.when(i > here)
        def _():
            pass_on(i + 1)

    pass_on(late + 1)

    @pl.loop(late - here, late)
    def _(i):
        arrived(i + 2)
        late_multiply(i)

    z_copy = remote(z.at[yn], zr, z_s, z_r, yn_dev)
    z_copy.start()
    o_copy(yn, yi).wait_send()
    for e in range(2):
        to_xn(e, xi).wait_send()
        to_sib(e, xi).wait_send()
        forward(e, xn).wait_send()

    @pl.loop(2, late + 2)
    def _(e):
        to_xn(e, xi).wait_send()
        to_sib(e, xi).wait_send()
        forward(e, xn).wait_send()

    @pl.loop(here, late)
    def _(i):
        x_send(i).wait_send()

    z_copy.wait()
    y_ref[...] = (x_ref[...].astype(F32) + (z[yi] + zr[...])).astype(BF16)


def back(x_loc, o_halves, a1, own, perm, send, wao, wmo):
    rows, width = x_loc.shape
    num_o, num_c = wao.shape[0] // C, wmo.shape[0] // C
    num_k, late, groups = num_o + num_c, num_c - N1, 2 + num_c - N1
    quarter = rows // 4
    dma = pltpu.SemaphoreType.DMA
    any_spec = pl.BlockSpec(memory_space=pl.ANY)
    vmem_spec = pl.BlockSpec(memory_space=pltpu.VMEM)
    return pl.pallas_call(
        back_kernel,
        name="back",
        out_shape=jax.ShapeDtypeStruct((rows, width), BF16),
        in_specs=[vmem_spec] * 3 + [any_spec] * 5,
        out_specs=vmem_spec,
        scratch_shapes=[
            pltpu.VMEM((num_k, C, 2 * width), BF16),
            pltpu.VMEM((late, quarter, 2 * C), F32),
            pltpu.VMEM((late, quarter, 2 * C), F32),
            pltpu.VMEM((8, rows // 8, num_k * C), BF16),
            pltpu.VMEM((2, rows, width), F32),
            pltpu.VMEM((rows, width), F32),
            dma((num_k,)), dma((late,)), dma((num_c - N2,)), dma((late,)), dma, dma,
            dma((groups,)), dma((groups,)), dma((groups,)), dma((groups,)), dma((groups,)), dma((groups,)), dma, dma,
        ],
        compiler_params=pltpu.CompilerParams(collective_id=1, has_side_effects=True, vmem_limit_bytes=VMEM_LIMIT),
        cost_estimate=pl.CostEstimate(
            flops=4 * rows * num_k * C * width, bytes_accessed=4 * num_k * C * width, transcendentals=0
        ),
    )(x_loc, o_halves, a1, own, perm, send, wao, wmo)


def solution(mesh):
    x_size, yz_size = mesh.shape["x"], mesh.shape["yz"]
    both_axes = ("x", "yz")
    row_spec = P("dp", both_axes)
    in_w_spec = P("x", "yz")
    out_w_spec = P("yz", "x")
    cache_spec = P(("dp", "x", "yz"), None, None)
    len_spec = P(("dp", "x", "yz"))
    across = [(i, (i + 2) % 4) for i in range(4)]

    def local_layer(x_loc, gain_loc, wqkv_loc, wgate_loc, wup_loc, wao_loc, wmo_loc, kc_loc, vc_loc, len_loc):
        d_model = x_loc.shape[1] * x_size * yz_size
        reqs, _, head_dim = kc_loc.shape
        half = head_dim // 2
        inv_freq = 10000.0 ** (-jnp.arange(half, dtype=F32) / half)
        angles = len_loc.astype(F32)[:, None] * inv_freq
        cos, sin = jnp.cos(angles), jnp.sin(angles)
        cos = jnp.concatenate([cos, cos], axis=1)[:, None, :]
        sin = jnp.concatenate([-sin, sin], axis=1)[:, None, :]

        qkv, a1, perm, send, own = front(
            x_loc, gain_loc, wqkv_loc, wgate_loc, wup_loc, d_model
        )
        perm = lax.ppermute(perm, "x", across)
        qkv = jnp.concatenate([qkv[0], qkv[1]], axis=1).reshape(reqs, -1, head_dim)
        k_all, v_all, attn = attend(qkv, cos, sin, kc_loc, vc_loc, len_loc)
        o_halves = jnp.swapaxes(attn.reshape(reqs, 2, -1), 0, 1)
        y_loc = back(x_loc, o_halves, a1, own, perm, send, wao_loc, wmo_loc)
        return y_loc, k_all, v_all

    in_specs = (row_spec, P(both_axes), in_w_spec, in_w_spec, in_w_spec, out_w_spec, out_w_spec, cache_spec, cache_spec, len_spec)
    out_specs = (row_spec, cache_spec, cache_spec)
    return jax.shard_map(local_layer, mesh=mesh, in_specs=in_specs, out_specs=out_specs, check_vma=False)
```

```python
import functools

import jax
import jax.numpy as jnp
from jax import lax
from jax.experimental import pallas as pl
from jax.experimental.pallas import tpu as pltpu
from jax.sharding import PartitionSpec as P

MESH = pl.DeviceIdType.MESH
F32 = jnp.float32
BF16 = jnp.bfloat16
VMEM_LIMIT = 66_900_000

C = 768
CQ = 640
SLOTS = 3
N1 = 4
N2 = 12
PIECE = 3


def remote(src, dst, send_sem, recv_sem, device):
    return pltpu.make_async_remote_copy(
        src_ref=src, dst_ref=dst, send_sem=send_sem, recv_sem=recv_sem, device_id=device, device_id_type=MESH
    )


def places():
    xi = lax.axis_index("x")
    yi = lax.axis_index("yz")
    sib = xi + 1 - 2 * (xi % 2)
    xn = (xi + 2) % 4
    return xi, yi, sib, xn, (sib + 2) % 4, 1 - yi


def activation(total):
    gate = total[:, :C].astype(BF16).astype(F32)
    up = total[:, C:].astype(BF16).astype(F32)
    return (jax.nn.silu(gate) * up).astype(BF16)


def front_kernel(
    d_model, x_ref, g_ref, wq_hbm, wg_hbm, wu_hbm,
    qkv_hbm, a_hbm, perm_hbm, send_hbm, own_hbm,
    stat, xbuf, gbuf, h, wq, wg, wu, pq, rq, xq, qs, qd, p, r, xr, a,
    wq_sem, wg_sem, wu_sem, st_s, st_r, xg_s, xg_r,
    dq_s, dq_r, xq_s, xq_r, yq_s, yq_r, d_s, d_r, x_s, x_r, out_sem, own_sem, q_sem, a_sem,
):
    xi, yi, sib, xn, sibn, yn = places()
    me = yi * 4 + xi
    rows, width = x_ref.shape
    num_q = wq_hbm.shape[1] // CQ
    num_c = wg_hbm.shape[1] // C
    sib_dev, xn_dev, yn_dev = {"x": sib}, {"x": xn}, {"yz": yn}

    def wq_copy(c):
        return pltpu.make_async_copy(wq_hbm.at[:, pl.ds(c * CQ, CQ)], wq.at[c], wq_sem.at[c])

    def w_copies(i, slot):
        start = pl.multiple_of(i * C, C)
        return (
            pltpu.make_async_copy(wg_hbm.at[:, pl.ds(start, C)], wg.at[slot], wg_sem.at[slot]),
            pltpu.make_async_copy(wu_hbm.at[:, pl.ds(start, C)], wu.at[slot], wu_sem.at[slot]),
        )

    for c in range(num_q):
        wq_copy(c).start()
    for i in range(SLOTS):
        for copy in w_copies(i, i):
            copy.start()

    barrier = pltpu.get_barrier_semaphore()
    offsets = [(dy, dx) for dy in range(2) for dx in range(4)][1:]
    for dy, dx in offsets:
        pl.semaphore_signal(barrier, inc=1, device_id={"yz": (yi + dy) % 2, "x": (xi + dx) % 4}, device_id_type=MESH)

    x_f32 = x_ref[...].astype(F32)
    lane = lax.broadcasted_iota(jnp.int32, (rows, rows), 1)
    sums = jnp.where(
        lane == 0,
        jnp.sum(x_f32, axis=1, keepdims=True),
        jnp.where(lane == 1, jnp.sum(x_f32 * x_f32, axis=1, keepdims=True), 0.0),
    )
    stat[me] = sums.T[0:8, :]
    gbuf[yi] = jnp.broadcast_to(g_ref[...].astype(F32)[None, :], (8, width))
    xbuf[yi] = x_ref[...]
    pl.semaphore_wait(barrier, 7)

    def stat_copy(k, slot):
        dy, dx = offsets[k]
        dev = {"yz": (yi + dy) % 2, "x": (xi + dx) % 4}
        return remote(stat.at[slot], stat.at[slot], st_s.at[k], st_r.at[k], dev)

    def x_copy(slot):
        return remote(x_ref, xbuf.at[slot], xg_s.at[0], xg_r.at[0], yn_dev)

    def g_copy(slot):
        return remote(gbuf.at[slot], gbuf.at[slot], xg_s.at[1], xg_r.at[1], yn_dev)

    for k in range(7):
        stat_copy(k, me).start()
    g_copy(yi).start()
    x_copy(yi).start()
    for k, (dy, dx) in enumerate(offsets):
        stat_copy(k, ((yi + 2 - dy) % 2) * 4 + (xi + 4 - dx) % 4).wait_recv()
    total = stat[0]
    for k in range(1, 8):
        total = total + stat[k]
    cols = jnp.concatenate([total, jnp.zeros((rows - 8, rows), F32)], axis=0).T
    mean = cols[:, 0:1] / d_model
    var = cols[:, 1:2] / d_model - mean * mean
    scale = lax.rsqrt(var + 1e-6)
    g_copy(yn).wait_recv()
    x_copy(yn).wait_recv()
    for b in range(2):
        part = (xbuf[b].astype(F32) - mean) * scale * gbuf[b][0:1, :]
        h[:, b * width:(b + 1) * width] = part.astype(BF16)

    def dq(c, k):
        src = sib if k == 0 else sibn
        return remote(pq.at[c, src], rq.at[c, k], dq_s.at[c, k], dq_r.at[c, k], sib_dev)

    def xq_copy(c):
        return remote(pq.at[c, xn], xq.at[c], xq_s.at[c], xq_r.at[c], xn_dev)

    def q_sum(c):
        dq(c, 1).wait_recv()
        dq(c, 1).wait_send()
        pq[c, xn] = pq[c, xn] + rq[c, 1]
        xq_copy(c).start()
        dq(c, 0).wait_recv()
        dq(c, 0).wait_send()
        pq[c, xi] = pq[c, xi] + rq[c, 0]

    @pl.loop(0, num_q)
    def _(c):
        wq_copy(c).wait()
        prod = jnp.dot(h[...], wq[c], preferred_element_type=F32)
        pq[c] = prod.reshape(4, rows // 4, CQ)
        dq(c, 1).start()
        dq(c, 0).start()

        @pl.when(c >= 1)
        def _():
            q_sum(c - 1)

    def d_copy(i, k):
        src = sib if k == 0 else sibn
        return remote(p.at[i, src], r.at[i, k], d_s.at[i, k], d_r.at[i, k], sib_dev)

    def x_send(i):
        return remote(p.at[i, xn], xr.at[i], x_s.at[i], x_r.at[i], xn_dev)

    def perm_copy(i):
        return pltpu.make_async_copy(p.at[i, xn], perm_hbm.at[i - N1], out_sem.at[i])

    def send_copy(i):
        return pltpu.make_async_copy(p.at[i, xn], send_hbm.at[i - N2], out_sem.at[i])

    def own_copy(i):
        return pltpu.make_async_copy(p.at[i, xi], own_hbm.at[i - N1], own_sem.at[i])

    def chip_sum(i):
        d_copy(i, 1).wait_recv()
        d_copy(i, 1).wait_send()
        p[i, xn] = p[i, xn] + r[i, 1]

        @pl.when(i < N1)
        def _():
            x_send(i).start()

        @pl.when((i >= N1) & (i < N2))
        def _():
            perm_copy(i).start()

        @pl.when(i >= N2)
        def _():
            send_copy(i).start()

        d_copy(i, 0).wait_recv()
        d_copy(i, 0).wait_send()
        p[i, xi] = p[i, xi] + r[i, 0]

        @pl.when(i >= N1)
        def _():
            own_copy(i).start()

    def product(i):
        slot = i % SLOTS
        g_w, u_w = w_copies(i, slot)
        g_w.wait()
        p[i, :, :, :C] = jnp.dot(h[...], wg[slot], preferred_element_type=F32).reshape(4, rows // 4, C)
        u_w.wait()
        p[i, :, :, C:] = jnp.dot(h[...], wu[slot], preferred_element_type=F32).reshape(4, rows // 4, C)
        d_copy(i, 1).start()
        d_copy(i, 0).start()

        @pl.when(i + SLOTS < num_c)
        def _():
            for copy in w_copies(i + SLOTS, slot):
                copy.start()

    product(0)
    q_sum(num_q - 1)

    def step(i):
        product(i)
        chip_sum(i - 1)

    half = num_c // 2 + 1
    pl.loop(1, half)(step)

    @pl.loop(0, num_q)
    def _(c):
        xq_copy(c).wait_recv()
        xq_copy(c).wait_send()
        value = (pq[c, xi] + xq[c]).astype(BF16)
        qs[:, :, pl.ds(pl.multiple_of(c * CQ, CQ), CQ)] = value.reshape(2, rows // 8, CQ)

    def yq_copy(k):
        return remote(qs.at[1 - k], qd.at[k], yq_s, yq_r, yn_dev)

    yq_copy(yi).start()
    qd[yi] = qs[yi]

    pl.loop(half, num_c)(step)
    chip_sum(num_c - 1)
    yq_copy(yn).wait_recv()
    q_out = pltpu.make_async_copy(qd, qkv_hbm, q_sem)
    q_out.start()

    @pl.loop(0, N1)
    def _(i):
        x_send(i).wait_recv()
        x_send(i).wait_send()
        act = activation(p[i, xi] + xr[i])
        a[:, :, pl.ds(pl.multiple_of(i * C, C), C)] = act.reshape(2, rows // 8, C)

    a_out = pltpu.make_async_copy(a, a_hbm, a_sem)
    a_out.start()
    for k in range(7):
        stat_copy(k, me).wait_send()
    g_copy(yi).wait_send()
    x_copy(yi).wait_send()
    yq_copy(yi).wait_send()

    @pl.loop(N1, N2)
    def _(i):
        perm_copy(i).wait()
        own_copy(i).wait()

    @pl.loop(N2, num_c)
    def _(i):
        send_copy(i).wait()
        own_copy(i).wait()

    q_out.wait()
    a_out.wait()


def front(x_loc, gain_loc, wqkv, wgate, wup, d_model):
    rows, width = x_loc.shape
    depth, q_cols = wqkv.shape
    num_q, num_c = q_cols // CQ, wgate.shape[1] // C
    quarter = rows // 4
    dma = pltpu.SemaphoreType.DMA
    any_spec = pl.BlockSpec(memory_space=pl.ANY)
    vmem_spec = pl.BlockSpec(memory_space=pltpu.VMEM)
    return pl.pallas_call(
        functools.partial(front_kernel, d_model),
        name="front",
        out_shape=(
            jax.ShapeDtypeStruct((2, rows // 8, q_cols), BF16),
            jax.ShapeDtypeStruct((2, rows // 8, N1 * C), BF16),
            jax.ShapeDtypeStruct((N2 - N1, quarter, 2 * C), F32),
            jax.ShapeDtypeStruct((num_c - N2, quarter, 2 * C), F32),
            jax.ShapeDtypeStruct((num_c - N1, quarter, 2 * C), F32),
        ),
        in_specs=[vmem_spec, vmem_spec, any_spec, any_spec, any_spec],
        out_specs=(any_spec,) * 5,
        scratch_shapes=[
            pltpu.VMEM((8, 8, rows), F32),
            pltpu.VMEM((2, rows, width), BF16),
            pltpu.VMEM((2, 8, width), F32),
            pltpu.VMEM((rows, depth), BF16),
            pltpu.VMEM((num_q, depth, CQ), BF16),
            pltpu.VMEM((SLOTS, depth, C), BF16),
            pltpu.VMEM((SLOTS, depth, C), BF16),
            pltpu.VMEM((num_q, 4, quarter, CQ), F32),
            pltpu.VMEM((num_q, 2, quarter, CQ), F32),
            pltpu.VMEM((num_q, quarter, CQ), F32),
            pltpu.VMEM((2, rows // 8, q_cols), BF16),
            pltpu.VMEM((2, rows // 8, q_cols), BF16),
            pltpu.VMEM((num_c, 4, quarter, 2 * C), F32),
            pltpu.VMEM((num_c, 2, quarter, 2 * C), F32),
            pltpu.VMEM((N1, quarter, 2 * C), F32),
            pltpu.VMEM((2, rows // 8, N1 * C), BF16),
            dma((num_q,)), dma((SLOTS,)), dma((SLOTS,)), dma((7,)), dma((7,)), dma((2,)), dma((2,)),
            dma((num_q, 2)), dma((num_q, 2)), dma((num_q,)), dma((num_q,)), dma, dma,
            dma((num_c, 2)), dma((num_c, 2)), dma((N1,)), dma((N1,)), dma((num_c,)), dma((num_c,)), dma, dma,
        ],
        compiler_params=pltpu.CompilerParams(collective_id=0, has_side_effects=True, vmem_limit_bytes=VMEM_LIMIT),
        cost_estimate=pl.CostEstimate(
            flops=2 * rows * depth * (q_cols + 2 * wgate.shape[1]),
            bytes_accessed=2 * depth * (q_cols + 2 * wgate.shape[1]),
            transcendentals=0,
        ),
    )(x_loc, gain_loc, wqkv, wgate, wup)


def attend_kernel(len_ref, qkv_ref, cos_ref, sin_ref, k_ref, v_ref, ko_ref, vo_ref, o_ref):
    pos = len_ref[pl.program_id(0)]
    qkv = qkv_ref[0]
    heads, head_dim = qkv.shape[0] - 2, qkv.shape[1]
    wide = qkv.astype(F32)
    turned = (wide * cos_ref[0] + pltpu.roll(wide, head_dim // 2, 1) * sin_ref[0]).astype(BF16)
    query = turned[:heads]
    ko_ref[...] = k_ref[...]
    vo_ref[...] = v_ref[...]
    base = pl.multiple_of((pos // 16) * 16, 16)
    here = lax.broadcasted_iota(jnp.int32, (16, head_dim), 0) == pos - base
    for out, new in ((ko_ref, turned[heads:heads + 1]), (vo_ref, qkv[heads + 1:heads + 2])):
        tile = out[0, pl.ds(base, 16), :].astype(F32)
        out[0, pl.ds(base, 16), :] = jnp.where(here, new.astype(F32), tile).astype(BF16)
    scores = lax.dot_general(query, ko_ref[0], (((1,), (1,)), ((), ())), preferred_element_type=F32)
    scores = scores * head_dim ** -0.5
    at = lax.broadcasted_iota(jnp.int32, scores.shape, 1)
    scores = jnp.where(at <= pos, scores, -1e30)
    weight = jnp.exp(scores - jnp.max(scores, axis=1, keepdims=True))
    probs = (weight / jnp.sum(weight, axis=1, keepdims=True)).astype(BF16)
    o_ref[0] = jnp.dot(probs, vo_ref[0], preferred_element_type=F32).astype(BF16)


def attend(qkv, cos, sin, k_cache, v_cache, ctx_len):
    reqs, length, head_dim = k_cache.shape
    heads = qkv.shape[1] - 2
    cache_spec = pl.BlockSpec((1, length, head_dim), lambda i, lens: (i, 0, 0))
    table_spec = pl.BlockSpec((1, 1, head_dim), lambda i, lens: (i, 0, 0))
    return pl.pallas_call(
        attend_kernel,
        name="attend",
        grid_spec=pltpu.PrefetchScalarGridSpec(
            num_scalar_prefetch=1,
            grid=(reqs,),
            in_specs=[
                pl.BlockSpec((1, heads + 2, head_dim), lambda i, lens: (i, 0, 0)),
                table_spec, table_spec, cache_spec, cache_spec,
            ],
            out_specs=[cache_spec, cache_spec, pl.BlockSpec((1, heads, head_dim), lambda i, lens: (i, 0, 0))],
        ),
        out_shape=(
            jax.ShapeDtypeStruct(k_cache.shape, BF16),
            jax.ShapeDtypeStruct(v_cache.shape, BF16),
            jax.ShapeDtypeStruct((reqs, heads, head_dim), BF16),
        ),
        compiler_params=pltpu.CompilerParams(dimension_semantics=("arbitrary",)),
        cost_estimate=pl.CostEstimate(
            flops=64 * reqs * heads * length * head_dim,
            bytes_accessed=8 * reqs * length * head_dim,
            transcendentals=reqs * heads * length,
        ),
    )(ctx_len, qkv, cos, sin, k_cache, v_cache)


def back_kernel(
    x_ref, o_ref, a1_ref, own_hbm, perm_hbm, send_hbm, wao_hbm, wmo_hbm, y_ref,
    w, own, xr, act, z, zr,
    w_sem, own_sem, x_s, x_r, o_s, o_r, sib_s, sib_r, xn_s, xn_r, fwd_s, fwd_r, z_s, z_r,
):
    xi, yi, sib, xn, _, yn = places()
    sib_dev, xn_dev, yn_dev = {"x": sib}, {"x": xn}, {"yz": yn}
    width = x_ref.shape[3]
    half_rows = act.shape[1] * act.shape[2]
    num_o, num_c = wao_hbm.shape[0] // C, wmo_hbm.shape[0] // C
    num_k = num_o + num_c
    o_cols = wao_hbm.shape[0]
    late = num_c - N1
    here = N2 - N1
    pieces = late // PIECE

    def w_copy(k):
        src = wao_hbm.at[pl.ds(k * C, C), :] if k < num_o else wmo_hbm.at[pl.ds((k - num_o) * C, C), :]
        return pltpu.make_async_copy(src, w.at[k], w_sem.at[k])

    def own_copy(i):
        return pltpu.make_async_copy(own_hbm.at[i], own.at[i], own_sem.at[i])

    def perm_copy(i):
        return pltpu.make_async_copy(perm_hbm.at[i], xr.at[i], x_r.at[i])

    def x_send(i):
        return remote(send_hbm.at[i - here], xr.at[i], x_s.at[i - here], x_r.at[i], xn_dev)

    barrier = pltpu.get_barrier_semaphore()
    for dev in (sib_dev, xn_dev, yn_dev):
        pl.semaphore_signal(barrier, inc=1, device_id=dev, device_id_type=MESH)
    for i in range(late):
        own_copy(i).start()
    for i in range(here):
        perm_copy(i).start()
    for k in range(num_k):
        w_copy(k).start()
    act[yi, xi, :, :o_cols] = o_ref[yi]
    act[:, xi, :, o_cols:o_cols + N1 * C] = a1_ref[...]
    pl.semaphore_wait(barrier, 3)

    def o_copy(half, row):
        return remote(o_ref.at[half], act.at[row, xi, :, 0:o_cols], o_s, o_r, yn_dev)

    def block_of(e, owner):
        if e == 0:
            return act.at[:, owner, :, pl.ds(o_cols, N1 * C)]
        if e == 1:
            return act.at[:, owner, :, pl.ds(0, o_cols)]
        half, n = divmod(e - 2, pieces)
        return act.at[half, owner, :, pl.ds(o_cols + (N1 + n * PIECE) * C, PIECE * C)]

    def to_sib(e, owner):
        block = block_of(e, owner)
        return remote(block, block, sib_s.at[e], sib_r.at[e], sib_dev)

    def to_xn(e, owner):
        block = block_of(e, owner)
        return remote(block, block, xn_s.at[e], xn_r.at[e], xn_dev)

    def forward(e, owner):
        block = block_of(e, owner)
        return remote(block, block, fwd_s.at[e], fwd_r.at[e], sib_dev)

    def send_own(e):
        to_xn(e, xi).start()
        to_sib(e, xi).start()

    def pass_on(e):
        to_xn(e, xn).wait_recv()
        forward(e, xn).start()

    def arrived(e):
        to_sib(e, sib).wait_recv()
        forward(e, (sib + 2) % 4).wait_recv()

    def activate(i):
        own_copy(i).wait()
        value = activation(own[i] + xr[i])
        start = pl.multiple_of(o_cols + (N1 + i) * C, C)
        act[:, xi, :, pl.ds(start, C)] = value.reshape(2, value.shape[0] // 2, C)

    def w_wait(k):
        pltpu.make_async_copy(wmo_hbm.at[pl.ds(0, C), :], w.at[k], w_sem.at[k]).wait()

    def multiply(first, count):
        @pl.loop(first, first + count)
        def _(k):
            w_wait(k)
            lhs = act[:, :, :, pl.ds(pl.multiple_of(k * C, C), C)].reshape(2 * half_rows, C)
            for b in range(2):
                prod = jnp.dot(lhs, w[k, :, b * width:(b + 1) * width], preferred_element_type=F32)
                z[b] = z[b] + prod.reshape(2, half_rows, width)

    def multiply_half(half, n):
        @pl.loop(num_o + N1 + n * PIECE, num_o + N1 + (n + 1) * PIECE)
        def _(k):
            if half == 0:
                w_wait(k)
            lhs = act[half, :, :, pl.ds(pl.multiple_of(k * C, C), C)].reshape(half_rows, C)
            for b in range(2):
                prod = jnp.dot(lhs, w[k, :, b * width:(b + 1) * width], preferred_element_type=F32)
                z[b, half] = z[b, half] + prod

    first = (late - here) // 2
    for i in range(here, here + first):
        x_send(i).start()
    o_copy(yn, yi).start()
    z[...] = jnp.zeros_like(z)

    @pl.loop(0, here)
    def _(i):
        perm_copy(i).wait()
        activate(i)

    o_copy(yi, yn).wait_recv()
    send_own(1)
    send_own(0)
    for i in range(here + first, late):
        x_send(i).start()
    ready = here // PIECE
    for n in range(ready):
        send_own(2 + n)

    @pl.loop(here, here + first)
    def _(i):
        x_send(i).wait_recv()
        activate(i)

    pass_on(1)
    pass_on(0)
    arrived(1)
    multiply(0, num_o)
    arrived(0)
    multiply(num_o, N1)

    @pl.loop(here + first, late)
    def _(i):
        x_send(i).wait_recv()
        activate(i)

    groups = 2 + 2 * pieces
    for e in range(2 + ready, groups):
        send_own(e)
    z_copies = [remote(z.at[yn, half], zr.at[half], z_s.at[half], z_r.at[half], yn_dev) for half in range(2)]
    pass_on(2)
    for e in range(2, groups):
        if e + 1 < groups:
            pass_on(e + 1)
        arrived(e)
        half, n = divmod(e - 2, pieces)
        multiply_half(half, n)
        if n == pieces - 1:
            z_copies[half].start()

    o_copy(yn, yi).wait_send()
    for e in range(groups):
        to_xn(e, xi).wait_send()
        to_sib(e, xi).wait_send()
        forward(e, xn).wait_send()

    @pl.loop(here, late)
    def _(i):
        x_send(i).wait_send()

    for half in range(2):
        z_copies[half].wait()
        total = (z[yi, half] + zr[half]).reshape(act.shape[1], act.shape[2], width)
        y_ref[:, half] = (x_ref[:, half].astype(F32) + total).astype(BF16)


def back(x_loc, o_halves, a1, own, perm, send, wao, wmo):
    rows, width = x_loc.shape
    num_o, num_c = wao.shape[0] // C, wmo.shape[0] // C
    num_k, late = num_o + num_c, num_c - N1
    groups = 2 + 2 * (late // PIECE)
    quarter = rows // 4
    dma = pltpu.SemaphoreType.DMA
    any_spec = pl.BlockSpec(memory_space=pl.ANY)
    vmem_spec = pl.BlockSpec(memory_space=pltpu.VMEM)
    y = pl.pallas_call(
        back_kernel,
        name="back",
        out_shape=jax.ShapeDtypeStruct((4, 2, rows // 8, width), BF16),
        in_specs=[vmem_spec] * 3 + [any_spec] * 5,
        out_specs=vmem_spec,
        scratch_shapes=[
            pltpu.VMEM((num_k, C, 2 * width), BF16),
            pltpu.VMEM((late, quarter, 2 * C), F32),
            pltpu.VMEM((late, quarter, 2 * C), F32),
            pltpu.VMEM((2, 4, rows // 8, num_k * C), BF16),
            pltpu.VMEM((2, 2, rows // 2, width), F32),
            pltpu.VMEM((2, rows // 2, width), F32),
            dma((num_k,)), dma((late,)), dma((num_c - N2,)), dma((late,)), dma, dma,
            dma((groups,)), dma((groups,)), dma((groups,)), dma((groups,)), dma((groups,)), dma((groups,)),
            dma((2,)), dma((2,)),
        ],
        compiler_params=pltpu.CompilerParams(collective_id=1, has_side_effects=True, vmem_limit_bytes=VMEM_LIMIT),
        cost_estimate=pl.CostEstimate(
            flops=4 * rows * num_k * C * width, bytes_accessed=4 * num_k * C * width, transcendentals=0
        ),
    )(x_loc.reshape(4, 2, rows // 8, width), o_halves, a1, own, perm, send, wao, wmo)
    return y.reshape(rows, width)


def solution(mesh):
    x_size, yz_size = mesh.shape["x"], mesh.shape["yz"]
    both_axes = ("x", "yz")
    row_spec = P("dp", both_axes)
    in_w_spec = P("x", "yz")
    out_w_spec = P("yz", "x")
    cache_spec = P(("dp", "x", "yz"), None, None)
    len_spec = P(("dp", "x", "yz"))
    across = [(i, (i + 2) % 4) for i in range(4)]

    def local_layer(x_loc, gain_loc, wqkv_loc, wgate_loc, wup_loc, wao_loc, wmo_loc, kc_loc, vc_loc, len_loc):
        d_model = x_loc.shape[1] * x_size * yz_size
        reqs, _, head_dim = kc_loc.shape
        half = head_dim // 2
        inv_freq = 10000.0 ** (-jnp.arange(half, dtype=F32) / half)
        angles = len_loc.astype(F32)[:, None] * inv_freq
        cos, sin = jnp.cos(angles), jnp.sin(angles)
        cos = jnp.concatenate([cos, cos], axis=1)[:, None, :]
        sin = jnp.concatenate([-sin, sin], axis=1)[:, None, :]

        qkv, a1, perm, send, own = front(
            x_loc, gain_loc, wqkv_loc, wgate_loc, wup_loc, d_model
        )
        perm = lax.ppermute(perm, "x", across)
        qkv = jnp.concatenate([qkv[0], qkv[1]], axis=1).reshape(reqs, -1, head_dim)
        k_all, v_all, attn = attend(qkv, cos, sin, kc_loc, vc_loc, len_loc)
        o_halves = jnp.swapaxes(attn.reshape(reqs, 2, -1), 0, 1)
        y_loc = back(x_loc, o_halves, a1, own, perm, send, wao_loc, wmo_loc)
        return y_loc, k_all, v_all

    in_specs = (row_spec, P(both_axes), in_w_spec, in_w_spec, in_w_spec, out_w_spec, out_w_spec, cache_spec, cache_spec, len_spec)
    out_specs = (row_spec, cache_spec, cache_spec)
    return jax.shard_map(local_layer, mesh=mesh, in_specs=in_specs, out_specs=out_specs, check_vma=False)
```

```python
import functools

import jax
import jax.numpy as jnp
from jax import lax
from jax.experimental import pallas as pl
from jax.experimental.pallas import tpu as pltpu
from jax.sharding import PartitionSpec as P

MESH = pl.DeviceIdType.MESH
F32 = jnp.float32
BF16 = jnp.bfloat16
VMEM_LIMIT = 66_900_000

C = 768
CQ = 640
SLOTS = 3
N1 = 4
N2 = 12
PIECE = 3


def remote(src, dst, send_sem, recv_sem, device):
    return pltpu.make_async_remote_copy(
        src_ref=src, dst_ref=dst, send_sem=send_sem, recv_sem=recv_sem, device_id=device, device_id_type=MESH
    )


def places():
    xi = lax.axis_index("x")
    yi = lax.axis_index("yz")
    sib = xi + 1 - 2 * (xi % 2)
    xn = (xi + 2) % 4
    return xi, yi, sib, xn, (sib + 2) % 4, 1 - yi


def activation(total):
    gate = total[:, :C].astype(BF16).astype(F32)
    up = total[:, C:].astype(BF16).astype(F32)
    return (jax.nn.silu(gate) * up).astype(BF16)


def front_kernel(
    d_model, x_ref, g_ref, wq_hbm, wg_hbm, wu_hbm,
    qkv_hbm, a_hbm, perm_hbm, send_hbm, own_hbm,
    stat, xbuf, gbuf, h, wq, wg, wu, pq, rq, xq, qs, qd, p, r, xr, a,
    wq_sem, wg_sem, wu_sem, st_s, st_r, xg_s, xg_r,
    dq_s, dq_r, xq_s, xq_r, yq_s, yq_r, d_s, d_r, x_s, x_r, out_sem, own_sem, q_sem, a_sem,
):
    xi, yi, sib, xn, sibn, yn = places()
    me = yi * 4 + xi
    rows, width = x_ref.shape
    num_q = wq_hbm.shape[1] // CQ
    num_c = wg_hbm.shape[1] // C
    sib_dev, xn_dev, yn_dev = {"x": sib}, {"x": xn}, {"yz": yn}

    def wq_copy(c):
        return pltpu.make_async_copy(wq_hbm.at[:, pl.ds(c * CQ, CQ)], wq.at[c], wq_sem.at[c])

    def w_copies(i, slot):
        start = pl.multiple_of(i * C, C)
        return (
            pltpu.make_async_copy(wg_hbm.at[:, pl.ds(start, C)], wg.at[slot], wg_sem.at[slot]),
            pltpu.make_async_copy(wu_hbm.at[:, pl.ds(start, C)], wu.at[slot], wu_sem.at[slot]),
        )

    barrier = pltpu.get_barrier_semaphore()
    offsets = [(dy, dx) for dy in range(2) for dx in range(4)][1:]
    for dy, dx in offsets:
        pl.semaphore_signal(barrier, inc=1, device_id={"yz": (yi + dy) % 2, "x": (xi + dx) % 4}, device_id_type=MESH)

    x_f32 = x_ref[...].astype(F32)
    lane = lax.broadcasted_iota(jnp.int32, (rows, rows), 1)
    sums = jnp.where(
        lane == 0,
        jnp.sum(x_f32, axis=1, keepdims=True),
        jnp.where(lane == 1, jnp.sum(x_f32 * x_f32, axis=1, keepdims=True), 0.0),
    )
    stat[me] = sums.T[0:8, :]
    gbuf[yi] = jnp.broadcast_to(g_ref[...].astype(F32)[None, :], (8, width))
    xbuf[yi] = x_ref[...]
    pl.semaphore_wait(barrier, 7)

    def stat_copy(k, slot):
        dy, dx = offsets[k]
        dev = {"yz": (yi + dy) % 2, "x": (xi + dx) % 4}
        return remote(stat.at[slot], stat.at[slot], st_s.at[k], st_r.at[k], dev)

    def x_copy(slot):
        return remote(x_ref, xbuf.at[slot], xg_s.at[0], xg_r.at[0], yn_dev)

    def g_copy(slot):
        return remote(gbuf.at[slot], gbuf.at[slot], xg_s.at[1], xg_r.at[1], yn_dev)

    for k in range(7):
        stat_copy(k, me).start()
    g_copy(yi).start()
    x_copy(yi).start()
    for c in range(num_q):
        wq_copy(c).start()
    for i in range(SLOTS):
        for copy in w_copies(i, i):
            copy.start()
    for k, (dy, dx) in enumerate(offsets):
        stat_copy(k, ((yi + 2 - dy) % 2) * 4 + (xi + 4 - dx) % 4).wait_recv()
    total = stat[0]
    for k in range(1, 8):
        total = total + stat[k]
    cols = jnp.concatenate([total, jnp.zeros((rows - 8, rows), F32)], axis=0).T
    mean = cols[:, 0:1] / d_model
    var = cols[:, 1:2] / d_model - mean * mean
    scale = lax.rsqrt(var + 1e-6)
    g_copy(yn).wait_recv()
    x_copy(yn).wait_recv()
    for b in range(2):
        part = (xbuf[b].astype(F32) - mean) * scale * gbuf[b][0:1, :]
        h[:, b * width:(b + 1) * width] = part.astype(BF16)

    def dq(c, k):
        src = sib if k == 0 else sibn
        return remote(pq.at[c, src], rq.at[c, k], dq_s.at[c, k], dq_r.at[c, k], sib_dev)

    def xq_copy(c):
        return remote(pq.at[c, xn], xq.at[c], xq_s.at[c], xq_r.at[c], xn_dev)

    def q_sum(c):
        dq(c, 1).wait_recv()
        dq(c, 1).wait_send()
        pq[c, xn] = pq[c, xn] + rq[c, 1]
        xq_copy(c).start()
        dq(c, 0).wait_recv()
        dq(c, 0).wait_send()
        pq[c, xi] = pq[c, xi] + rq[c, 0]

    @pl.loop(0, num_q)
    def _(c):
        wq_copy(c).wait()
        prod = jnp.dot(h[...], wq[c], preferred_element_type=F32)
        pq[c] = prod.reshape(4, rows // 4, CQ)
        dq(c, 1).start()
        dq(c, 0).start()

        @pl.when(c >= 1)
        def _():
            q_sum(c - 1)

    def d_copy(i, k):
        src = sib if k == 0 else sibn
        return remote(p.at[i, src], r.at[i, k], d_s.at[i, k], d_r.at[i, k], sib_dev)

    def x_send(i):
        return remote(p.at[i, xn], xr.at[i], x_s.at[i], x_r.at[i], xn_dev)

    def perm_copy(i):
        return pltpu.make_async_copy(p.at[i, xn], perm_hbm.at[i - N1], out_sem.at[i])

    def send_copy(i):
        return pltpu.make_async_copy(p.at[i, xn], send_hbm.at[i - N2], out_sem.at[i])

    def own_copy(i):
        return pltpu.make_async_copy(p.at[i, xi], own_hbm.at[i - N1], own_sem.at[i])

    def chip_sum(i):
        d_copy(i, 1).wait_recv()
        d_copy(i, 1).wait_send()
        p[i, xn] = p[i, xn] + r[i, 1]

        @pl.when(i < N1)
        def _():
            x_send(i).start()

        @pl.when((i >= N1) & (i < N2))
        def _():
            perm_copy(i).start()

        @pl.when(i >= N2)
        def _():
            send_copy(i).start()

        d_copy(i, 0).wait_recv()
        d_copy(i, 0).wait_send()
        p[i, xi] = p[i, xi] + r[i, 0]

        @pl.when(i >= N1)
        def _():
            own_copy(i).start()

    def product(i):
        slot = i % SLOTS
        g_w, u_w = w_copies(i, slot)
        g_w.wait()
        p[i, :, :, :C] = jnp.dot(h[...], wg[slot], preferred_element_type=F32).reshape(4, rows // 4, C)
        u_w.wait()
        p[i, :, :, C:] = jnp.dot(h[...], wu[slot], preferred_element_type=F32).reshape(4, rows // 4, C)
        d_copy(i, 1).start()
        d_copy(i, 0).start()

        @pl.when(i + SLOTS < num_c)
        def _():
            for copy in w_copies(i + SLOTS, slot):
                copy.start()

    product(0)
    q_sum(num_q - 1)

    def step(i):
        product(i)
        chip_sum(i - 1)

    half = num_c // 2 + 1
    pl.loop(1, half)(step)

    @pl.loop(0, num_q)
    def _(c):
        xq_copy(c).wait_recv()
        xq_copy(c).wait_send()
        value = (pq[c, xi] + xq[c]).astype(BF16)
        qs[:, :, pl.ds(pl.multiple_of(c * CQ, CQ), CQ)] = value.reshape(2, rows // 8, CQ)

    def yq_copy(k):
        return remote(qs.at[1 - k], qd.at[k], yq_s, yq_r, yn_dev)

    yq_copy(yi).start()
    qd[yi] = qs[yi]

    pl.loop(half, num_c)(step)
    chip_sum(num_c - 1)
    yq_copy(yn).wait_recv()
    q_out = pltpu.make_async_copy(qd, qkv_hbm, q_sem)
    q_out.start()

    @pl.loop(0, N1)
    def _(i):
        x_send(i).wait_recv()
        x_send(i).wait_send()
        act = activation(p[i, xi] + xr[i])
        a[:, :, pl.ds(pl.multiple_of(i * C, C), C)] = act.reshape(2, rows // 8, C)

    a_out = pltpu.make_async_copy(a, a_hbm, a_sem)
    a_out.start()
    for k in range(7):
        stat_copy(k, me).wait_send()
    g_copy(yi).wait_send()
    x_copy(yi).wait_send()
    yq_copy(yi).wait_send()

    @pl.loop(N1, N2)
    def _(i):
        perm_copy(i).wait()
        own_copy(i).wait()

    @pl.loop(N2, num_c)
    def _(i):
        send_copy(i).wait()
        own_copy(i).wait()

    q_out.wait()
    a_out.wait()


def front(x_loc, gain_loc, wqkv, wgate, wup, d_model):
    rows, width = x_loc.shape
    depth, q_cols = wqkv.shape
    num_q, num_c = q_cols // CQ, wgate.shape[1] // C
    quarter = rows // 4
    dma = pltpu.SemaphoreType.DMA
    any_spec = pl.BlockSpec(memory_space=pl.ANY)
    vmem_spec = pl.BlockSpec(memory_space=pltpu.VMEM)
    return pl.pallas_call(
        functools.partial(front_kernel, d_model),
        name="front",
        out_shape=(
            jax.ShapeDtypeStruct((2, rows // 8, q_cols), BF16),
            jax.ShapeDtypeStruct((2, rows // 8, N1 * C), BF16),
            jax.ShapeDtypeStruct((N2 - N1, quarter, 2 * C), F32),
            jax.ShapeDtypeStruct((num_c - N2, quarter, 2 * C), F32),
            jax.ShapeDtypeStruct((num_c - N1, quarter, 2 * C), F32),
        ),
        in_specs=[vmem_spec, vmem_spec, any_spec, any_spec, any_spec],
        out_specs=(any_spec,) * 5,
        scratch_shapes=[
            pltpu.VMEM((8, 8, rows), F32),
            pltpu.VMEM((2, rows, width), BF16),
            pltpu.VMEM((2, 8, width), F32),
            pltpu.VMEM((rows, depth), BF16),
            pltpu.VMEM((num_q, depth, CQ), BF16),
            pltpu.VMEM((SLOTS, depth, C), BF16),
            pltpu.VMEM((SLOTS, depth, C), BF16),
            pltpu.VMEM((num_q, 4, quarter, CQ), F32),
            pltpu.VMEM((num_q, 2, quarter, CQ), F32),
            pltpu.VMEM((num_q, quarter, CQ), F32),
            pltpu.VMEM((2, rows // 8, q_cols), BF16),
            pltpu.VMEM((2, rows // 8, q_cols), BF16),
            pltpu.VMEM((num_c, 4, quarter, 2 * C), F32),
            pltpu.VMEM((num_c, 2, quarter, 2 * C), F32),
            pltpu.VMEM((N1, quarter, 2 * C), F32),
            pltpu.VMEM((2, rows // 8, N1 * C), BF16),
            dma((num_q,)), dma((SLOTS,)), dma((SLOTS,)), dma((7,)), dma((7,)), dma((2,)), dma((2,)),
            dma((num_q, 2)), dma((num_q, 2)), dma((num_q,)), dma((num_q,)), dma, dma,
            dma((num_c, 2)), dma((num_c, 2)), dma((N1,)), dma((N1,)), dma((num_c,)), dma((num_c,)), dma, dma,
        ],
        compiler_params=pltpu.CompilerParams(collective_id=0, has_side_effects=True, vmem_limit_bytes=VMEM_LIMIT),
        cost_estimate=pl.CostEstimate(
            flops=2 * rows * depth * (q_cols + 2 * wgate.shape[1]),
            bytes_accessed=2 * depth * (q_cols + 2 * wgate.shape[1]),
            transcendentals=0,
        ),
    )(x_loc, gain_loc, wqkv, wgate, wup)


def attend_kernel(len_ref, qkv_ref, cos_ref, sin_ref, k_ref, v_ref, ko_ref, vo_ref, o_ref):
    pos = len_ref[pl.program_id(0)]
    qkv = qkv_ref[0]
    heads, head_dim = qkv.shape[0] - 2, qkv.shape[1]
    wide = qkv.astype(F32)
    turned = (wide * cos_ref[0] + pltpu.roll(wide, head_dim // 2, 1) * sin_ref[0]).astype(BF16)
    query = turned[:heads]
    ko_ref[...] = k_ref[...]
    vo_ref[...] = v_ref[...]
    base = pl.multiple_of((pos // 16) * 16, 16)
    here = lax.broadcasted_iota(jnp.int32, (16, head_dim), 0) == pos - base
    for out, new in ((ko_ref, turned[heads:heads + 1]), (vo_ref, qkv[heads + 1:heads + 2])):
        tile = out[0, pl.ds(base, 16), :].astype(F32)
        out[0, pl.ds(base, 16), :] = jnp.where(here, new.astype(F32), tile).astype(BF16)
    scores = lax.dot_general(query, ko_ref[0], (((1,), (1,)), ((), ())), preferred_element_type=F32)
    scores = scores * head_dim ** -0.5
    at = lax.broadcasted_iota(jnp.int32, scores.shape, 1)
    scores = jnp.where(at <= pos, scores, -1e30)
    weight = jnp.exp(scores - jnp.max(scores, axis=1, keepdims=True))
    probs = (weight / jnp.sum(weight, axis=1, keepdims=True)).astype(BF16)
    o_ref[0] = jnp.dot(probs, vo_ref[0], preferred_element_type=F32).astype(BF16)


def attend(qkv, cos, sin, k_cache, v_cache, ctx_len):
    reqs, length, head_dim = k_cache.shape
    heads = qkv.shape[1] - 2
    cache_spec = pl.BlockSpec((1, length, head_dim), lambda i, lens: (i, 0, 0))
    table_spec = pl.BlockSpec((1, 1, head_dim), lambda i, lens: (i, 0, 0))
    return pl.pallas_call(
        attend_kernel,
        name="attend",
        grid_spec=pltpu.PrefetchScalarGridSpec(
            num_scalar_prefetch=1,
            grid=(reqs,),
            in_specs=[
                pl.BlockSpec((1, heads + 2, head_dim), lambda i, lens: (i, 0, 0)),
                table_spec, table_spec, cache_spec, cache_spec,
            ],
            out_specs=[cache_spec, cache_spec, pl.BlockSpec((1, heads, head_dim), lambda i, lens: (i, 0, 0))],
        ),
        out_shape=(
            jax.ShapeDtypeStruct(k_cache.shape, BF16),
            jax.ShapeDtypeStruct(v_cache.shape, BF16),
            jax.ShapeDtypeStruct((reqs, heads, head_dim), BF16),
        ),
        compiler_params=pltpu.CompilerParams(dimension_semantics=("arbitrary",)),
        cost_estimate=pl.CostEstimate(
            flops=64 * reqs * heads * length * head_dim,
            bytes_accessed=8 * reqs * length * head_dim,
            transcendentals=reqs * heads * length,
        ),
    )(ctx_len, qkv, cos, sin, k_cache, v_cache)


def back_kernel(
    x_ref, o_ref, a1_ref, own_hbm, perm_hbm, send_hbm, wao_hbm, wmo_hbm, y_ref,
    w, own, xr, act, z, zr,
    w_sem, own_sem, x_s, x_r, o_s, o_r, sib_s, sib_r, xn_s, xn_r, fwd_s, fwd_r, z_s, z_r,
):
    xi, yi, sib, xn, _, yn = places()
    sib_dev, xn_dev, yn_dev = {"x": sib}, {"x": xn}, {"yz": yn}
    width = x_ref.shape[3]
    half_rows = act.shape[1] * act.shape[2]
    num_o, num_c = wao_hbm.shape[0] // C, wmo_hbm.shape[0] // C
    num_k = num_o + num_c
    o_cols = wao_hbm.shape[0]
    late = num_c - N1
    here = N2 - N1
    pieces = late // PIECE

    def w_copy(k):
        src = wao_hbm.at[pl.ds(k * C, C), :] if k < num_o else wmo_hbm.at[pl.ds((k - num_o) * C, C), :]
        return pltpu.make_async_copy(src, w.at[k], w_sem.at[k])

    def own_copy(i):
        return pltpu.make_async_copy(own_hbm.at[i], own.at[i], own_sem.at[i])

    def perm_copy(i):
        return pltpu.make_async_copy(perm_hbm.at[i], xr.at[i], x_r.at[i])

    def x_send(i):
        return remote(send_hbm.at[i - here], xr.at[i], x_s.at[i - here], x_r.at[i], xn_dev)

    barrier = pltpu.get_barrier_semaphore()
    for dev in (sib_dev, xn_dev, yn_dev):
        pl.semaphore_signal(barrier, inc=1, device_id=dev, device_id_type=MESH)
    for i in range(late):
        own_copy(i).start()
    for i in range(here):
        perm_copy(i).start()
    act[yi, xi, :, :o_cols] = o_ref[yi]
    act[:, xi, :, o_cols:o_cols + N1 * C] = a1_ref[...]
    pl.semaphore_wait(barrier, 3)

    def o_copy(half, row):
        return remote(o_ref.at[half], act.at[row, xi, :, 0:o_cols], o_s, o_r, yn_dev)

    def block_of(e, owner):
        if e == 0:
            return act.at[:, owner, :, pl.ds(o_cols, N1 * C)]
        if e == 1:
            return act.at[:, owner, :, pl.ds(0, o_cols)]
        half, n = divmod(e - 2, pieces)
        return act.at[half, owner, :, pl.ds(o_cols + (N1 + n * PIECE) * C, PIECE * C)]

    def to_sib(e, owner):
        block = block_of(e, owner)
        return remote(block, block, sib_s.at[e], sib_r.at[e], sib_dev)

    def to_xn(e, owner):
        block = block_of(e, owner)
        return remote(block, block, xn_s.at[e], xn_r.at[e], xn_dev)

    def forward(e, owner):
        block = block_of(e, owner)
        return remote(block, block, fwd_s.at[e], fwd_r.at[e], sib_dev)

    def send_own(e):
        to_xn(e, xi).start()
        to_sib(e, xi).start()

    def pass_on(e):
        to_xn(e, xn).wait_recv()
        forward(e, xn).start()

    def arrived(e):
        to_sib(e, sib).wait_recv()
        forward(e, (sib + 2) % 4).wait_recv()

    def activate(i):
        own_copy(i).wait()
        value = activation(own[i] + xr[i])
        start = pl.multiple_of(o_cols + (N1 + i) * C, C)
        act[:, xi, :, pl.ds(start, C)] = value.reshape(2, value.shape[0] // 2, C)

    def w_wait(k):
        pltpu.make_async_copy(wmo_hbm.at[pl.ds(0, C), :], w.at[k], w_sem.at[k]).wait()

    def multiply(first, count):
        @pl.loop(first, first + count)
        def _(k):
            w_wait(k)
            lhs = act[:, :, :, pl.ds(pl.multiple_of(k * C, C), C)].reshape(2 * half_rows, C)
            for b in range(2):
                prod = jnp.dot(lhs, w[k, :, b * width:(b + 1) * width], preferred_element_type=F32)
                z[b] = z[b] + prod.reshape(2, half_rows, width)

    def multiply_half(half, n):
        @pl.loop(num_o + N1 + n * PIECE, num_o + N1 + (n + 1) * PIECE)
        def _(k):
            if half == 0:
                w_wait(k)
            lhs = act[half, :, :, pl.ds(pl.multiple_of(k * C, C), C)].reshape(half_rows, C)
            for b in range(2):
                prod = jnp.dot(lhs, w[k, :, b * width:(b + 1) * width], preferred_element_type=F32)
                z[b, half] = z[b, half] + prod

    first = (late - here) // 2
    for i in range(here, here + first):
        x_send(i).start()
    o_copy(yn, yi).start()
    for k in range(num_k):
        w_copy(k).start()
    z[...] = jnp.zeros_like(z)

    @pl.loop(0, here)
    def _(i):
        perm_copy(i).wait()
        activate(i)

    o_copy(yi, yn).wait_recv()
    send_own(1)
    send_own(0)
    for i in range(here + first, late):
        x_send(i).start()
    ready = here // PIECE
    for n in range(ready):
        send_own(2 + n)

    @pl.loop(here, here + first)
    def _(i):
        x_send(i).wait_recv()
        activate(i)

    pass_on(1)
    pass_on(0)
    arrived(1)
    multiply(0, num_o)
    arrived(0)
    multiply(num_o, N1)

    @pl.loop(here + first, late)
    def _(i):
        x_send(i).wait_recv()
        activate(i)

    groups = 2 + 2 * pieces
    for e in range(2 + ready, groups):
        send_own(e)
    z_copies = [remote(z.at[yn, half], zr.at[half], z_s.at[half], z_r.at[half], yn_dev) for half in range(2)]
    pass_on(2)
    for e in range(2, groups):
        if e + 1 < groups:
            pass_on(e + 1)
        arrived(e)
        half, n = divmod(e - 2, pieces)
        multiply_half(half, n)
        if n == pieces - 1:
            z_copies[half].start()

    o_copy(yn, yi).wait_send()
    for e in range(groups):
        to_xn(e, xi).wait_send()
        to_sib(e, xi).wait_send()
        forward(e, xn).wait_send()

    @pl.loop(here, late)
    def _(i):
        x_send(i).wait_send()

    for half in range(2):
        z_copies[half].wait()
        total = (z[yi, half] + zr[half]).reshape(act.shape[1], act.shape[2], width)
        y_ref[:, half] = (x_ref[:, half].astype(F32) + total).astype(BF16)


def back(x_loc, o_halves, a1, own, perm, send, wao, wmo):
    rows, width = x_loc.shape
    num_o, num_c = wao.shape[0] // C, wmo.shape[0] // C
    num_k, late = num_o + num_c, num_c - N1
    groups = 2 + 2 * (late // PIECE)
    quarter = rows // 4
    dma = pltpu.SemaphoreType.DMA
    any_spec = pl.BlockSpec(memory_space=pl.ANY)
    vmem_spec = pl.BlockSpec(memory_space=pltpu.VMEM)
    y = pl.pallas_call(
        back_kernel,
        name="back",
        out_shape=jax.ShapeDtypeStruct((4, 2, rows // 8, width), BF16),
        in_specs=[vmem_spec] * 3 + [any_spec] * 5,
        out_specs=vmem_spec,
        scratch_shapes=[
            pltpu.VMEM((num_k, C, 2 * width), BF16),
            pltpu.VMEM((late, quarter, 2 * C), F32),
            pltpu.VMEM((late, quarter, 2 * C), F32),
            pltpu.VMEM((2, 4, rows // 8, num_k * C), BF16),
            pltpu.VMEM((2, 2, rows // 2, width), F32),
            pltpu.VMEM((2, rows // 2, width), F32),
            dma((num_k,)), dma((late,)), dma((num_c - N2,)), dma((late,)), dma, dma,
            dma((groups,)), dma((groups,)), dma((groups,)), dma((groups,)), dma((groups,)), dma((groups,)),
            dma((2,)), dma((2,)),
        ],
        compiler_params=pltpu.CompilerParams(collective_id=1, has_side_effects=True, vmem_limit_bytes=VMEM_LIMIT),
        cost_estimate=pl.CostEstimate(
            flops=4 * rows * num_k * C * width, bytes_accessed=4 * num_k * C * width, transcendentals=0
        ),
    )(x_loc.reshape(4, 2, rows // 8, width), o_halves, a1, own, perm, send, wao, wmo)
    return y.reshape(rows, width)


def solution(mesh):
    x_size, yz_size = mesh.shape["x"], mesh.shape["yz"]
    both_axes = ("x", "yz")
    row_spec = P("dp", both_axes)
    in_w_spec = P("x", "yz")
    out_w_spec = P("yz", "x")
    cache_spec = P(("dp", "x", "yz"), None, None)
    len_spec = P(("dp", "x", "yz"))
    across = [(i, (i + 2) % 4) for i in range(4)]

    def local_layer(x_loc, gain_loc, wqkv_loc, wgate_loc, wup_loc, wao_loc, wmo_loc, kc_loc, vc_loc, len_loc):
        d_model = x_loc.shape[1] * x_size * yz_size
        reqs, _, head_dim = kc_loc.shape
        half = head_dim // 2
        inv_freq = 10000.0 ** (-jnp.arange(half, dtype=F32) / half)
        angles = len_loc.astype(F32)[:, None] * inv_freq
        cos, sin = jnp.cos(angles), jnp.sin(angles)
        cos = jnp.concatenate([cos, cos], axis=1)[:, None, :]
        sin = jnp.concatenate([-sin, sin], axis=1)[:, None, :]

        qkv, a1, perm, send, own = front(
            x_loc, gain_loc, wqkv_loc, wgate_loc, wup_loc, d_model
        )
        perm = lax.ppermute(perm, "x", across)
        qkv = jnp.concatenate([qkv[0], qkv[1]], axis=1).reshape(reqs, -1, head_dim)
        k_all, v_all, attn = attend(qkv, cos, sin, kc_loc, vc_loc, len_loc)
        o_halves = jnp.swapaxes(attn.reshape(reqs, 2, -1), 0, 1)
        y_loc = back(x_loc, o_halves, a1, own, perm, send, wao_loc, wmo_loc)
        return y_loc, k_all, v_all

    in_specs = (row_spec, P(both_axes), in_w_spec, in_w_spec, in_w_spec, out_w_spec, out_w_spec, cache_spec, cache_spec, len_spec)
    out_specs = (row_spec, cache_spec, cache_spec)
    return jax.shard_map(local_layer, mesh=mesh, in_specs=in_specs, out_specs=out_specs, check_vma=False)
```

```python
import functools

import jax
import jax.numpy as jnp
from jax import lax
from jax.experimental import pallas as pl
from jax.experimental.pallas import tpu as pltpu
from jax.sharding import PartitionSpec as P

MESH = pl.DeviceIdType.MESH
F32 = jnp.float32
BF16 = jnp.bfloat16
VMEM_LIMIT = 66_900_000

C = 768
CQ = 640
SLOTS = 3
N1 = 4
N2 = 13
PIECES = (3, 3, 3, 2, 1)


def remote(src, dst, send_sem, recv_sem, device):
    return pltpu.make_async_remote_copy(
        src_ref=src, dst_ref=dst, send_sem=send_sem, recv_sem=recv_sem, device_id=device, device_id_type=MESH
    )


def places():
    xi = lax.axis_index("x")
    yi = lax.axis_index("yz")
    sib = xi + 1 - 2 * (xi % 2)
    xn = (xi + 2) % 4
    return xi, yi, sib, xn, (sib + 2) % 4, 1 - yi


def activation(total):
    gate = total[:, :C].astype(BF16).astype(F32)
    up = total[:, C:].astype(BF16).astype(F32)
    return (jax.nn.silu(gate) * up).astype(BF16)


def front_kernel(
    d_model, x_hbm, g_hbm, wq_hbm, wg_hbm, wu_hbm,
    qkv_hbm, a_hbm, perm_hbm, send_hbm, own_hbm,
    stat, xbuf, gain, gbuf, moments, h, wq, wg, wu, pq, rq, xq, qs, qd, p, r, xr, a,
    in_sem, wq_sem, wg_sem, wu_sem, st_s, st_r, xg_s, xg_r,
    dq_s, dq_r, xq_s, xq_r, yq_s, yq_r, d_s, d_r, x_s, x_r, out_sem, own_sem, q_sem, a_sem,
):
    xi, yi, sib, xn, sibn, yn = places()
    me = yi * 4 + xi
    sides, side_rows, width = x_hbm.shape
    rows = sides * side_rows
    near = xi // 2
    far = 1 - near
    num_q = wq_hbm.shape[1] // CQ
    num_c = wg_hbm.shape[1] // C
    sib_dev, xn_dev, yn_dev = {"x": sib}, {"x": xn}, {"yz": yn}

    def wq_copy(c):
        return pltpu.make_async_copy(wq_hbm.at[:, pl.ds(c * CQ, CQ)], wq.at[c], wq_sem.at[c])

    def w_copies(i, slot):
        start = pl.multiple_of(i * C, C)
        return (
            pltpu.make_async_copy(wg_hbm.at[:, pl.ds(start, C)], wg.at[slot], wg_sem.at[slot]),
            pltpu.make_async_copy(wu_hbm.at[:, pl.ds(start, C)], wu.at[slot], wu_sem.at[slot]),
        )

    x_in = pltpu.make_async_copy(x_hbm, xbuf.at[yi], in_sem.at[0])
    g_in = pltpu.make_async_copy(g_hbm, gain, in_sem.at[1])
    x_in.start()
    g_in.start()
    barrier = pltpu.get_barrier_semaphore()
    offsets = [(dy, dx) for dy in range(2) for dx in range(4)][1:]
    for dy, dx in offsets:
        pl.semaphore_signal(barrier, inc=1, device_id={"yz": (yi + dy) % 2, "x": (xi + dx) % 4}, device_id_type=MESH)

    x_in.wait()
    x_f32 = xbuf[yi].reshape(rows, width).astype(F32)
    lane = lax.broadcasted_iota(jnp.int32, (rows, rows), 1)
    sums = jnp.where(
        lane == 0,
        jnp.sum(x_f32, axis=1, keepdims=True),
        jnp.where(lane == 1, jnp.sum(x_f32 * x_f32, axis=1, keepdims=True), 0.0),
    )
    stat[me] = sums.T[0:8, :]
    g_in.wait()
    gbuf[yi] = jnp.broadcast_to(gain[...].astype(F32)[None, :], (8, width))
    pl.semaphore_wait(barrier, 7)

    def stat_copy(k, slot):
        dy, dx = offsets[k]
        dev = {"yz": (yi + dy) % 2, "x": (xi + dx) % 4}
        return remote(stat.at[slot], stat.at[slot], st_s.at[k], st_r.at[k], dev)

    def x_copies(slot):
        return [
            remote(xbuf.at[slot, side], xbuf.at[slot, side], xg_s.at[1 + n], xg_r.at[1 + n], yn_dev)
            for n, side in enumerate((far, near))
        ]

    def g_copy(slot):
        return remote(gbuf.at[slot], gbuf.at[slot], xg_s.at[0], xg_r.at[0], yn_dev)

    for k in range(7):
        stat_copy(k, me).start()
    g_copy(yi).start()
    for copy in x_copies(yi):
        copy.start()
    for c in range(num_q):
        wq_copy(c).start()
    for i in range(SLOTS):
        for copy in w_copies(i, i):
            copy.start()
    for k, (dy, dx) in enumerate(offsets):
        stat_copy(k, ((yi + 2 - dy) % 2) * 4 + (xi + 4 - dx) % 4).wait_recv()
    total = stat[0]
    for k in range(1, 8):
        total = total + stat[k]
    cols = jnp.concatenate([total, jnp.zeros((rows - 8, rows), F32)], axis=0).T
    mean = cols[:, 0:1] / d_model
    var = cols[:, 1:2] / d_model - mean * mean
    moments[0] = jnp.broadcast_to(mean, (rows, 128)).reshape(sides, side_rows, 128)
    moments[1] = jnp.broadcast_to(lax.rsqrt(var + 1e-6), (rows, 128)).reshape(sides, side_rows, 128)
    g_copy(yn).wait_recv()

    def normalize(side):
        for b in range(2):
            part = (xbuf[b, side].astype(F32) - moments[0, side][:, 0:1]) * moments[1, side][:, 0:1]
            h[side, :, b * width:(b + 1) * width] = (part * gbuf[b][0:1, :]).astype(BF16)

    def dq(c, k):
        src = sib if k == 0 else sibn
        return remote(pq.at[c, src], rq.at[c, k], dq_s.at[c, k], dq_r.at[c, k], sib_dev)

    def xq_copy(c):
        return remote(pq.at[c, xn], xq.at[c], xq_s.at[c], xq_r.at[c], xn_dev)

    def q_product(c, side):
        prod = jnp.dot(h[side], wq[c], preferred_element_type=F32)
        pq[c, pl.ds(2 * side, 2)] = prod.reshape(2, rows // 4, CQ)

    def q_send(c):
        dq(c, 1).wait_recv()
        dq(c, 1).wait_send()
        pq[c, xn] = pq[c, xn] + rq[c, 1]
        xq_copy(c).start()

    x_copies(yn)[0].wait_recv()
    normalize(far)

    @pl.loop(0, num_q)
    def _(c):
        wq_copy(c).wait()
        q_product(c, far)
        dq(c, 1).start()

        @pl.when(c >= 1)
        def _():
            q_send(c - 1)

    x_copies(yn)[1].wait_recv()
    normalize(near)
    q_send(num_q - 1)

    @pl.loop(0, num_q)
    def _(c):
        q_product(c, near)
        dq(c, 0).start()

    def d_copy(i, k):
        src = sib if k == 0 else sibn
        return remote(p.at[i, src], r.at[i, k], d_s.at[i, k], d_r.at[i, k], sib_dev)

    def x_send(i):
        return remote(p.at[i, xn], xr.at[i], x_s.at[i], x_r.at[i], xn_dev)

    def perm_copy(i):
        return pltpu.make_async_copy(p.at[i, xn], perm_hbm.at[i - N1], out_sem.at[i])

    def send_copy(i):
        return pltpu.make_async_copy(p.at[i, xn], send_hbm.at[i - N2], out_sem.at[i])

    def own_copy(i):
        return pltpu.make_async_copy(p.at[i, xi], own_hbm.at[i - N1], own_sem.at[i])

    def chip_sum(i):
        d_copy(i, 1).wait_recv()
        d_copy(i, 1).wait_send()
        p[i, xn] = p[i, xn] + r[i, 1]

        @pl.when(i < N1)
        def _():
            x_send(i).start()

        @pl.when((i >= N1) & (i < N2))
        def _():
            perm_copy(i).start()

        @pl.when(i >= N2)
        def _():
            send_copy(i).start()

        d_copy(i, 0).wait_recv()
        d_copy(i, 0).wait_send()
        p[i, xi] = p[i, xi] + r[i, 0]

        @pl.when(i >= N1)
        def _():
            own_copy(i).start()

    def product(i):
        slot = i % SLOTS
        g_w, u_w = w_copies(i, slot)
        h_all = h[...].reshape(rows, h.shape[2])
        g_w.wait()
        p[i, :, :, :C] = jnp.dot(h_all, wg[slot], preferred_element_type=F32).reshape(4, rows // 4, C)
        u_w.wait()
        p[i, :, :, C:] = jnp.dot(h_all, wu[slot], preferred_element_type=F32).reshape(4, rows // 4, C)
        d_copy(i, 1).start()
        d_copy(i, 0).start()

        @pl.when(i + SLOTS < num_c)
        def _():
            for copy in w_copies(i + SLOTS, slot):
                copy.start()

    product(0)

    def step(i):
        product(i)
        chip_sum(i - 1)

    half = num_c // 2 + 1
    pl.loop(1, half)(step)

    @pl.loop(0, num_q)
    def _(c):
        dq(c, 0).wait_recv()
        dq(c, 0).wait_send()
        mine = pq[c, xi] + rq[c, 0]
        xq_copy(c).wait_recv()
        xq_copy(c).wait_send()
        value = (mine + xq[c]).astype(BF16)
        qs[:, :, pl.ds(pl.multiple_of(c * CQ, CQ), CQ)] = value.reshape(2, rows // 8, CQ)

    def yq_copy(k):
        return remote(qs.at[1 - k], qd.at[k], yq_s, yq_r, yn_dev)

    yq_copy(yi).start()
    qd[yi] = qs[yi]

    pl.loop(half, num_c)(step)
    chip_sum(num_c - 1)
    yq_copy(yn).wait_recv()
    q_out = pltpu.make_async_copy(qd, qkv_hbm, q_sem)
    q_out.start()

    @pl.loop(0, N1)
    def _(i):
        x_send(i).wait_recv()
        x_send(i).wait_send()
        act = activation(p[i, xi] + xr[i])
        a[:, :, pl.ds(pl.multiple_of(i * C, C), C)] = act.reshape(2, rows // 8, C)

    a_out = pltpu.make_async_copy(a, a_hbm, a_sem)
    a_out.start()
    for k in range(7):
        stat_copy(k, me).wait_send()
    g_copy(yi).wait_send()
    for copy in x_copies(yi):
        copy.wait_send()
    yq_copy(yi).wait_send()

    @pl.loop(N1, N2)
    def _(i):
        perm_copy(i).wait()
        own_copy(i).wait()

    @pl.loop(N2, num_c)
    def _(i):
        send_copy(i).wait()
        own_copy(i).wait()

    q_out.wait()
    a_out.wait()


def front(x_loc, gain_loc, wqkv, wgate, wup, d_model):
    rows, width = x_loc.shape
    depth, q_cols = wqkv.shape
    num_q, num_c = q_cols // CQ, wgate.shape[1] // C
    quarter = rows // 4
    dma = pltpu.SemaphoreType.DMA
    any_spec = pl.BlockSpec(memory_space=pl.ANY)
    return pl.pallas_call(
        functools.partial(front_kernel, d_model),
        name="front",
        out_shape=(
            jax.ShapeDtypeStruct((2, rows // 8, q_cols), BF16),
            jax.ShapeDtypeStruct((2, rows // 8, N1 * C), BF16),
            jax.ShapeDtypeStruct((N2 - N1, quarter, 2 * C), F32),
            jax.ShapeDtypeStruct((num_c - N2, quarter, 2 * C), F32),
            jax.ShapeDtypeStruct((num_c - N1, quarter, 2 * C), F32),
        ),
        in_specs=[any_spec] * 5,
        out_specs=(any_spec,) * 5,
        scratch_shapes=[
            pltpu.VMEM((8, 8, rows), F32),
            pltpu.VMEM((2, 2, rows // 2, width), BF16),
            pltpu.VMEM((width,), BF16),
            pltpu.VMEM((2, 8, width), F32),
            pltpu.VMEM((2, 2, rows // 2, 128), F32),
            pltpu.VMEM((2, rows // 2, depth), BF16),
            pltpu.VMEM((num_q, depth, CQ), BF16),
            pltpu.VMEM((SLOTS, depth, C), BF16),
            pltpu.VMEM((SLOTS, depth, C), BF16),
            pltpu.VMEM((num_q, 4, quarter, CQ), F32),
            pltpu.VMEM((num_q, 2, quarter, CQ), F32),
            pltpu.VMEM((num_q, quarter, CQ), F32),
            pltpu.VMEM((2, rows // 8, q_cols), BF16),
            pltpu.VMEM((2, rows // 8, q_cols), BF16),
            pltpu.VMEM((num_c, 4, quarter, 2 * C), F32),
            pltpu.VMEM((num_c, 2, quarter, 2 * C), F32),
            pltpu.VMEM((N1, quarter, 2 * C), F32),
            pltpu.VMEM((2, rows // 8, N1 * C), BF16),
            dma((2,)), dma((num_q,)), dma((SLOTS,)), dma((SLOTS,)), dma((7,)), dma((7,)), dma((3,)), dma((3,)),
            dma((num_q, 2)), dma((num_q, 2)), dma((num_q,)), dma((num_q,)), dma, dma,
            dma((num_c, 2)), dma((num_c, 2)), dma((N1,)), dma((N1,)), dma((num_c,)), dma((num_c,)), dma, dma,
        ],
        compiler_params=pltpu.CompilerParams(collective_id=0, has_side_effects=True, vmem_limit_bytes=VMEM_LIMIT),
        cost_estimate=pl.CostEstimate(
            flops=2 * rows * depth * (q_cols + 2 * wgate.shape[1]),
            bytes_accessed=2 * depth * (q_cols + 2 * wgate.shape[1]),
            transcendentals=0,
        ),
    )(x_loc.reshape(2, rows // 2, width), gain_loc, wqkv, wgate, wup)


def attend_kernel(len_ref, qkv_ref, cos_ref, sin_ref, k_ref, v_ref, ko_ref, vo_ref, o_ref):
    pos = len_ref[pl.program_id(0)]
    qkv = qkv_ref[0]
    heads, head_dim = qkv.shape[0] - 2, qkv.shape[1]
    wide = qkv.astype(F32)
    turned = (wide * cos_ref[0] + pltpu.roll(wide, head_dim // 2, 1) * sin_ref[0]).astype(BF16)
    query = turned[:heads]
    ko_ref[...] = k_ref[...]
    vo_ref[...] = v_ref[...]
    base = pl.multiple_of((pos // 16) * 16, 16)
    here = lax.broadcasted_iota(jnp.int32, (16, head_dim), 0) == pos - base
    for out, new in ((ko_ref, turned[heads:heads + 1]), (vo_ref, qkv[heads + 1:heads + 2])):
        tile = out[0, pl.ds(base, 16), :].astype(F32)
        out[0, pl.ds(base, 16), :] = jnp.where(here, new.astype(F32), tile).astype(BF16)
    scores = lax.dot_general(query, ko_ref[0], (((1,), (1,)), ((), ())), preferred_element_type=F32)
    scores = scores * head_dim ** -0.5
    at = lax.broadcasted_iota(jnp.int32, scores.shape, 1)
    scores = jnp.where(at <= pos, scores, -1e30)
    weight = jnp.exp(scores - jnp.max(scores, axis=1, keepdims=True))
    probs = (weight / jnp.sum(weight, axis=1, keepdims=True)).astype(BF16)
    o_ref[0] = jnp.dot(probs, vo_ref[0], preferred_element_type=F32).astype(BF16)


def attend(qkv, cos, sin, k_cache, v_cache, ctx_len):
    reqs, length, head_dim = k_cache.shape
    heads = qkv.shape[1] - 2
    cache_spec = pl.BlockSpec((1, length, head_dim), lambda i, lens: (i, 0, 0))
    table_spec = pl.BlockSpec((1, 1, head_dim), lambda i, lens: (i, 0, 0))
    return pl.pallas_call(
        attend_kernel,
        name="attend",
        grid_spec=pltpu.PrefetchScalarGridSpec(
            num_scalar_prefetch=1,
            grid=(reqs,),
            in_specs=[
                pl.BlockSpec((1, heads + 2, head_dim), lambda i, lens: (i, 0, 0)),
                table_spec, table_spec, cache_spec, cache_spec,
            ],
            out_specs=[cache_spec, cache_spec, pl.BlockSpec((1, heads, head_dim), lambda i, lens: (i, 0, 0))],
        ),
        out_shape=(
            jax.ShapeDtypeStruct(k_cache.shape, BF16),
            jax.ShapeDtypeStruct(v_cache.shape, BF16),
            jax.ShapeDtypeStruct((reqs, heads, head_dim), BF16),
        ),
        compiler_params=pltpu.CompilerParams(dimension_semantics=("arbitrary",)),
        cost_estimate=pl.CostEstimate(
            flops=64 * reqs * heads * length * head_dim,
            bytes_accessed=8 * reqs * length * head_dim,
            transcendentals=reqs * heads * length,
        ),
    )(ctx_len, qkv, cos, sin, k_cache, v_cache)


def back_kernel(
    o_hbm, a1_hbm, own_hbm, perm_hbm, send_hbm, wao_hbm, wmo_hbm, z_hbm,
    w, own, xr, act, z, zr,
    in_sem, out_sem, w_sem, own_sem, x_s, x_r, o_s, o_r, sib_s, sib_r, xn_s, xn_r, fwd_s, fwd_r, z_s, z_r,
):
    xi, yi, sib, xn, _, yn = places()
    sib_dev, xn_dev, yn_dev = {"x": sib}, {"x": xn}, {"yz": yn}
    width = z_hbm.shape[3]
    half_rows = act.shape[1] * act.shape[2]
    num_o, num_c = wao_hbm.shape[0] // C, wmo_hbm.shape[0] // C
    num_k = num_o + num_c
    o_cols = wao_hbm.shape[0]
    late = num_c - N1
    here = N2 - N1
    pieces = len(PIECES)
    starts = [sum(PIECES[:n]) for n in range(pieces + 1)]

    def w_copy(k):
        src = wao_hbm.at[pl.ds(k * C, C), :] if k < num_o else wmo_hbm.at[pl.ds((k - num_o) * C, C), :]
        return pltpu.make_async_copy(src, w.at[k], w_sem.at[k])

    def own_copy(i):
        return pltpu.make_async_copy(own_hbm.at[i], own.at[i], own_sem.at[i])

    def perm_copy(i):
        return pltpu.make_async_copy(perm_hbm.at[i], xr.at[i], x_r.at[i])

    def x_send(i):
        return remote(send_hbm.at[i - here], xr.at[i], x_s.at[i - here], x_r.at[i], xn_dev)

    barrier = pltpu.get_barrier_semaphore()
    for dev in (sib_dev, xn_dev, yn_dev):
        pl.semaphore_signal(barrier, inc=1, device_id=dev, device_id_type=MESH)
    o_in = pltpu.make_async_copy(o_hbm.at[yi], act.at[yi, xi, :, 0:o_cols], in_sem.at[0])
    a1_in = pltpu.make_async_copy(a1_hbm, act.at[:, xi, :, pl.ds(o_cols, N1 * C)], in_sem.at[1])
    o_in.start()
    a1_in.start()
    for i in range(late):
        own_copy(i).start()
    for i in range(here):
        perm_copy(i).start()
    pl.semaphore_wait(barrier, 3)

    def o_copy(half, row):
        return remote(o_hbm.at[half], act.at[row, xi, :, 0:o_cols], o_s, o_r, yn_dev)

    def block_of(e, owner):
        if e == 0:
            return act.at[:, owner, :, pl.ds(o_cols, N1 * C)]
        if e == 1:
            return act.at[:, owner, :, pl.ds(0, o_cols)]
        half, n = divmod(e - 2, pieces)
        return act.at[half, owner, :, pl.ds(o_cols + (N1 + starts[n]) * C, PIECES[n] * C)]

    def to_sib(e, owner):
        block = block_of(e, owner)
        return remote(block, block, sib_s.at[e], sib_r.at[e], sib_dev)

    def to_xn(e, owner):
        block = block_of(e, owner)
        return remote(block, block, xn_s.at[e], xn_r.at[e], xn_dev)

    def forward(e, owner):
        block = block_of(e, owner)
        return remote(block, block, fwd_s.at[e], fwd_r.at[e], sib_dev)

    def send_own(e):
        to_xn(e, xi).start()
        to_sib(e, xi).start()

    def pass_on(e):
        to_xn(e, xn).wait_recv()
        forward(e, xn).start()

    def arrived(e):
        to_sib(e, sib).wait_recv()
        forward(e, (sib + 2) % 4).wait_recv()

    def activate(i):
        own_copy(i).wait()
        value = activation(own[i] + xr[i])
        start = pl.multiple_of(o_cols + (N1 + i) * C, C)
        act[:, xi, :, pl.ds(start, C)] = value.reshape(2, value.shape[0] // 2, C)

    def w_wait(k):
        pltpu.make_async_copy(wmo_hbm.at[pl.ds(0, C), :], w.at[k], w_sem.at[k]).wait()

    def multiply(first, count):
        @pl.loop(first, first + count)
        def _(k):
            w_wait(k)
            lhs = act[:, :, :, pl.ds(pl.multiple_of(k * C, C), C)].reshape(2 * half_rows, C)
            for b in range(2):
                prod = jnp.dot(lhs, w[k, :, b * width:(b + 1) * width], preferred_element_type=F32)
                z[b] = z[b] + prod.reshape(z.shape[1:])

    def multiply_half(half, n):
        @pl.loop(num_o + N1 + starts[n], num_o + N1 + starts[n + 1])
        def _(k):
            if half == 0:
                w_wait(k)
            lhs = act[half, :, :, pl.ds(pl.multiple_of(k * C, C), C)].reshape(half_rows, C)
            for b in range(2):
                prod = jnp.dot(lhs, w[k, :, b * width:(b + 1) * width], preferred_element_type=F32)
                z[b, half] = z[b, half] + prod.reshape(z.shape[2:])

    first = (late - here + 1) // 2
    for i in range(here, here + first):
        x_send(i).start()
    o_copy(yn, yi).start()
    for k in range(num_k):
        w_copy(k).start()
    z[...] = jnp.zeros_like(z)

    @pl.loop(0, here)
    def _(i):
        perm_copy(i).wait()
        activate(i)

    a1_in.wait()
    o_in.wait()
    o_copy(yi, yn).wait_recv()
    send_own(1)
    send_own(0)
    for i in range(here + first, late):
        x_send(i).start()
    ready = sum(end <= here for end in starts[1:])
    for n in range(ready):
        send_own(2 + n)

    @pl.loop(here, here + first)
    def _(i):
        x_send(i).wait_recv()
        activate(i)

    pass_on(1)
    pass_on(0)
    arrived(1)
    multiply(0, num_o)
    arrived(0)
    multiply(num_o, N1)

    @pl.loop(here + first, late)
    def _(i):
        x_send(i).wait_recv()
        activate(i)

    groups = 2 + 2 * pieces
    for e in range(2 + ready, groups):
        send_own(e)
    z_copies = [remote(z.at[yn, half], zr.at[half], z_s.at[half], z_r.at[half], yn_dev) for half in range(2)]
    pass_on(2)
    for e in range(2, groups):
        if e + 1 < groups:
            pass_on(e + 1)
        arrived(e)
        half, n = divmod(e - 2, pieces)
        multiply_half(half, n)
        if n == pieces - 1:
            z_copies[half].start()

    o_copy(yn, yi).wait_send()
    for e in range(groups):
        to_xn(e, xi).wait_send()
        to_sib(e, xi).wait_send()
        forward(e, xn).wait_send()

    @pl.loop(here, late)
    def _(i):
        x_send(i).wait_send()

    outs = [pltpu.make_async_copy(zr.at[half], z_hbm.at[:, half], out_sem.at[half]) for half in range(2)]
    for half in range(2):
        z_copies[half].wait()
        zr[half] = z[yi, half] + zr[half]
        outs[half].start()
    for half in range(2):
        outs[half].wait()


def back(x_loc, o_halves, a1, own, perm, send, wao, wmo):
    rows, width = x_loc.shape
    num_o, num_c = wao.shape[0] // C, wmo.shape[0] // C
    num_k, late = num_o + num_c, num_c - N1
    groups = 2 + 2 * len(PIECES)
    quarter = rows // 4
    dma = pltpu.SemaphoreType.DMA
    any_spec = pl.BlockSpec(memory_space=pl.ANY)
    z = pl.pallas_call(
        back_kernel,
        name="back",
        out_shape=jax.ShapeDtypeStruct((4, 2, rows // 8, width), F32),
        in_specs=[any_spec] * 7,
        out_specs=any_spec,
        scratch_shapes=[
            pltpu.VMEM((num_k, C, 2 * width), BF16),
            pltpu.VMEM((late, quarter, 2 * C), F32),
            pltpu.VMEM((late, quarter, 2 * C), F32),
            pltpu.VMEM((2, 4, rows // 8, num_k * C), BF16),
            pltpu.VMEM((2, 2, 4, rows // 8, width), F32),
            pltpu.VMEM((2, 4, rows // 8, width), F32),
            dma((2,)), dma((2,)), dma((num_k,)), dma((late,)), dma((num_c - N2,)), dma((late,)), dma, dma,
            dma((groups,)), dma((groups,)), dma((groups,)), dma((groups,)), dma((groups,)), dma((groups,)),
            dma((2,)), dma((2,)),
        ],
        compiler_params=pltpu.CompilerParams(collective_id=1, has_side_effects=True, vmem_limit_bytes=VMEM_LIMIT),
        cost_estimate=pl.CostEstimate(
            flops=4 * rows * num_k * C * width, bytes_accessed=4 * num_k * C * width, transcendentals=0
        ),
    )(o_halves, a1, own, perm, send, wao, wmo)
    return (x_loc.astype(F32) + z.reshape(rows, width)).astype(BF16)


def solution(mesh):
    x_size, yz_size = mesh.shape["x"], mesh.shape["yz"]
    both_axes = ("x", "yz")
    row_spec = P("dp", both_axes)
    in_w_spec = P("x", "yz")
    out_w_spec = P("yz", "x")
    cache_spec = P(("dp", "x", "yz"), None, None)
    len_spec = P(("dp", "x", "yz"))
    across = [(i, (i + 2) % 4) for i in range(4)]

    def local_layer(x_loc, gain_loc, wqkv_loc, wgate_loc, wup_loc, wao_loc, wmo_loc, kc_loc, vc_loc, len_loc):
        d_model = x_loc.shape[1] * x_size * yz_size
        reqs, _, head_dim = kc_loc.shape
        half = head_dim // 2
        inv_freq = 10000.0 ** (-jnp.arange(half, dtype=F32) / half)
        angles = len_loc.astype(F32)[:, None] * inv_freq
        cos, sin = jnp.cos(angles), jnp.sin(angles)
        cos = jnp.concatenate([cos, cos], axis=1)[:, None, :]
        sin = jnp.concatenate([-sin, sin], axis=1)[:, None, :]

        qkv, a1, perm, send, own = front(
            x_loc, gain_loc, wqkv_loc, wgate_loc, wup_loc, d_model
        )
        perm = lax.ppermute(perm, "x", across)
        qkv = jnp.concatenate([qkv[0], qkv[1]], axis=1).reshape(reqs, -1, head_dim)
        k_all, v_all, attn = attend(qkv, cos, sin, kc_loc, vc_loc, len_loc)
        o_halves = jnp.swapaxes(attn.reshape(reqs, 2, -1), 0, 1)
        y_loc = back(x_loc, o_halves, a1, own, perm, send, wao_loc, wmo_loc)
        return y_loc, k_all, v_all

    in_specs = (row_spec, P(both_axes), in_w_spec, in_w_spec, in_w_spec, out_w_spec, out_w_spec, cache_spec, cache_spec, len_spec)
    out_specs = (row_spec, cache_spec, cache_spec)
    return jax.shard_map(local_layer, mesh=mesh, in_specs=in_specs, out_specs=out_specs, check_vma=False)
```

```python
import functools

import jax
import jax.numpy as jnp
from jax import lax
from jax.experimental import pallas as pl
from jax.experimental.pallas import tpu as pltpu
from jax.sharding import PartitionSpec as P

MESH = pl.DeviceIdType.MESH
F32 = jnp.float32
BF16 = jnp.bfloat16
VMEM_LIMIT = 66_900_000

C = 768
CQ = 640
PER_STEP = 2
SLOTS = 3
N1 = 5
N2 = 13
PIECES = (3, 3, 2, 2, 1)


def remote(src, dst, send_sem, recv_sem, device):
    return pltpu.make_async_remote_copy(
        src_ref=src, dst_ref=dst, send_sem=send_sem, recv_sem=recv_sem, device_id=device, device_id_type=MESH
    )


def places():
    xi = lax.axis_index("x")
    yi = lax.axis_index("yz")
    sib = xi + 1 - 2 * (xi % 2)
    xn = (xi + 2) % 4
    return xi, yi, sib, xn, (sib + 2) % 4, 1 - yi


def activation(total):
    gate = total[:, :C].astype(BF16).astype(F32)
    up = total[:, C:].astype(BF16).astype(F32)
    return (jax.nn.silu(gate) * up).astype(BF16)


def front_kernel(
    d_model, x_hbm, g_hbm, wq_hbm, wg_hbm, wu_hbm,
    qkv_hbm, a_hbm, perm_hbm, send_hbm, own_hbm,
    stat, xbuf, gain, gbuf, moments, h, wq, wg, wu, pq, rq, xq, qs, qd, p, r, xr, a,
    in_sem, wq_sem, wg_sem, wu_sem, st_s, st_r, xg_s, xg_r,
    dq_s, dq_r, xq_s, xq_r, yq_s, yq_r, d_s, d_r, x_s, x_r, out_sem, own_sem, q_sem, a_sem,
):
    xi, yi, sib, xn, sibn, yn = places()
    me = yi * 4 + xi
    sides, side_rows, width = x_hbm.shape
    rows = sides * side_rows
    near = xi // 2
    far = 1 - near
    num_q = wq_hbm.shape[1] // CQ
    num_c = wg_hbm.shape[1] // C
    sib_dev, xn_dev, yn_dev = {"x": sib}, {"x": xn}, {"yz": yn}

    def wq_copy(c):
        return pltpu.make_async_copy(wq_hbm.at[:, pl.ds(c * CQ, CQ)], wq.at[c], wq_sem.at[c])

    def w_copies(i, slot):
        start = pl.multiple_of(i * C, C)
        return (
            pltpu.make_async_copy(wg_hbm.at[:, pl.ds(start, C)], wg.at[slot], wg_sem.at[slot]),
            pltpu.make_async_copy(wu_hbm.at[:, pl.ds(start, C)], wu.at[slot], wu_sem.at[slot]),
        )

    x_in = pltpu.make_async_copy(x_hbm, xbuf.at[yi], in_sem.at[0])
    g_in = pltpu.make_async_copy(g_hbm, gain, in_sem.at[1])
    x_in.start()
    g_in.start()
    barrier = pltpu.get_barrier_semaphore()
    offsets = [(dy, dx) for dy in range(2) for dx in range(4)][1:]
    for dy, dx in offsets:
        pl.semaphore_signal(barrier, inc=1, device_id={"yz": (yi + dy) % 2, "x": (xi + dx) % 4}, device_id_type=MESH)

    x_in.wait()
    x_f32 = xbuf[yi].reshape(rows, width).astype(F32)
    lane = lax.broadcasted_iota(jnp.int32, (rows, rows), 1)
    sums = jnp.where(
        lane == 0,
        jnp.sum(x_f32, axis=1, keepdims=True),
        jnp.where(lane == 1, jnp.sum(x_f32 * x_f32, axis=1, keepdims=True), 0.0),
    )
    stat[me] = sums.T[0:8, :]
    g_in.wait()
    gbuf[yi] = jnp.broadcast_to(gain[...].astype(F32)[None, :], (8, width))
    pl.semaphore_wait(barrier, 7)

    def stat_copy(k, slot):
        dy, dx = offsets[k]
        dev = {"yz": (yi + dy) % 2, "x": (xi + dx) % 4}
        return remote(stat.at[slot], stat.at[slot], st_s.at[k], st_r.at[k], dev)

    def x_copies(slot):
        return [
            remote(xbuf.at[slot, side], xbuf.at[slot, side], xg_s.at[1 + n], xg_r.at[1 + n], yn_dev)
            for n, side in enumerate((far, near))
        ]

    def g_copy(slot):
        return remote(gbuf.at[slot], gbuf.at[slot], xg_s.at[0], xg_r.at[0], yn_dev)

    for k in range(7):
        stat_copy(k, me).start()
    g_copy(yi).start()
    for copy in x_copies(yi):
        copy.start()
    for c in range(num_q):
        wq_copy(c).start()
    for i in range(SLOTS):
        for copy in w_copies(i, i):
            copy.start()
    for k, (dy, dx) in enumerate(offsets):
        stat_copy(k, ((yi + 2 - dy) % 2) * 4 + (xi + 4 - dx) % 4).wait_recv()
    total = stat[0]
    for k in range(1, 8):
        total = total + stat[k]
    cols = jnp.concatenate([total, jnp.zeros((rows - 8, rows), F32)], axis=0).T
    mean = cols[:, 0:1] / d_model
    var = cols[:, 1:2] / d_model - mean * mean
    moments[0] = jnp.broadcast_to(mean, (rows, 128)).reshape(sides, side_rows, 128)
    moments[1] = jnp.broadcast_to(lax.rsqrt(var + 1e-6), (rows, 128)).reshape(sides, side_rows, 128)
    g_copy(yn).wait_recv()

    def normalize(side):
        for b in range(2):
            part = (xbuf[b, side].astype(F32) - moments[0, side][:, 0:1]) * moments[1, side][:, 0:1]
            h[side, :, b * width:(b + 1) * width] = (part * gbuf[b][0:1, :]).astype(BF16)

    def dq(c, k):
        src = sib if k == 0 else sibn
        return remote(pq.at[c, src], rq.at[c, k], dq_s.at[c, k], dq_r.at[c, k], sib_dev)

    def xq_copy(c):
        return remote(pq.at[c, xn], xq.at[c], xq_s.at[c], xq_r.at[c], xn_dev)

    def q_product(c, side):
        prod = jnp.dot(h[side], wq[c], preferred_element_type=F32)
        pq[c, pl.ds(2 * side, 2)] = prod.reshape(2, rows // 4, CQ)

    def q_send(c):
        dq(c, 1).wait_recv()
        dq(c, 1).wait_send()
        pq[c, xn] = pq[c, xn] + rq[c, 1]
        xq_copy(c).start()

    x_copies(yn)[0].wait_recv()
    normalize(far)

    @pl.loop(0, num_q)
    def _(c):
        wq_copy(c).wait()
        q_product(c, far)
        dq(c, 1).start()

        @pl.when(c >= 1)
        def _():
            q_send(c - 1)

    x_copies(yn)[1].wait_recv()
    normalize(near)
    q_send(num_q - 1)

    @pl.loop(0, num_q)
    def _(c):
        q_product(c, near)
        dq(c, 0).start()

    def d_copy(i, k):
        src = sib if k == 0 else sibn
        return remote(p.at[i, src], r.at[i, k], d_s.at[i, k], d_r.at[i, k], sib_dev)

    def x_send(i):
        return remote(p.at[i, xn], xr.at[i], x_s.at[i], x_r.at[i], xn_dev)

    def perm_copy(i):
        return pltpu.make_async_copy(p.at[i, xn], perm_hbm.at[i - N1], out_sem.at[i])

    def send_copy(i):
        return pltpu.make_async_copy(p.at[i, xn], send_hbm.at[i - N2], out_sem.at[i])

    def own_copy(i):
        return pltpu.make_async_copy(p.at[i, xi], own_hbm.at[i - N1], own_sem.at[i])

    def chip_sum(i):
        d_copy(i, 1).wait_recv()
        d_copy(i, 1).wait_send()
        p[i, xn] = p[i, xn] + r[i, 1]

        @pl.when(i < N1)
        def _():
            x_send(i).start()

        @pl.when((i >= N1) & (i < N2))
        def _():
            perm_copy(i).start()

        @pl.when(i >= N2)
        def _():
            send_copy(i).start()

        d_copy(i, 0).wait_recv()
        d_copy(i, 0).wait_send()
        p[i, xi] = p[i, xi] + r[i, 0]

        @pl.when(i >= N1)
        def _():
            own_copy(i).start()

    def product(i):
        slot = i % SLOTS
        g_w, u_w = w_copies(i, slot)
        h_all = h[...].reshape(rows, h.shape[2])
        g_w.wait()
        p[i, :, :, :C] = jnp.dot(h_all, wg[slot], preferred_element_type=F32).reshape(4, rows // 4, C)
        u_w.wait()
        p[i, :, :, C:] = jnp.dot(h_all, wu[slot], preferred_element_type=F32).reshape(4, rows // 4, C)
        d_copy(i, 1).start()
        d_copy(i, 0).start()

        @pl.when(i + SLOTS < num_c)
        def _():
            for copy in w_copies(i + SLOTS, slot):
                copy.start()

    product(0)

    def step(i):
        product(i)
        chip_sum(i - 1)

    half = num_c // 2 + 1
    pl.loop(1, half)(step)

    @pl.loop(0, num_q)
    def _(c):
        dq(c, 0).wait_recv()
        dq(c, 0).wait_send()
        mine = pq[c, xi] + rq[c, 0]
        xq_copy(c).wait_recv()
        xq_copy(c).wait_send()
        value = (mine + xq[c]).astype(BF16)
        qs[:, :, pl.ds(pl.multiple_of(c * CQ, CQ), CQ)] = value.reshape(2, rows // 8, CQ)

    def yq_copy(k):
        return remote(qs.at[1 - k], qd.at[k], yq_s, yq_r, yn_dev)

    yq_copy(yi).start()
    qd[yi] = qs[yi]

    pl.loop(half, num_c)(step)
    chip_sum(num_c - 1)
    yq_copy(yn).wait_recv()
    q_out = pltpu.make_async_copy(qd, qkv_hbm, q_sem)
    q_out.start()

    @pl.loop(0, N1)
    def _(i):
        x_send(i).wait_recv()
        x_send(i).wait_send()
        act = activation(p[i, xi] + xr[i])
        a[:, :, pl.ds(pl.multiple_of(i * C, C), C)] = act.reshape(2, rows // 8, C)

    a_out = pltpu.make_async_copy(a, a_hbm, a_sem)
    a_out.start()
    for k in range(7):
        stat_copy(k, me).wait_send()
    g_copy(yi).wait_send()
    for copy in x_copies(yi):
        copy.wait_send()
    yq_copy(yi).wait_send()

    @pl.loop(N1, N2)
    def _(i):
        perm_copy(i).wait()
        own_copy(i).wait()

    @pl.loop(N2, num_c)
    def _(i):
        send_copy(i).wait()
        own_copy(i).wait()

    q_out.wait()
    a_out.wait()


def front(x_loc, gain_loc, wqkv, wgate, wup, d_model):
    rows, width = x_loc.shape
    depth, q_cols = wqkv.shape
    num_q, num_c = q_cols // CQ, wgate.shape[1] // C
    quarter = rows // 4
    dma = pltpu.SemaphoreType.DMA
    any_spec = pl.BlockSpec(memory_space=pl.ANY)
    return pl.pallas_call(
        functools.partial(front_kernel, d_model),
        name="front",
        out_shape=(
            jax.ShapeDtypeStruct((2, rows // 8, q_cols), BF16),
            jax.ShapeDtypeStruct((2, rows // 8, N1 * C), BF16),
            jax.ShapeDtypeStruct((N2 - N1, quarter, 2 * C), F32),
            jax.ShapeDtypeStruct((num_c - N2, quarter, 2 * C), F32),
            jax.ShapeDtypeStruct((num_c - N1, quarter, 2 * C), F32),
        ),
        in_specs=[any_spec] * 5,
        out_specs=(any_spec,) * 5,
        scratch_shapes=[
            pltpu.VMEM((8, 8, rows), F32),
            pltpu.VMEM((2, 2, rows // 2, width), BF16),
            pltpu.VMEM((width,), BF16),
            pltpu.VMEM((2, 8, width), F32),
            pltpu.VMEM((2, 2, rows // 2, 128), F32),
            pltpu.VMEM((2, rows // 2, depth), BF16),
            pltpu.VMEM((num_q, depth, CQ), BF16),
            pltpu.VMEM((SLOTS, depth, C), BF16),
            pltpu.VMEM((SLOTS, depth, C), BF16),
            pltpu.VMEM((num_q, 4, quarter, CQ), F32),
            pltpu.VMEM((num_q, 2, quarter, CQ), F32),
            pltpu.VMEM((num_q, quarter, CQ), F32),
            pltpu.VMEM((2, rows // 8, q_cols), BF16),
            pltpu.VMEM((2, rows // 8, q_cols), BF16),
            pltpu.VMEM((num_c, 4, quarter, 2 * C), F32),
            pltpu.VMEM((num_c, 2, quarter, 2 * C), F32),
            pltpu.VMEM((N1, quarter, 2 * C), F32),
            pltpu.VMEM((2, rows // 8, N1 * C), BF16),
            dma((2,)), dma((num_q,)), dma((SLOTS,)), dma((SLOTS,)), dma((7,)), dma((7,)), dma((3,)), dma((3,)),
            dma((num_q, 2)), dma((num_q, 2)), dma((num_q,)), dma((num_q,)), dma, dma,
            dma((num_c, 2)), dma((num_c, 2)), dma((N1,)), dma((N1,)), dma((num_c,)), dma((num_c,)), dma, dma,
        ],
        compiler_params=pltpu.CompilerParams(collective_id=0, has_side_effects=True, vmem_limit_bytes=VMEM_LIMIT),
        cost_estimate=pl.CostEstimate(
            flops=2 * rows * depth * (q_cols + 2 * wgate.shape[1]),
            bytes_accessed=2 * depth * (q_cols + 2 * wgate.shape[1]),
            transcendentals=0,
        ),
    )(x_loc.reshape(2, rows // 2, width), gain_loc, wqkv, wgate, wup)


def attend_kernel(len_ref, qkv_ref, cos_ref, sin_ref, k_ref, v_ref, ko_ref, vo_ref, o_ref):
    ko_ref[...] = k_ref[...]
    vo_ref[...] = v_ref[...]
    for n in range(PER_STEP):
        pos = len_ref[pl.program_id(0) * PER_STEP + n]
        qkv = qkv_ref[n]
        heads, head_dim = qkv.shape[0] - 2, qkv.shape[1]
        wide = qkv.astype(F32)
        turned = (wide * cos_ref[n] + pltpu.roll(wide, head_dim // 2, 1) * sin_ref[n]).astype(BF16)
        query = turned[:heads]
        base = pl.multiple_of((pos // 16) * 16, 16)
        here = lax.broadcasted_iota(jnp.int32, (16, head_dim), 0) == pos - base
        for out, new in ((ko_ref, turned[heads:heads + 1]), (vo_ref, qkv[heads + 1:heads + 2])):
            tile = out[n, pl.ds(base, 16), :].astype(F32)
            out[n, pl.ds(base, 16), :] = jnp.where(here, new.astype(F32), tile).astype(BF16)
        scores = lax.dot_general(query, ko_ref[n], (((1,), (1,)), ((), ())), preferred_element_type=F32)
        scores = scores * head_dim ** -0.5
        at = lax.broadcasted_iota(jnp.int32, scores.shape, 1)
        scores = jnp.where(at <= pos, scores, -1e30)
        weight = jnp.exp(scores - jnp.max(scores, axis=1, keepdims=True))
        probs = (weight / jnp.sum(weight, axis=1, keepdims=True)).astype(BF16)
        o_ref[n] = jnp.dot(probs, vo_ref[n], preferred_element_type=F32).astype(BF16)


def attend(qkv, cos, sin, k_cache, v_cache, ctx_len):
    reqs, length, head_dim = k_cache.shape
    heads = qkv.shape[1] - 2
    cache_spec = pl.BlockSpec((PER_STEP, length, head_dim), lambda i, lens: (i, 0, 0))
    table_spec = pl.BlockSpec((PER_STEP, 1, head_dim), lambda i, lens: (i, 0, 0))
    return pl.pallas_call(
        attend_kernel,
        name="attend",
        grid_spec=pltpu.PrefetchScalarGridSpec(
            num_scalar_prefetch=1,
            grid=(reqs // PER_STEP,),
            in_specs=[
                pl.BlockSpec((PER_STEP, heads + 2, head_dim), lambda i, lens: (i, 0, 0)),
                table_spec, table_spec, cache_spec, cache_spec,
            ],
            out_specs=[cache_spec, cache_spec, pl.BlockSpec((PER_STEP, heads, head_dim), lambda i, lens: (i, 0, 0))],
        ),
        out_shape=(
            jax.ShapeDtypeStruct(k_cache.shape, BF16),
            jax.ShapeDtypeStruct(v_cache.shape, BF16),
            jax.ShapeDtypeStruct((reqs, heads, head_dim), BF16),
        ),
        compiler_params=pltpu.CompilerParams(dimension_semantics=("arbitrary",)),
        cost_estimate=pl.CostEstimate(
            flops=64 * reqs * heads * length * head_dim,
            bytes_accessed=8 * reqs * length * head_dim,
            transcendentals=reqs * heads * length,
        ),
    )(ctx_len, qkv, cos, sin, k_cache, v_cache)


def back_kernel(
    o_hbm, a1_hbm, own_hbm, perm_hbm, send_hbm, wao_hbm, wmo_hbm, z_hbm,
    w, own, xr, act, z, zr,
    in_sem, out_sem, w_sem, own_sem, x_s, x_r, o_s, o_r, sib_s, sib_r, xn_s, xn_r, fwd_s, fwd_r, z_s, z_r,
):
    xi, yi, sib, xn, _, yn = places()
    sib_dev, xn_dev, yn_dev = {"x": sib}, {"x": xn}, {"yz": yn}
    width = z_hbm.shape[3]
    half_rows = act.shape[1] * act.shape[2]
    num_o, num_c = wao_hbm.shape[0] // C, wmo_hbm.shape[0] // C
    num_k = num_o + num_c
    o_cols = wao_hbm.shape[0]
    late = num_c - N1
    here = N2 - N1
    pieces = len(PIECES)
    starts = [sum(PIECES[:n]) for n in range(pieces + 1)]

    def w_copy(k):
        src = wao_hbm.at[pl.ds(k * C, C), :] if k < num_o else wmo_hbm.at[pl.ds((k - num_o) * C, C), :]
        return pltpu.make_async_copy(src, w.at[k], w_sem.at[k])

    def own_copy(i):
        return pltpu.make_async_copy(own_hbm.at[i], own.at[i], own_sem.at[i])

    def perm_copy(i):
        return pltpu.make_async_copy(perm_hbm.at[i], xr.at[i], x_r.at[i])

    def x_send(i):
        return remote(send_hbm.at[i - here], xr.at[i], x_s.at[i - here], x_r.at[i], xn_dev)

    barrier = pltpu.get_barrier_semaphore()
    for dev in (sib_dev, xn_dev, yn_dev):
        pl.semaphore_signal(barrier, inc=1, device_id=dev, device_id_type=MESH)
    o_in = pltpu.make_async_copy(o_hbm.at[yi], act.at[yi, xi, :, 0:o_cols], in_sem.at[0])
    a1_in = pltpu.make_async_copy(a1_hbm, act.at[:, xi, :, pl.ds(o_cols, N1 * C)], in_sem.at[1])
    o_in.start()
    a1_in.start()
    for i in range(late):
        own_copy(i).start()
    for i in range(here):
        perm_copy(i).start()
    pl.semaphore_wait(barrier, 3)

    def o_copy(half, row):
        return remote(o_hbm.at[half], act.at[row, xi, :, 0:o_cols], o_s, o_r, yn_dev)

    def block_of(e, owner):
        if e == 0:
            return act.at[:, owner, :, pl.ds(o_cols, N1 * C)]
        if e == 1:
            return act.at[:, owner, :, pl.ds(0, o_cols)]
        half, n = divmod(e - 2, pieces)
        return act.at[half, owner, :, pl.ds(o_cols + (N1 + starts[n]) * C, PIECES[n] * C)]

    def to_sib(e, owner):
        block = block_of(e, owner)
        return remote(block, block, sib_s.at[e], sib_r.at[e], sib_dev)

    def to_xn(e, owner):
        block = block_of(e, owner)
        return remote(block, block, xn_s.at[e], xn_r.at[e], xn_dev)

    def forward(e, owner):
        block = block_of(e, owner)
        return remote(block, block, fwd_s.at[e], fwd_r.at[e], sib_dev)

    def send_own(e):
        to_xn(e, xi).start()
        to_sib(e, xi).start()

    def pass_on(e):
        to_xn(e, xn).wait_recv()
        forward(e, xn).start()

    def arrived(e):
        to_sib(e, sib).wait_recv()
        forward(e, (sib + 2) % 4).wait_recv()

    def activate(i):
        own_copy(i).wait()
        value = activation(own[i] + xr[i])
        start = pl.multiple_of(o_cols + (N1 + i) * C, C)
        act[:, xi, :, pl.ds(start, C)] = value.reshape(2, value.shape[0] // 2, C)

    def w_wait(k):
        pltpu.make_async_copy(wmo_hbm.at[pl.ds(0, C), :], w.at[k], w_sem.at[k]).wait()

    def multiply(first, count):
        @pl.loop(first, first + count)
        def _(k):
            w_wait(k)
            lhs = act[:, :, :, pl.ds(pl.multiple_of(k * C, C), C)].reshape(2 * half_rows, C)
            for b in range(2):
                prod = jnp.dot(lhs, w[k, :, b * width:(b + 1) * width], preferred_element_type=F32)
                z[b] = z[b] + prod.reshape(z.shape[1:])

    def multiply_half(half, n):
        @pl.loop(num_o + N1 + starts[n], num_o + N1 + starts[n + 1])
        def _(k):
            if half == 0:
                w_wait(k)
            lhs = act[half, :, :, pl.ds(pl.multiple_of(k * C, C), C)].reshape(half_rows, C)
            for b in range(2):
                prod = jnp.dot(lhs, w[k, :, b * width:(b + 1) * width], preferred_element_type=F32)
                z[b, half] = z[b, half] + prod.reshape(z.shape[2:])

    first = (late - here + 1) // 2
    for i in range(here, here + first):
        x_send(i).start()
    o_copy(yn, yi).start()
    for k in range(num_k):
        w_copy(k).start()
    z[...] = jnp.zeros_like(z)

    @pl.loop(0, here)
    def _(i):
        perm_copy(i).wait()
        activate(i)

    a1_in.wait()
    o_in.wait()
    o_copy(yi, yn).wait_recv()
    send_own(1)
    send_own(0)
    for i in range(here + first, late):
        x_send(i).start()
    ready = sum(end <= here for end in starts[1:])
    for n in range(ready):
        send_own(2 + n)

    @pl.loop(here, here + first)
    def _(i):
        x_send(i).wait_recv()
        activate(i)

    pass_on(1)
    pass_on(0)
    arrived(1)
    multiply(0, num_o)
    arrived(0)
    multiply(num_o, N1)

    @pl.loop(here + first, late)
    def _(i):
        x_send(i).wait_recv()
        activate(i)

    groups = 2 + 2 * pieces
    for e in range(2 + ready, groups):
        send_own(e)
    z_copies = [remote(z.at[yn, half], zr.at[half], z_s.at[half], z_r.at[half], yn_dev) for half in range(2)]
    pass_on(2)
    for e in range(2, groups):
        if e + 1 < groups:
            pass_on(e + 1)
        arrived(e)
        half, n = divmod(e - 2, pieces)
        multiply_half(half, n)
        if n == pieces - 1:
            z_copies[half].start()

    o_copy(yn, yi).wait_send()
    for e in range(groups):
        to_xn(e, xi).wait_send()
        to_sib(e, xi).wait_send()
        forward(e, xn).wait_send()

    @pl.loop(here, late)
    def _(i):
        x_send(i).wait_send()

    outs = [pltpu.make_async_copy(zr.at[half], z_hbm.at[:, half], out_sem.at[half]) for half in range(2)]
    for half in range(2):
        z_copies[half].wait()
        zr[half] = z[yi, half] + zr[half]
        outs[half].start()
    for half in range(2):
        outs[half].wait()


def back(x_loc, o_halves, a1, own, perm, send, wao, wmo):
    rows, width = x_loc.shape
    num_o, num_c = wao.shape[0] // C, wmo.shape[0] // C
    num_k, late = num_o + num_c, num_c - N1
    groups = 2 + 2 * len(PIECES)
    quarter = rows // 4
    dma = pltpu.SemaphoreType.DMA
    any_spec = pl.BlockSpec(memory_space=pl.ANY)
    z = pl.pallas_call(
        back_kernel,
        name="back",
        out_shape=jax.ShapeDtypeStruct((4, 2, rows // 8, width), F32),
        in_specs=[any_spec] * 7,
        out_specs=any_spec,
        scratch_shapes=[
            pltpu.VMEM((num_k, C, 2 * width), BF16),
            pltpu.VMEM((late, quarter, 2 * C), F32),
            pltpu.VMEM((late, quarter, 2 * C), F32),
            pltpu.VMEM((2, 4, rows // 8, num_k * C), BF16),
            pltpu.VMEM((2, 2, 4, rows // 8, width), F32),
            pltpu.VMEM((2, 4, rows // 8, width), F32),
            dma((2,)), dma((2,)), dma((num_k,)), dma((late,)), dma((num_c - N2,)), dma((late,)), dma, dma,
            dma((groups,)), dma((groups,)), dma((groups,)), dma((groups,)), dma((groups,)), dma((groups,)),
            dma((2,)), dma((2,)),
        ],
        compiler_params=pltpu.CompilerParams(collective_id=1, has_side_effects=True, vmem_limit_bytes=VMEM_LIMIT),
        cost_estimate=pl.CostEstimate(
            flops=4 * rows * num_k * C * width, bytes_accessed=4 * num_k * C * width, transcendentals=0
        ),
    )(o_halves, a1, own, perm, send, wao, wmo)
    return (x_loc.astype(F32) + z.reshape(rows, width)).astype(BF16)


def solution(mesh):
    x_size, yz_size = mesh.shape["x"], mesh.shape["yz"]
    both_axes = ("x", "yz")
    row_spec = P("dp", both_axes)
    in_w_spec = P("x", "yz")
    out_w_spec = P("yz", "x")
    cache_spec = P(("dp", "x", "yz"), None, None)
    len_spec = P(("dp", "x", "yz"))
    across = [(i, (i + 2) % 4) for i in range(4)]

    def local_layer(x_loc, gain_loc, wqkv_loc, wgate_loc, wup_loc, wao_loc, wmo_loc, kc_loc, vc_loc, len_loc):
        d_model = x_loc.shape[1] * x_size * yz_size
        reqs, _, head_dim = kc_loc.shape
        half = head_dim // 2
        inv_freq = 10000.0 ** (-jnp.arange(half, dtype=F32) / half)
        angles = len_loc.astype(F32)[:, None] * inv_freq
        cos, sin = jnp.cos(angles), jnp.sin(angles)
        cos = jnp.concatenate([cos, cos], axis=1)[:, None, :]
        sin = jnp.concatenate([-sin, sin], axis=1)[:, None, :]

        qkv, a1, perm, send, own = front(
            x_loc, gain_loc, wqkv_loc, wgate_loc, wup_loc, d_model
        )
        perm = lax.ppermute(perm, "x", across)
        qkv = jnp.concatenate([qkv[0], qkv[1]], axis=1).reshape(reqs, -1, head_dim)
        k_all, v_all, attn = attend(qkv, cos, sin, kc_loc, vc_loc, len_loc)
        o_halves = jnp.swapaxes(attn.reshape(reqs, 2, -1), 0, 1)
        y_loc = back(x_loc, o_halves, a1, own, perm, send, wao_loc, wmo_loc)
        return y_loc, k_all, v_all

    in_specs = (row_spec, P(both_axes), in_w_spec, in_w_spec, in_w_spec, out_w_spec, out_w_spec, cache_spec, cache_spec, len_spec)
    out_specs = (row_spec, cache_spec, cache_spec)
    return jax.shard_map(local_layer, mesh=mesh, in_specs=in_specs, out_specs=out_specs, check_vma=False)
```

```python
import functools

import jax
import jax.numpy as jnp
from jax import lax
from jax.experimental import pallas as pl
from jax.experimental.pallas import tpu as pltpu
from jax.sharding import PartitionSpec as P

MESH = pl.DeviceIdType.MESH
F32 = jnp.float32
BF16 = jnp.bfloat16
VMEM_LIMIT = 66_900_000

C = 768
CQ = 640
PER_STEP = 2
SLOTS = 3
N1 = 5
N2 = 13
FULL = 5
PIECES = (3, 3, 2, 2, 1)


def remote(src, dst, send_sem, recv_sem, device):
    return pltpu.make_async_remote_copy(
        src_ref=src, dst_ref=dst, send_sem=send_sem, recv_sem=recv_sem, device_id=device, device_id_type=MESH
    )


def places():
    xi = lax.axis_index("x")
    yi = lax.axis_index("yz")
    sib = xi + 1 - 2 * (xi % 2)
    xn = (xi + 2) % 4
    return xi, yi, sib, xn, (sib + 2) % 4, 1 - yi


def activation(total):
    gate = total[:, :C].astype(BF16).astype(F32)
    up = total[:, C:].astype(BF16).astype(F32)
    return (jax.nn.silu(gate) * up).astype(BF16)


def front_kernel(
    d_model, x_hbm, g_hbm, wq_hbm, wg_hbm, wu_hbm,
    qkv_hbm, got_hbm, perm_hbm, send_hbm, own_hbm,
    stat, xbuf, gain, gbuf, moments, h, wq, wg, wu, pq, rq, xq, qs, qd, p, r,
    in_sem, wq_sem, wg_sem, wu_sem, st_s, st_r, xg_s, xg_r,
    dq_s, dq_r, xq_s, xq_r, yq_s, yq_r, d_s, d_r, x_s, x_r, out_sem, own_sem, q_sem,
):
    xi, yi, sib, xn, sibn, yn = places()
    me = yi * 4 + xi
    sides, side_rows, width = x_hbm.shape
    rows = sides * side_rows
    near = xi // 2
    far = 1 - near
    num_q = wq_hbm.shape[1] // CQ
    num_c = wg_hbm.shape[1] // C
    sib_dev, xn_dev, yn_dev = {"x": sib}, {"x": xn}, {"yz": yn}

    def wq_copy(c):
        return pltpu.make_async_copy(wq_hbm.at[:, pl.ds(c * CQ, CQ)], wq.at[c], wq_sem.at[c])

    def w_copies(i, slot):
        start = pl.multiple_of(i * C, C)
        return (
            pltpu.make_async_copy(wg_hbm.at[:, pl.ds(start, C)], wg.at[slot], wg_sem.at[slot]),
            pltpu.make_async_copy(wu_hbm.at[:, pl.ds(start, C)], wu.at[slot], wu_sem.at[slot]),
        )

    x_in = pltpu.make_async_copy(x_hbm, xbuf.at[yi], in_sem.at[0])
    g_in = pltpu.make_async_copy(g_hbm, gain, in_sem.at[1])
    x_in.start()
    g_in.start()
    barrier = pltpu.get_barrier_semaphore()
    offsets = [(dy, dx) for dy in range(2) for dx in range(4)][1:]
    for dy, dx in offsets:
        pl.semaphore_signal(barrier, inc=1, device_id={"yz": (yi + dy) % 2, "x": (xi + dx) % 4}, device_id_type=MESH)

    x_in.wait()
    x_f32 = xbuf[yi].reshape(rows, width).astype(F32)
    lane = lax.broadcasted_iota(jnp.int32, (rows, rows), 1)
    sums = jnp.where(
        lane == 0,
        jnp.sum(x_f32, axis=1, keepdims=True),
        jnp.where(lane == 1, jnp.sum(x_f32 * x_f32, axis=1, keepdims=True), 0.0),
    )
    stat[me] = sums.T[0:8, :]
    g_in.wait()
    gbuf[yi] = jnp.broadcast_to(gain[...].astype(F32)[None, :], (8, width))
    pl.semaphore_wait(barrier, 7)

    def stat_copy(k, slot):
        dy, dx = offsets[k]
        dev = {"yz": (yi + dy) % 2, "x": (xi + dx) % 4}
        return remote(stat.at[slot], stat.at[slot], st_s.at[k], st_r.at[k], dev)

    def x_copies(slot):
        return [
            remote(xbuf.at[slot, side], xbuf.at[slot, side], xg_s.at[1 + n], xg_r.at[1 + n], yn_dev)
            for n, side in enumerate((far, near))
        ]

    def g_copy(slot):
        return remote(gbuf.at[slot], gbuf.at[slot], xg_s.at[0], xg_r.at[0], yn_dev)

    for k in range(7):
        stat_copy(k, me).start()
    g_copy(yi).start()
    for copy in x_copies(yi):
        copy.start()
    for c in range(num_q):
        wq_copy(c).start()
    for i in range(SLOTS):
        for copy in w_copies(i, i):
            copy.start()
    for k, (dy, dx) in enumerate(offsets):
        stat_copy(k, ((yi + 2 - dy) % 2) * 4 + (xi + 4 - dx) % 4).wait_recv()
    total = stat[0]
    for k in range(1, 8):
        total = total + stat[k]
    cols = jnp.concatenate([total, jnp.zeros((rows - 8, rows), F32)], axis=0).T
    mean = cols[:, 0:1] / d_model
    var = cols[:, 1:2] / d_model - mean * mean
    moments[0] = jnp.broadcast_to(mean, (rows, 128)).reshape(sides, side_rows, 128)
    moments[1] = jnp.broadcast_to(lax.rsqrt(var + 1e-6), (rows, 128)).reshape(sides, side_rows, 128)
    g_copy(yn).wait_recv()

    def normalize(side):
        for b in range(2):
            part = (xbuf[b, side].astype(F32) - moments[0, side][:, 0:1]) * moments[1, side][:, 0:1]
            h[side, :, b * width:(b + 1) * width] = (part * gbuf[b][0:1, :]).astype(BF16)

    def dq(c, k):
        src = sib if k == 0 else sibn
        return remote(pq.at[c, src], rq.at[c, k], dq_s.at[c, k], dq_r.at[c, k], sib_dev)

    def xq_copy(c):
        return remote(pq.at[c, xn], xq.at[c], xq_s.at[c], xq_r.at[c], xn_dev)

    def q_product(c, side):
        prod = jnp.dot(h[side], wq[c], preferred_element_type=F32)
        pq[c, pl.ds(2 * side, 2)] = prod.reshape(2, rows // 4, CQ)

    def q_send(c):
        dq(c, 1).wait_recv()
        dq(c, 1).wait_send()
        pq[c, xn] = pq[c, xn] + rq[c, 1]
        xq_copy(c).start()

    x_copies(yn)[0].wait_recv()
    normalize(far)

    @pl.loop(0, num_q)
    def _(c):
        wq_copy(c).wait()
        q_product(c, far)
        dq(c, 1).start()

        @pl.when(c >= 1)
        def _():
            q_send(c - 1)

    x_copies(yn)[1].wait_recv()
    normalize(near)
    q_send(num_q - 1)

    @pl.loop(0, num_q)
    def _(c):
        q_product(c, near)
        dq(c, 0).start()

    def d_copy(i, k):
        src = sib if k == 0 else sibn
        return remote(p.at[i, src], r.at[i, k], d_s.at[i, k], d_r.at[i, k], sib_dev)

    def x_send(i):
        return remote(p.at[i, xn], got_hbm.at[i], x_s.at[i], x_r.at[i], xn_dev)

    def perm_copy(i):
        return pltpu.make_async_copy(p.at[i, xn], perm_hbm.at[i - N1], out_sem.at[i])

    def send_copy(i):
        return pltpu.make_async_copy(p.at[i, xn], send_hbm.at[i - N2], out_sem.at[i])

    def own_copy(i):
        return pltpu.make_async_copy(p.at[i, xi], own_hbm.at[i], own_sem.at[i])

    def chip_sum(i):
        d_copy(i, 1).wait_recv()
        d_copy(i, 1).wait_send()
        p[i, xn] = p[i, xn] + r[i, 1]

        @pl.when(i < N1)
        def _():
            x_send(i).start()

        @pl.when((i >= N1) & (i < N2))
        def _():
            perm_copy(i).start()

        @pl.when(i >= N2)
        def _():
            send_copy(i).start()

        d_copy(i, 0).wait_recv()
        d_copy(i, 0).wait_send()
        p[i, xi] = p[i, xi] + r[i, 0]
        own_copy(i).start()

    def product(i):
        slot = i % SLOTS
        g_w, u_w = w_copies(i, slot)
        h_all = h[...].reshape(rows, h.shape[2])
        g_w.wait()
        p[i, :, :, :C] = jnp.dot(h_all, wg[slot], preferred_element_type=F32).reshape(4, rows // 4, C)
        u_w.wait()
        p[i, :, :, C:] = jnp.dot(h_all, wu[slot], preferred_element_type=F32).reshape(4, rows // 4, C)
        d_copy(i, 1).start()
        d_copy(i, 0).start()

        @pl.when(i + SLOTS < num_c)
        def _():
            for copy in w_copies(i + SLOTS, slot):
                copy.start()

    product(0)

    def step(i):
        product(i)
        chip_sum(i - 1)

    half = num_c // 2 + 1
    pl.loop(1, half)(step)

    @pl.loop(0, num_q)
    def _(c):
        dq(c, 0).wait_recv()
        dq(c, 0).wait_send()
        mine = pq[c, xi] + rq[c, 0]
        xq_copy(c).wait_recv()
        xq_copy(c).wait_send()
        value = (mine + xq[c]).astype(BF16)
        qs[:, :, pl.ds(pl.multiple_of(c * CQ, CQ), CQ)] = value.reshape(2, rows // 8, CQ)

    def yq_copy(k):
        return remote(qs.at[1 - k], qd.at[k], yq_s, yq_r, yn_dev)

    yq_copy(yi).start()
    qd[yi] = qs[yi]

    pl.loop(half, num_c)(step)
    chip_sum(num_c - 1)
    yq_copy(yn).wait_recv()
    q_out = pltpu.make_async_copy(qd, qkv_hbm, q_sem)
    q_out.start()

    for k in range(7):
        stat_copy(k, me).wait_send()
    g_copy(yi).wait_send()
    for copy in x_copies(yi):
        copy.wait_send()
    yq_copy(yi).wait_send()

    @pl.loop(0, num_c)
    def _(i):
        own_copy(i).wait()

    @pl.loop(N1, N2)
    def _(i):
        perm_copy(i).wait()

    @pl.loop(N2, num_c)
    def _(i):
        send_copy(i).wait()

    q_out.wait()

    @pl.loop(0, N1)
    def _(i):
        x_send(i).wait()


def front(x_loc, gain_loc, wqkv, wgate, wup, d_model):
    rows, width = x_loc.shape
    depth, q_cols = wqkv.shape
    num_q, num_c = q_cols // CQ, wgate.shape[1] // C
    quarter = rows // 4
    dma = pltpu.SemaphoreType.DMA
    any_spec = pl.BlockSpec(memory_space=pl.ANY)
    return pl.pallas_call(
        functools.partial(front_kernel, d_model),
        name="front",
        out_shape=(
            jax.ShapeDtypeStruct((2, rows // 8, q_cols), BF16),
            jax.ShapeDtypeStruct((N1, quarter, 2 * C), F32),
            jax.ShapeDtypeStruct((N2 - N1, quarter, 2 * C), F32),
            jax.ShapeDtypeStruct((num_c - N2, quarter, 2 * C), F32),
            jax.ShapeDtypeStruct((num_c, quarter, 2 * C), F32),
        ),
        in_specs=[any_spec] * 5,
        out_specs=(any_spec,) * 5,
        scratch_shapes=[
            pltpu.VMEM((8, 8, rows), F32),
            pltpu.VMEM((2, 2, rows // 2, width), BF16),
            pltpu.VMEM((width,), BF16),
            pltpu.VMEM((2, 8, width), F32),
            pltpu.VMEM((2, 2, rows // 2, 128), F32),
            pltpu.VMEM((2, rows // 2, depth), BF16),
            pltpu.VMEM((num_q, depth, CQ), BF16),
            pltpu.VMEM((SLOTS, depth, C), BF16),
            pltpu.VMEM((SLOTS, depth, C), BF16),
            pltpu.VMEM((num_q, 4, quarter, CQ), F32),
            pltpu.VMEM((num_q, 2, quarter, CQ), F32),
            pltpu.VMEM((num_q, quarter, CQ), F32),
            pltpu.VMEM((2, rows // 8, q_cols), BF16),
            pltpu.VMEM((2, rows // 8, q_cols), BF16),
            pltpu.VMEM((num_c, 4, quarter, 2 * C), F32),
            pltpu.VMEM((num_c, 2, quarter, 2 * C), F32),
            dma((2,)), dma((num_q,)), dma((SLOTS,)), dma((SLOTS,)), dma((7,)), dma((7,)), dma((3,)), dma((3,)),
            dma((num_q, 2)), dma((num_q, 2)), dma((num_q,)), dma((num_q,)), dma, dma,
            dma((num_c, 2)), dma((num_c, 2)), dma((N1,)), dma((N1,)), dma((num_c,)), dma((num_c,)), dma,
        ],
        compiler_params=pltpu.CompilerParams(collective_id=0, has_side_effects=True, vmem_limit_bytes=VMEM_LIMIT),
        cost_estimate=pl.CostEstimate(
            flops=2 * rows * depth * (q_cols + 2 * wgate.shape[1]),
            bytes_accessed=2 * depth * (q_cols + 2 * wgate.shape[1]),
            transcendentals=0,
        ),
    )(x_loc.reshape(2, rows // 2, width), gain_loc, wqkv, wgate, wup)


def attend_kernel(len_ref, qkv_ref, cos_ref, sin_ref, k_ref, v_ref, ko_ref, vo_ref, o_ref):
    ko_ref[...] = k_ref[...]
    vo_ref[...] = v_ref[...]
    for n in range(PER_STEP):
        pos = len_ref[pl.program_id(0) * PER_STEP + n]
        qkv = qkv_ref[n]
        heads, head_dim = qkv.shape[0] - 2, qkv.shape[1]
        wide = qkv.astype(F32)
        turned = (wide * cos_ref[n] + pltpu.roll(wide, head_dim // 2, 1) * sin_ref[n]).astype(BF16)
        query = turned[:heads]
        base = pl.multiple_of((pos // 16) * 16, 16)
        here = lax.broadcasted_iota(jnp.int32, (16, head_dim), 0) == pos - base
        for out, new in ((ko_ref, turned[heads:heads + 1]), (vo_ref, qkv[heads + 1:heads + 2])):
            tile = out[n, pl.ds(base, 16), :].astype(F32)
            out[n, pl.ds(base, 16), :] = jnp.where(here, new.astype(F32), tile).astype(BF16)
        scores = lax.dot_general(query, ko_ref[n], (((1,), (1,)), ((), ())), preferred_element_type=F32)
        scores = scores * head_dim ** -0.5
        at = lax.broadcasted_iota(jnp.int32, scores.shape, 1)
        scores = jnp.where(at <= pos, scores, -1e30)
        weight = jnp.exp(scores - jnp.max(scores, axis=1, keepdims=True))
        probs = (weight / jnp.sum(weight, axis=1, keepdims=True)).astype(BF16)
        o_ref[n] = jnp.dot(probs, vo_ref[n], preferred_element_type=F32).astype(BF16)


def attend(qkv, cos, sin, k_cache, v_cache, ctx_len):
    reqs, length, head_dim = k_cache.shape
    heads = qkv.shape[1] - 2
    cache_spec = pl.BlockSpec((PER_STEP, length, head_dim), lambda i, lens: (i, 0, 0))
    table_spec = pl.BlockSpec((PER_STEP, 1, head_dim), lambda i, lens: (i, 0, 0))
    return pl.pallas_call(
        attend_kernel,
        name="attend",
        grid_spec=pltpu.PrefetchScalarGridSpec(
            num_scalar_prefetch=1,
            grid=(reqs // PER_STEP,),
            in_specs=[
                pl.BlockSpec((PER_STEP, heads + 2, head_dim), lambda i, lens: (i, 0, 0)),
                table_spec, table_spec, cache_spec, cache_spec,
            ],
            out_specs=[cache_spec, cache_spec, pl.BlockSpec((PER_STEP, heads, head_dim), lambda i, lens: (i, 0, 0))],
        ),
        out_shape=(
            jax.ShapeDtypeStruct(k_cache.shape, BF16),
            jax.ShapeDtypeStruct(v_cache.shape, BF16),
            jax.ShapeDtypeStruct((reqs, heads, head_dim), BF16),
        ),
        compiler_params=pltpu.CompilerParams(dimension_semantics=("arbitrary",)),
        cost_estimate=pl.CostEstimate(
            flops=64 * reqs * heads * length * head_dim,
            bytes_accessed=8 * reqs * length * head_dim,
            transcendentals=reqs * heads * length,
        ),
    )(ctx_len, qkv, cos, sin, k_cache, v_cache)


def back_kernel(
    o_hbm, own_hbm, got_hbm, perm_hbm, send_hbm, wao_hbm, wmo_hbm, z_out,
    w, own, xr, xs, act, z, zr,
    in_sem, w_sem, own_sem, x_s, x_r, o_s, o_r, sib_s, sib_r, xn_s, xn_r, fwd_s, fwd_r, z_s, z_r,
):
    xi, yi, sib, xn, _, yn = places()
    sib_dev, xn_dev, yn_dev = {"x": sib}, {"x": xn}, {"yz": yn}
    width = z_out.shape[3]
    half_rows = act.shape[1] * act.shape[2]
    num_o, num_c = wao_hbm.shape[0] // C, wmo_hbm.shape[0] // C
    num_k = num_o + num_c
    o_cols = wao_hbm.shape[0]
    pieces = len(PIECES)
    starts = [FULL + sum(PIECES[:n]) for n in range(pieces + 1)]

    def w_copy(k):
        src = wao_hbm.at[pl.ds(k * C, C), :] if k < num_o else wmo_hbm.at[pl.ds((k - num_o) * C, C), :]
        return pltpu.make_async_copy(src, w.at[k], w_sem.at[k])

    def own_copy(i):
        return pltpu.make_async_copy(own_hbm.at[i], own.at[i], own_sem.at[i])

    def here_copy(i):
        src = got_hbm.at[i] if i < N1 else perm_hbm.at[i - N1]
        return pltpu.make_async_copy(src, xr.at[i], x_r.at[i])

    def x_send(i):
        return remote(xs.at[i - N2], xr.at[i], x_s.at[i - N2], x_r.at[i], xn_dev)

    barrier = pltpu.get_barrier_semaphore()
    for dev in (sib_dev, xn_dev, yn_dev):
        pl.semaphore_signal(barrier, inc=1, device_id=dev, device_id_type=MESH)
    xs_in = pltpu.make_async_copy(send_hbm, xs, in_sem.at[1])
    xs_in.start()
    o_in = pltpu.make_async_copy(o_hbm.at[yi], act.at[yi, xi, :, 0:o_cols], in_sem.at[0])
    o_in.start()
    for i in range(N2):
        own_copy(i).start()
        here_copy(i).start()
    for i in range(N2, num_c):
        own_copy(i).start()
    xs_in.wait()
    pl.semaphore_wait(barrier, 3)

    def o_copy(half, row):
        return remote(o_hbm.at[half], act.at[row, xi, :, 0:o_cols], o_s, o_r, yn_dev)

    def block_of(e, owner):
        if e == 0:
            return act.at[:, owner, :, pl.ds(o_cols, FULL * C)]
        if e == 1:
            return act.at[:, owner, :, pl.ds(0, o_cols)]
        half, n = divmod(e - 2, pieces)
        return act.at[half, owner, :, pl.ds(o_cols + starts[n] * C, PIECES[n] * C)]

    def to_sib(e, owner):
        block = block_of(e, owner)
        return remote(block, block, sib_s.at[e], sib_r.at[e], sib_dev)

    def to_xn(e, owner):
        block = block_of(e, owner)
        return remote(block, block, xn_s.at[e], xn_r.at[e], xn_dev)

    def forward(e, owner):
        block = block_of(e, owner)
        return remote(block, block, fwd_s.at[e], fwd_r.at[e], sib_dev)

    def send_own(e):
        to_xn(e, xi).start()
        to_sib(e, xi).start()

    def pass_on(e):
        to_xn(e, xn).wait_recv()
        forward(e, xn).start()

    def arrived(e):
        to_sib(e, sib).wait_recv()
        forward(e, (sib + 2) % 4).wait_recv()

    def activate(i):
        own_copy(i).wait()
        value = activation(own[i] + xr[i])
        start = pl.multiple_of(o_cols + i * C, C)
        act[:, xi, :, pl.ds(start, C)] = value.reshape(2, value.shape[0] // 2, C)

    def w_wait(k):
        pltpu.make_async_copy(wmo_hbm.at[pl.ds(0, C), :], w.at[k], w_sem.at[k]).wait()

    def multiply(first, count):
        @pl.loop(first, first + count)
        def _(k):
            w_wait(k)
            lhs = act[:, :, :, pl.ds(pl.multiple_of(k * C, C), C)].reshape(2 * half_rows, C)
            for b in range(2):
                prod = jnp.dot(lhs, w[k, :, b * width:(b + 1) * width], preferred_element_type=F32)
                z[b] = z[b] + prod.reshape(z.shape[1:])

    def multiply_one(half, n, b):
        @pl.loop(num_o + starts[n], num_o + starts[n + 1])
        def _(k):
            lhs = act[half, :, :, pl.ds(pl.multiple_of(k * C, C), C)].reshape(half_rows, C)
            cols = pl.ds(pl.multiple_of(b * width, width), width)
            prod = jnp.dot(lhs, w[k, :, cols], preferred_element_type=F32)
            z[b, half] = z[b, half] + prod.reshape(z.shape[2:])

    def multiply_half(half, n):
        @pl.loop(num_o + starts[n], num_o + starts[n + 1])
        def _(k):
            if half == 0:
                w_wait(k)
            lhs = act[half, :, :, pl.ds(pl.multiple_of(k * C, C), C)].reshape(half_rows, C)
            for b in range(2):
                prod = jnp.dot(lhs, w[k, :, b * width:(b + 1) * width], preferred_element_type=F32)
                z[b, half] = z[b, half] + prod.reshape(z.shape[2:])

    first = (num_c - N2 + 1) // 2
    for i in range(N2, N2 + first):
        x_send(i).start()
    o_copy(yn, yi).start()
    for k in range(num_k):
        w_copy(k).start()
    z[...] = jnp.zeros_like(z)

    def start_here(i):
        pltpu.make_async_copy(got_hbm.at[0], xr.at[i], x_r.at[i]).wait()
        activate(i)

    pl.loop(0, FULL)(start_here)
    o_in.wait()
    o_copy(yi, yn).wait_recv()
    send_own(1)
    for i in range(N2 + first, num_c):
        x_send(i).start()
    send_own(0)
    pl.loop(FULL, N2)(start_here)
    ready = sum(end <= N2 for end in starts[1:])
    for n in range(ready):
        send_own(2 + n)

    @pl.loop(N2, N2 + first)
    def _(i):
        x_send(i).wait_recv()
        activate(i)

    pass_on(1)
    arrived(1)
    multiply(0, num_o)

    @pl.loop(N2 + first, num_c)
    def _(i):
        x_send(i).wait_recv()
        activate(i)

    groups = 2 + 2 * pieces
    for e in range(2 + ready, groups):
        send_own(e)
    pass_on(0)
    arrived(0)
    multiply(num_o, FULL)
    z_copies = [remote(z.at[yn, half], zr.at[half], z_s.at[half], z_r.at[half], yn_dev) for half in range(2)]
    pass_on(2)
    for e in range(2, groups):
        if e + 1 < groups:
            pass_on(e + 1)
        arrived(e)
        half, n = divmod(e - 2, pieces)
        if e + 1 < groups:
            multiply_half(half, n)
        else:
            multiply_one(half, n, yn)
        if n == pieces - 1:
            z_copies[half].start()
    multiply_one(1, pieces - 1, yi)

    o_copy(yn, yi).wait_send()
    for e in range(groups):
        to_xn(e, xi).wait_send()
        to_sib(e, xi).wait_send()
        forward(e, xn).wait_send()

    @pl.loop(N2, num_c)
    def _(i):
        x_send(i).wait_send()

    for half in range(2):
        z_copies[half].wait()
        z_out[:, half] = z[yi, half] + zr[half]


def back(x_loc, o_halves, own, got, perm, send, wao, wmo):
    rows, width = x_loc.shape
    num_o, num_c = wao.shape[0] // C, wmo.shape[0] // C
    num_k = num_o + num_c
    groups = 2 + 2 * len(PIECES)
    quarter = rows // 4
    dma = pltpu.SemaphoreType.DMA
    any_spec = pl.BlockSpec(memory_space=pl.ANY)
    z = pl.pallas_call(
        back_kernel,
        name="back",
        out_shape=jax.ShapeDtypeStruct((4, 2, rows // 8, width), F32),
        in_specs=[any_spec] * 7,
        out_specs=pl.BlockSpec(memory_space=pltpu.VMEM),
        scratch_shapes=[
            pltpu.VMEM((num_k, C, 2 * width), BF16),
            pltpu.VMEM((num_c, quarter, 2 * C), F32),
            pltpu.VMEM((num_c, quarter, 2 * C), F32),
            pltpu.VMEM((num_c - N2, quarter, 2 * C), F32),
            pltpu.VMEM((2, 4, rows // 8, num_k * C), BF16),
            pltpu.VMEM((2, 2, 4, rows // 8, width), F32),
            pltpu.VMEM((2, 4, rows // 8, width), F32),
            dma((2,)), dma((num_k,)), dma((num_c,)), dma((num_c - N2,)), dma((num_c,)), dma, dma,
            dma((groups,)), dma((groups,)), dma((groups,)), dma((groups,)), dma((groups,)), dma((groups,)),
            dma((2,)), dma((2,)),
        ],
        compiler_params=pltpu.CompilerParams(collective_id=1, has_side_effects=True, vmem_limit_bytes=VMEM_LIMIT),
        cost_estimate=pl.CostEstimate(
            flops=4 * rows * num_k * C * width, bytes_accessed=4 * num_k * C * width, transcendentals=0
        ),
    )(o_halves, own, got, perm, send, wao, wmo)
    return (x_loc.astype(F32) + z.reshape(rows, width)).astype(BF16)


def solution(mesh):
    x_size, yz_size = mesh.shape["x"], mesh.shape["yz"]
    both_axes = ("x", "yz")
    row_spec = P("dp", both_axes)
    in_w_spec = P("x", "yz")
    out_w_spec = P("yz", "x")
    cache_spec = P(("dp", "x", "yz"), None, None)
    len_spec = P(("dp", "x", "yz"))
    across = [(i, (i + 2) % 4) for i in range(4)]

    def local_layer(x_loc, gain_loc, wqkv_loc, wgate_loc, wup_loc, wao_loc, wmo_loc, kc_loc, vc_loc, len_loc):
        d_model = x_loc.shape[1] * x_size * yz_size
        reqs, _, head_dim = kc_loc.shape
        half = head_dim // 2
        inv_freq = 10000.0 ** (-jnp.arange(half, dtype=F32) / half)
        angles = len_loc.astype(F32)[:, None] * inv_freq
        cos, sin = jnp.cos(angles), jnp.sin(angles)
        cos = jnp.concatenate([cos, cos], axis=1)[:, None, :]
        sin = jnp.concatenate([-sin, sin], axis=1)[:, None, :]

        qkv, got, perm, send, own = front(
            x_loc, gain_loc, wqkv_loc, wgate_loc, wup_loc, d_model
        )
        perm = lax.ppermute(perm, "x", across)
        qkv = jnp.concatenate([qkv[0], qkv[1]], axis=1).reshape(reqs, -1, head_dim)
        k_all, v_all, attn = attend(qkv, cos, sin, kc_loc, vc_loc, len_loc)
        o_halves = jnp.swapaxes(attn.reshape(reqs, 2, -1), 0, 1)
        y_loc = back(x_loc, o_halves, own, got, perm, send, wao_loc, wmo_loc)
        return y_loc, k_all, v_all

    in_specs = (row_spec, P(both_axes), in_w_spec, in_w_spec, in_w_spec, out_w_spec, out_w_spec, cache_spec, cache_spec, len_spec)
    out_specs = (row_spec, cache_spec, cache_spec)
    return jax.shard_map(local_layer, mesh=mesh, in_specs=in_specs, out_specs=out_specs, check_vma=False)
```

```python
import functools

import jax
import jax.numpy as jnp
from jax import lax
from jax.experimental import pallas as pl
from jax.experimental.pallas import tpu as pltpu
from jax.sharding import PartitionSpec as P

MESH = pl.DeviceIdType.MESH
F32 = jnp.float32
BF16 = jnp.bfloat16
VMEM_LIMIT = 66_900_000

C = 768
CQ = 640
PER_STEP = 2
SLOTS = 3
N1 = 5
N2 = 13
FULL = 5
PIECES = (3, 3, 2, 2, 1)


def remote(src, dst, send_sem, recv_sem, device):
    return pltpu.make_async_remote_copy(
        src_ref=src, dst_ref=dst, send_sem=send_sem, recv_sem=recv_sem, device_id=device, device_id_type=MESH
    )


def places():
    xi = lax.axis_index("x")
    yi = lax.axis_index("yz")
    sib = xi + 1 - 2 * (xi % 2)
    xn = (xi + 2) % 4
    return xi, yi, sib, xn, (sib + 2) % 4, 1 - yi


def activation(total):
    gate = total[:, :C].astype(BF16).astype(F32)
    up = total[:, C:].astype(BF16).astype(F32)
    return (jax.nn.silu(gate) * up).astype(BF16)


def front_kernel(
    d_model, x_hbm, g_hbm, wq_hbm, wg_hbm, wu_hbm,
    qkv_hbm, got_hbm, perm_hbm, send_hbm, own_hbm,
    stat, xbuf, gain, gbuf, moments, h, wq, wg, wu, pq, rq, xq, qs, qd, p, r,
    in_sem, wq_sem, wg_sem, wu_sem, st_s, st_r, xg_s, xg_r,
    dq_s, dq_r, xq_s, xq_r, yq_s, yq_r, d_s, d_r, x_s, x_r, out_sem, own_sem, q_sem,
):
    xi, yi, sib, xn, sibn, yn = places()
    me = yi * 4 + xi
    sides, side_rows, width = x_hbm.shape
    rows = sides * side_rows
    near = xi // 2
    far = 1 - near
    num_q = wq_hbm.shape[1] // CQ
    num_c = wg_hbm.shape[1] // C
    sib_dev, xn_dev, yn_dev = {"x": sib}, {"x": xn}, {"yz": yn}

    def wq_copy(c):
        return pltpu.make_async_copy(wq_hbm.at[:, pl.ds(c * CQ, CQ)], wq.at[c], wq_sem.at[c])

    def w_copies(i, slot):
        start = pl.multiple_of(i * C, C)
        return (
            pltpu.make_async_copy(wg_hbm.at[:, pl.ds(start, C)], wg.at[slot], wg_sem.at[slot]),
            pltpu.make_async_copy(wu_hbm.at[:, pl.ds(start, C)], wu.at[slot], wu_sem.at[slot]),
        )

    x_in = pltpu.make_async_copy(x_hbm, xbuf.at[yi], in_sem.at[0])
    g_in = pltpu.make_async_copy(g_hbm, gain, in_sem.at[1])
    x_in.start()
    g_in.start()
    barrier = pltpu.get_barrier_semaphore()
    offsets = [(dy, dx) for dy in range(2) for dx in range(4)][1:]
    for dy, dx in offsets:
        pl.semaphore_signal(barrier, inc=1, device_id={"yz": (yi + dy) % 2, "x": (xi + dx) % 4}, device_id_type=MESH)

    x_in.wait()
    x_f32 = xbuf[yi].reshape(rows, width).astype(F32)
    lane = lax.broadcasted_iota(jnp.int32, (rows, rows), 1)
    sums = jnp.where(
        lane == 0,
        jnp.sum(x_f32, axis=1, keepdims=True),
        jnp.where(lane == 1, jnp.sum(x_f32 * x_f32, axis=1, keepdims=True), 0.0),
    )
    stat[me] = sums.T[0:8, :]
    g_in.wait()
    gbuf[yi] = jnp.broadcast_to(gain[...].astype(F32)[None, :], (8, width))
    pl.semaphore_wait(barrier, 7)

    def stat_copy(k, slot):
        dy, dx = offsets[k]
        dev = {"yz": (yi + dy) % 2, "x": (xi + dx) % 4}
        return remote(stat.at[slot], stat.at[slot], st_s.at[k], st_r.at[k], dev)

    def x_copy(slot, n):
        block = xbuf.at[slot, (far, near)[n]]
        return remote(block, block, xg_s.at[1 + n], xg_r.at[1 + n], yn_dev)

    def g_copy(slot):
        return remote(gbuf.at[slot], gbuf.at[slot], xg_s.at[0], xg_r.at[0], yn_dev)

    for k in range(7):
        stat_copy(k, me).start()
    g_copy(yi).start()
    x_copy(yi, 0).start()
    x_copy(yi, 1).start()
    for c in range(num_q):
        wq_copy(c).start()
    for i in range(SLOTS):
        for copy in w_copies(i, i):
            copy.start()
    for k, (dy, dx) in enumerate(offsets):
        stat_copy(k, ((yi + 2 - dy) % 2) * 4 + (xi + 4 - dx) % 4).wait_recv()
    total = stat[0]
    for k in range(1, 8):
        total = total + stat[k]
    cols = jnp.concatenate([total, jnp.zeros((rows - 8, rows), F32)], axis=0).T
    mean = cols[:, 0:1] / d_model
    var = cols[:, 1:2] / d_model - mean * mean
    moments[0] = jnp.broadcast_to(mean, (rows, 128)).reshape(sides, side_rows, 128)
    moments[1] = jnp.broadcast_to(lax.rsqrt(var + 1e-6), (rows, 128)).reshape(sides, side_rows, 128)
    g_copy(yn).wait_recv()

    def normalize(side):
        for b in range(2):
            part = (xbuf[b, side].astype(F32) - moments[0, side][:, 0:1]) * moments[1, side][:, 0:1]
            h[side, :, b * width:(b + 1) * width] = (part * gbuf[b][0:1, :]).astype(BF16)

    def dq(c, k):
        src = sib if k == 0 else sibn
        return remote(pq.at[c, src], rq.at[c, k], dq_s.at[c, k], dq_r.at[c, k], sib_dev)

    def xq_copy(c):
        return remote(pq.at[c, xn], xq.at[c], xq_s.at[c], xq_r.at[c], xn_dev)

    def q_product(c, side):
        prod = jnp.dot(h[side], wq[c], preferred_element_type=F32)
        pq[c, pl.ds(2 * side, 2)] = prod.reshape(2, rows // 4, CQ)

    def q_send(c):
        dq(c, 1).wait_recv()
        dq(c, 1).wait_send()
        pq[c, xn] = pq[c, xn] + rq[c, 1]
        xq_copy(c).start()

    x_copy(yn, 0).wait_recv()
    normalize(far)

    @pl.loop(0, num_q)
    def _(c):
        wq_copy(c).wait()
        q_product(c, far)
        dq(c, 1).start()

        @pl.when(c >= 1)
        def _():
            q_send(c - 1)

    x_copy(yn, 1).wait_recv()
    normalize(near)
    q_send(num_q - 1)

    @pl.loop(0, num_q)
    def _(c):
        q_product(c, near)
        dq(c, 0).start()

    def d_copy(i, k):
        src = sib if k == 0 else sibn
        return remote(p.at[i, src], r.at[i, k], d_s.at[i, k], d_r.at[i, k], sib_dev)

    def x_send(i):
        return remote(p.at[i, xn], got_hbm.at[i], x_s.at[i], x_r.at[i], xn_dev)

    def perm_copy(i):
        return pltpu.make_async_copy(p.at[i, xn], perm_hbm.at[i - N1], out_sem.at[i])

    def send_copy(i):
        return pltpu.make_async_copy(p.at[i, xn], send_hbm.at[i - N2], out_sem.at[i])

    def own_copy(i):
        return pltpu.make_async_copy(p.at[i, xi], own_hbm.at[i], own_sem.at[i])

    def chip_sum(i):
        d_copy(i, 1).wait_recv()
        d_copy(i, 1).wait_send()
        p[i, xn] = p[i, xn] + r[i, 1]

        @pl.when(i < N1)
        def _():
            x_send(i).start()

        @pl.when((i >= N1) & (i < N2))
        def _():
            perm_copy(i).start()

        @pl.when(i >= N2)
        def _():
            send_copy(i).start()

        d_copy(i, 0).wait_recv()
        d_copy(i, 0).wait_send()
        p[i, xi] = p[i, xi] + r[i, 0]
        own_copy(i).start()

    def product(i):
        slot = i % SLOTS
        g_w, u_w = w_copies(i, slot)
        h_all = h[...].reshape(rows, h.shape[2])
        g_w.wait()
        p[i, :, :, :C] = jnp.dot(h_all, wg[slot], preferred_element_type=F32).reshape(4, rows // 4, C)
        u_w.wait()
        p[i, :, :, C:] = jnp.dot(h_all, wu[slot], preferred_element_type=F32).reshape(4, rows // 4, C)
        d_copy(i, 1).start()
        d_copy(i, 0).start()

        @pl.when(i + SLOTS < num_c)
        def _():
            for copy in w_copies(i + SLOTS, slot):
                copy.start()

    product(0)

    def step(i):
        product(i)
        chip_sum(i - 1)

    half = num_c // 2 + 1
    pl.loop(1, half)(step)

    @pl.loop(0, num_q)
    def _(c):
        dq(c, 0).wait_recv()
        dq(c, 0).wait_send()
        mine = pq[c, xi] + rq[c, 0]
        xq_copy(c).wait_recv()
        xq_copy(c).wait_send()
        value = (mine + xq[c]).astype(BF16)
        qs[:, :, pl.ds(pl.multiple_of(c * CQ, CQ), CQ)] = value.reshape(2, rows // 8, CQ)

    def yq_copy(k):
        return remote(qs.at[1 - k], qd.at[k], yq_s, yq_r, yn_dev)

    yq_copy(yi).start()
    qd[yi] = qs[yi]

    pl.loop(half, num_c)(step)
    chip_sum(num_c - 1)
    yq_copy(yn).wait_recv()
    q_out = pltpu.make_async_copy(qd, qkv_hbm, q_sem)
    q_out.start()

    for k in range(7):
        stat_copy(k, me).wait_send()
    g_copy(yi).wait_send()
    x_copy(yi, 0).wait_send()
    x_copy(yi, 1).wait_send()
    yq_copy(yi).wait_send()

    @pl.loop(0, num_c)
    def _(i):
        own_copy(i).wait()

    @pl.loop(N1, N2)
    def _(i):
        perm_copy(i).wait()

    @pl.loop(N2, num_c)
    def _(i):
        send_copy(i).wait()

    q_out.wait()

    @pl.loop(0, N1)
    def _(i):
        x_send(i).wait()


def front(x_loc, gain_loc, wqkv, wgate, wup, d_model):
    rows, width = x_loc.shape
    depth, q_cols = wqkv.shape
    num_q, num_c = q_cols // CQ, wgate.shape[1] // C
    quarter = rows // 4
    dma = pltpu.SemaphoreType.DMA
    any_spec = pl.BlockSpec(memory_space=pl.ANY)
    return pl.pallas_call(
        functools.partial(front_kernel, d_model),
        name="front",
        out_shape=(
            jax.ShapeDtypeStruct((2, rows // 8, q_cols), BF16),
            jax.ShapeDtypeStruct((N1, quarter, 2 * C), F32),
            jax.ShapeDtypeStruct((N2 - N1, quarter, 2 * C), F32),
            jax.ShapeDtypeStruct((num_c - N2, quarter, 2 * C), F32),
            jax.ShapeDtypeStruct((num_c, quarter, 2 * C), F32),
        ),
        in_specs=[any_spec] * 5,
        out_specs=(any_spec,) * 5,
        scratch_shapes=[
            pltpu.VMEM((8, 8, rows), F32),
            pltpu.VMEM((2, 2, rows // 2, width), BF16),
            pltpu.VMEM((width,), BF16),
            pltpu.VMEM((2, 8, width), F32),
            pltpu.VMEM((2, 2, rows // 2, 128), F32),
            pltpu.VMEM((2, rows // 2, depth), BF16),
            pltpu.VMEM((num_q, depth, CQ), BF16),
            pltpu.VMEM((SLOTS, depth, C), BF16),
            pltpu.VMEM((SLOTS, depth, C), BF16),
            pltpu.VMEM((num_q, 4, quarter, CQ), F32),
            pltpu.VMEM((num_q, 2, quarter, CQ), F32),
            pltpu.VMEM((num_q, quarter, CQ), F32),
            pltpu.VMEM((2, rows // 8, q_cols), BF16),
            pltpu.VMEM((2, rows // 8, q_cols), BF16),
            pltpu.VMEM((num_c, 4, quarter, 2 * C), F32),
            pltpu.VMEM((num_c, 2, quarter, 2 * C), F32),
            dma((2,)), dma((num_q,)), dma((SLOTS,)), dma((SLOTS,)), dma((7,)), dma((7,)), dma((3,)), dma((3,)),
            dma((num_q, 2)), dma((num_q, 2)), dma((num_q,)), dma((num_q,)), dma, dma,
            dma((num_c, 2)), dma((num_c, 2)), dma((N1,)), dma((N1,)), dma((num_c,)), dma((num_c,)), dma,
        ],
        compiler_params=pltpu.CompilerParams(collective_id=0, has_side_effects=True, vmem_limit_bytes=VMEM_LIMIT),
        cost_estimate=pl.CostEstimate(
            flops=2 * rows * depth * (q_cols + 2 * wgate.shape[1]),
            bytes_accessed=2 * depth * (q_cols + 2 * wgate.shape[1]),
            transcendentals=0,
        ),
    )(x_loc.reshape(2, rows // 2, width), gain_loc, wqkv, wgate, wup)


def attend_kernel(len_ref, qkv_ref, cos_ref, sin_ref, k_ref, v_ref, ko_ref, vo_ref, o_ref):
    ko_ref[...] = k_ref[...]
    vo_ref[...] = v_ref[...]
    for n in range(PER_STEP):
        pos = len_ref[pl.program_id(0) * PER_STEP + n]
        qkv = qkv_ref[n]
        heads, head_dim = qkv.shape[0] - 2, qkv.shape[1]
        wide = qkv.astype(F32)
        turned = (wide * cos_ref[n] + pltpu.roll(wide, head_dim // 2, 1) * sin_ref[n]).astype(BF16)
        query = turned[:heads]
        base = pl.multiple_of((pos // 16) * 16, 16)
        here = lax.broadcasted_iota(jnp.int32, (16, head_dim), 0) == pos - base
        for out, new in ((ko_ref, turned[heads:heads + 1]), (vo_ref, qkv[heads + 1:heads + 2])):
            tile = out[n, pl.ds(base, 16), :].astype(F32)
            out[n, pl.ds(base, 16), :] = jnp.where(here, new.astype(F32), tile).astype(BF16)
        scores = lax.dot_general(query, ko_ref[n], (((1,), (1,)), ((), ())), preferred_element_type=F32)
        scores = scores * head_dim ** -0.5
        at = lax.broadcasted_iota(jnp.int32, scores.shape, 1)
        scores = jnp.where(at <= pos, scores, -1e30)
        weight = jnp.exp(scores - jnp.max(scores, axis=1, keepdims=True))
        probs = (weight / jnp.sum(weight, axis=1, keepdims=True)).astype(BF16)
        o_ref[n] = jnp.dot(probs, vo_ref[n], preferred_element_type=F32).astype(BF16)


def attend(qkv, cos, sin, k_cache, v_cache, ctx_len):
    reqs, length, head_dim = k_cache.shape
    heads = qkv.shape[1] - 2
    cache_spec = pl.BlockSpec((PER_STEP, length, head_dim), lambda i, lens: (i, 0, 0))
    table_spec = pl.BlockSpec((PER_STEP, 1, head_dim), lambda i, lens: (i, 0, 0))
    return pl.pallas_call(
        attend_kernel,
        name="attend",
        grid_spec=pltpu.PrefetchScalarGridSpec(
            num_scalar_prefetch=1,
            grid=(reqs // PER_STEP,),
            in_specs=[
                pl.BlockSpec((PER_STEP, heads + 2, head_dim), lambda i, lens: (i, 0, 0)),
                table_spec, table_spec, cache_spec, cache_spec,
            ],
            out_specs=[cache_spec, cache_spec, pl.BlockSpec((PER_STEP, heads, head_dim), lambda i, lens: (i, 0, 0))],
        ),
        out_shape=(
            jax.ShapeDtypeStruct(k_cache.shape, BF16),
            jax.ShapeDtypeStruct(v_cache.shape, BF16),
            jax.ShapeDtypeStruct((reqs, heads, head_dim), BF16),
        ),
        compiler_params=pltpu.CompilerParams(dimension_semantics=("arbitrary",)),
        cost_estimate=pl.CostEstimate(
            flops=64 * reqs * heads * length * head_dim,
            bytes_accessed=8 * reqs * length * head_dim,
            transcendentals=reqs * heads * length,
        ),
    )(ctx_len, qkv, cos, sin, k_cache, v_cache)


def back_kernel(
    o_hbm, own_hbm, got_hbm, perm_hbm, send_hbm, wao_hbm, wmo_hbm, z_out,
    w, own, xr, xs, act, z, zr,
    in_sem, w_sem, own_sem, x_s, x_r, o_s, o_r, sib_s, sib_r, xn_s, xn_r, fwd_s, fwd_r, z_s, z_r,
):
    xi, yi, sib, xn, _, yn = places()
    sib_dev, xn_dev, yn_dev = {"x": sib}, {"x": xn}, {"yz": yn}
    width = z_out.shape[3]
    half_rows = act.shape[1] * act.shape[2]
    num_o, num_c = wao_hbm.shape[0] // C, wmo_hbm.shape[0] // C
    num_k = num_o + num_c
    o_cols = wao_hbm.shape[0]
    pieces = len(PIECES)
    starts = [FULL + sum(PIECES[:n]) for n in range(pieces + 1)]

    def w_copy(k):
        src = wao_hbm.at[pl.ds(k * C, C), :] if k < num_o else wmo_hbm.at[pl.ds((k - num_o) * C, C), :]
        return pltpu.make_async_copy(src, w.at[k], w_sem.at[k])

    def own_copy(i):
        return pltpu.make_async_copy(own_hbm.at[i], own.at[i], own_sem.at[i])

    def here_copy(i):
        src = got_hbm.at[i] if i < N1 else perm_hbm.at[i - N1]
        return pltpu.make_async_copy(src, xr.at[i], x_r.at[i])

    def x_send(i):
        return remote(xs.at[i - N2], xr.at[i], x_s.at[i - N2], x_r.at[i], xn_dev)

    barrier = pltpu.get_barrier_semaphore()
    for dev in (sib_dev, xn_dev, yn_dev):
        pl.semaphore_signal(barrier, inc=1, device_id=dev, device_id_type=MESH)
    xs_in = pltpu.make_async_copy(send_hbm, xs, in_sem.at[1])
    xs_in.start()
    o_in = pltpu.make_async_copy(o_hbm.at[yi], act.at[yi, xi, :, 0:o_cols], in_sem.at[0])
    o_in.start()
    for i in range(N2):
        own_copy(i).start()
        here_copy(i).start()
    for i in range(N2, num_c):
        own_copy(i).start()
    xs_in.wait()
    pl.semaphore_wait(barrier, 3)

    def o_copy(half, row):
        return remote(o_hbm.at[half], act.at[row, xi, :, 0:o_cols], o_s, o_r, yn_dev)

    def block_of(e, owner):
        if e == 0:
            return act.at[:, owner, :, pl.ds(o_cols, FULL * C)]
        if e == 1:
            return act.at[:, owner, :, pl.ds(0, o_cols)]
        half, n = divmod(e - 2, pieces)
        return act.at[half, owner, :, pl.ds(o_cols + starts[n] * C, PIECES[n] * C)]

    def to_sib(e, owner):
        block = block_of(e, owner)
        return remote(block, block, sib_s.at[e], sib_r.at[e], sib_dev)

    def to_xn(e, owner):
        block = block_of(e, owner)
        return remote(block, block, xn_s.at[e], xn_r.at[e], xn_dev)

    def forward(e, owner):
        block = block_of(e, owner)
        return remote(block, block, fwd_s.at[e], fwd_r.at[e], sib_dev)

    def send_own(e):
        to_xn(e, xi).start()
        to_sib(e, xi).start()

    def pass_on(e):
        to_xn(e, xn).wait_recv()
        forward(e, xn).start()

    def arrived(e):
        to_sib(e, sib).wait_recv()
        forward(e, (sib + 2) % 4).wait_recv()

    def activate(i):
        own_copy(i).wait()
        value = activation(own[i] + xr[i])
        start = o_cols + i * C if isinstance(i, int) else pl.multiple_of(o_cols + i * C, C)
        act[:, xi, :, pl.ds(start, C)] = value.reshape(2, value.shape[0] // 2, C)

    def w_wait(k):
        pltpu.make_async_copy(wmo_hbm.at[pl.ds(0, C), :], w.at[k], w_sem.at[k]).wait()

    def multiply(first, count):
        @pl.loop(first, first + count)
        def _(k):
            w_wait(k)
            lhs = act[:, :, :, pl.ds(pl.multiple_of(k * C, C), C)].reshape(2 * half_rows, C)
            for b in range(2):
                prod = jnp.dot(lhs, w[k, :, b * width:(b + 1) * width], preferred_element_type=F32)
                z[b] = z[b] + prod.reshape(z.shape[1:])

    def multiply_one(half, n, b):
        @pl.loop(num_o + starts[n], num_o + starts[n + 1])
        def _(k):
            lhs = act[half, :, :, pl.ds(pl.multiple_of(k * C, C), C)].reshape(half_rows, C)
            cols = pl.ds(pl.multiple_of(b * width, width), width)
            prod = jnp.dot(lhs, w[k, :, cols], preferred_element_type=F32)
            z[b, half] = z[b, half] + prod.reshape(z.shape[2:])

    def multiply_half(half, n):
        @pl.loop(num_o + starts[n], num_o + starts[n + 1])
        def _(k):
            if half == 0:
                w_wait(k)
            lhs = act[half, :, :, pl.ds(pl.multiple_of(k * C, C), C)].reshape(half_rows, C)
            for b in range(2):
                prod = jnp.dot(lhs, w[k, :, b * width:(b + 1) * width], preferred_element_type=F32)
                z[b, half] = z[b, half] + prod.reshape(z.shape[2:])

    first = (num_c - N2 + 1) // 2
    for i in range(N2, N2 + first):
        x_send(i).start()
    o_copy(yn, yi).start()
    unread = list(range(num_k))

    def read_weights(count):
        for k in unread[:count]:
            w_copy(k).start()
        del unread[:count]

    read_weights(2)
    z[...] = jnp.zeros_like(z)

    def start_here(i):
        pltpu.make_async_copy(got_hbm.at[0], xr.at[i], x_r.at[i]).wait()
        activate(i)

    pl.loop(0, FULL)(start_here)
    o_in.wait()
    o_copy(yi, yn).wait_recv()
    send_own(1)
    for i in range(N2 + first, num_c):
        x_send(i).start()
    send_own(0)
    read_weights(2)
    pl.loop(FULL, N2)(start_here)
    ready = sum(end <= N2 for end in starts[1:])
    for n in range(ready):
        send_own(2 + n)
    read_weights(2)
    for i in range(N2, N2 + first):
        x_send(i).wait_recv()
        activate(i)
        read_weights(2)
    pass_on(1)
    read_weights(2)
    arrived(1)
    multiply(0, num_o)
    read_weights(2)

    for i in range(N2 + first, num_c):
        x_send(i).wait_recv()
        activate(i)
        read_weights(2)
    groups = 2 + 2 * pieces
    for e in range(2 + ready, groups):
        send_own(e)
    pass_on(0)
    read_weights(num_k)
    arrived(0)
    multiply(num_o, FULL)
    z_copies = [remote(z.at[yn, half], zr.at[half], z_s.at[half], z_r.at[half], yn_dev) for half in range(2)]
    pass_on(2)
    for e in range(2, groups):
        if e + 1 < groups:
            pass_on(e + 1)
        arrived(e)
        half, n = divmod(e - 2, pieces)
        if e + 1 < groups:
            multiply_half(half, n)
        else:
            multiply_one(half, n, yn)
        if n == pieces - 1:
            z_copies[half].start()
    multiply_one(1, pieces - 1, yi)

    o_copy(yn, yi).wait_send()
    for e in range(groups):
        to_xn(e, xi).wait_send()
        to_sib(e, xi).wait_send()
        forward(e, xn).wait_send()

    @pl.loop(N2, num_c)
    def _(i):
        x_send(i).wait_send()

    for half in range(2):
        z_copies[half].wait()
        z_out[:, half] = z[yi, half] + zr[half]


def back(x_loc, o_halves, own, got, perm, send, wao, wmo):
    rows, width = x_loc.shape
    num_o, num_c = wao.shape[0] // C, wmo.shape[0] // C
    num_k = num_o + num_c
    groups = 2 + 2 * len(PIECES)
    quarter = rows // 4
    dma = pltpu.SemaphoreType.DMA
    any_spec = pl.BlockSpec(memory_space=pl.ANY)
    z = pl.pallas_call(
        back_kernel,
        name="back",
        out_shape=jax.ShapeDtypeStruct((4, 2, rows // 8, width), F32),
        in_specs=[any_spec] * 7,
        out_specs=pl.BlockSpec(memory_space=pltpu.VMEM),
        scratch_shapes=[
            pltpu.VMEM((num_k, C, 2 * width), BF16),
            pltpu.VMEM((num_c, quarter, 2 * C), F32),
            pltpu.VMEM((num_c, quarter, 2 * C), F32),
            pltpu.VMEM((num_c - N2, quarter, 2 * C), F32),
            pltpu.VMEM((2, 4, rows // 8, num_k * C), BF16),
            pltpu.VMEM((2, 2, 4, rows // 8, width), F32),
            pltpu.VMEM((2, 4, rows // 8, width), F32),
            dma((2,)), dma((num_k,)), dma((num_c,)), dma((num_c - N2,)), dma((num_c,)), dma, dma,
            dma((groups,)), dma((groups,)), dma((groups,)), dma((groups,)), dma((groups,)), dma((groups,)),
            dma((2,)), dma((2,)),
        ],
        compiler_params=pltpu.CompilerParams(collective_id=1, has_side_effects=True, vmem_limit_bytes=VMEM_LIMIT),
        cost_estimate=pl.CostEstimate(
            flops=4 * rows * num_k * C * width, bytes_accessed=4 * num_k * C * width, transcendentals=0
        ),
    )(o_halves, own, got, perm, send, wao, wmo)
    return (x_loc.astype(F32) + z.reshape(rows, width)).astype(BF16)


def solution(mesh):
    x_size, yz_size = mesh.shape["x"], mesh.shape["yz"]
    both_axes = ("x", "yz")
    row_spec = P("dp", both_axes)
    in_w_spec = P("x", "yz")
    out_w_spec = P("yz", "x")
    cache_spec = P(("dp", "x", "yz"), None, None)
    len_spec = P(("dp", "x", "yz"))
    across = [(i, (i + 2) % 4) for i in range(4)]

    def local_layer(x_loc, gain_loc, wqkv_loc, wgate_loc, wup_loc, wao_loc, wmo_loc, kc_loc, vc_loc, len_loc):
        d_model = x_loc.shape[1] * x_size * yz_size
        reqs, _, head_dim = kc_loc.shape
        half = head_dim // 2
        inv_freq = 10000.0 ** (-jnp.arange(half, dtype=F32) / half)
        angles = len_loc.astype(F32)[:, None] * inv_freq
        cos, sin = jnp.cos(angles), jnp.sin(angles)
        cos = jnp.concatenate([cos, cos], axis=1)[:, None, :]
        sin = jnp.concatenate([-sin, sin], axis=1)[:, None, :]

        qkv, got, perm, send, own = front(
            x_loc, gain_loc, wqkv_loc, wgate_loc, wup_loc, d_model
        )
        perm = lax.ppermute(perm, "x", across)
        qkv = jnp.concatenate([qkv[0], qkv[1]], axis=1).reshape(reqs, -1, head_dim)
        k_all, v_all, attn = attend(qkv, cos, sin, kc_loc, vc_loc, len_loc)
        o_halves = jnp.swapaxes(attn.reshape(reqs, 2, -1), 0, 1)
        y_loc = back(x_loc, o_halves, own, got, perm, send, wao_loc, wmo_loc)
        return y_loc, k_all, v_all

    in_specs = (row_spec, P(both_axes), in_w_spec, in_w_spec, in_w_spec, out_w_spec, out_w_spec, cache_spec, cache_spec, len_spec)
    out_specs = (row_spec, cache_spec, cache_spec)
    return jax.shard_map(local_layer, mesh=mesh, in_specs=in_specs, out_specs=out_specs, check_vma=False)
```

```python
import functools

import jax
import jax.numpy as jnp
from jax import lax
from jax.experimental import pallas as pl
from jax.experimental.pallas import tpu as pltpu
from jax.sharding import PartitionSpec as P

MESH = pl.DeviceIdType.MESH
F32 = jnp.float32
BF16 = jnp.bfloat16
VMEM_LIMIT = 66_900_000

C = 768
CQ = 640
PER_STEP = 2
SLOTS = 3
N1 = 5
N2 = 13
FULL = 5
PIECES = (8, 3)


def remote(src, dst, send_sem, recv_sem, device):
    return pltpu.make_async_remote_copy(
        src_ref=src, dst_ref=dst, send_sem=send_sem, recv_sem=recv_sem, device_id=device, device_id_type=MESH
    )


def places():
    xi = lax.axis_index("x")
    yi = lax.axis_index("yz")
    sib = xi + 1 - 2 * (xi % 2)
    xn = (xi + 2) % 4
    return xi, yi, sib, xn, (sib + 2) % 4, 1 - yi


def activation(total):
    gate = total[:, :C].astype(BF16).astype(F32)
    up = total[:, C:].astype(BF16).astype(F32)
    return (jax.nn.silu(gate) * up).astype(BF16)


def front_kernel(
    d_model, x_hbm, g_hbm, wq_hbm, wg_hbm, wu_hbm,
    qkv_hbm, got_hbm, perm_hbm, send_hbm, own_hbm,
    stat, xbuf, gain, gbuf, moments, h, wq, wg, wu, pq, rq, xq, qs, qd, p, r,
    in_sem, wq_sem, wg_sem, wu_sem, st_s, st_r, xg_s, xg_r,
    dq_s, dq_r, xq_s, xq_r, yq_s, yq_r, d_s, d_r, x_s, x_r, out_sem, own_sem, q_sem,
):
    xi, yi, sib, xn, sibn, yn = places()
    me = yi * 4 + xi
    sides, side_rows, width = x_hbm.shape
    rows = sides * side_rows
    near = xi // 2
    far = 1 - near
    num_q = wq_hbm.shape[1] // CQ
    num_c = wg_hbm.shape[1] // C
    sib_dev, xn_dev, yn_dev = {"x": sib}, {"x": xn}, {"yz": yn}

    def wq_copy(c):
        return pltpu.make_async_copy(wq_hbm.at[:, pl.ds(c * CQ, CQ)], wq.at[c], wq_sem.at[c])

    def w_copies(i, slot):
        start = pl.multiple_of(i * C, C)
        return (
            pltpu.make_async_copy(wg_hbm.at[:, pl.ds(start, C)], wg.at[slot], wg_sem.at[slot]),
            pltpu.make_async_copy(wu_hbm.at[:, pl.ds(start, C)], wu.at[slot], wu_sem.at[slot]),
        )

    x_in = pltpu.make_async_copy(x_hbm, xbuf.at[yi], in_sem.at[0])
    g_in = pltpu.make_async_copy(g_hbm, gain, in_sem.at[1])
    x_in.start()
    g_in.start()
    barrier = pltpu.get_barrier_semaphore()
    offsets = [(dy, dx) for dy in range(2) for dx in range(4)][1:]
    for dy, dx in offsets:
        pl.semaphore_signal(barrier, inc=1, device_id={"yz": (yi + dy) % 2, "x": (xi + dx) % 4}, device_id_type=MESH)

    x_in.wait()
    x_f32 = xbuf[yi].reshape(rows, width).astype(F32)
    lane = lax.broadcasted_iota(jnp.int32, (rows, rows), 1)
    sums = jnp.where(
        lane == 0,
        jnp.sum(x_f32, axis=1, keepdims=True),
        jnp.where(lane == 1, jnp.sum(x_f32 * x_f32, axis=1, keepdims=True), 0.0),
    )
    stat[me] = sums.T[0:8, :]
    g_in.wait()
    gbuf[yi] = jnp.broadcast_to(gain[...].astype(F32)[None, :], (8, width))
    pl.semaphore_wait(barrier, 7)

    def stat_copy(k, slot):
        dy, dx = offsets[k]
        dev = {"yz": (yi + dy) % 2, "x": (xi + dx) % 4}
        return remote(stat.at[slot], stat.at[slot], st_s.at[k], st_r.at[k], dev)

    def x_copy(slot, n):
        block = xbuf.at[slot, (far, near)[n]]
        return remote(block, block, xg_s.at[1 + n], xg_r.at[1 + n], yn_dev)

    def g_copy(slot):
        return remote(gbuf.at[slot], gbuf.at[slot], xg_s.at[0], xg_r.at[0], yn_dev)

    for k in range(7):
        stat_copy(k, me).start()
    g_copy(yi).start()
    x_copy(yi, 0).start()
    x_copy(yi, 1).start()
    for c in range(num_q):
        wq_copy(c).start()
    for i in range(SLOTS):
        for copy in w_copies(i, i):
            copy.start()
    for k, (dy, dx) in enumerate(offsets):
        stat_copy(k, ((yi + 2 - dy) % 2) * 4 + (xi + 4 - dx) % 4).wait_recv()
    total = stat[0]
    for k in range(1, 8):
        total = total + stat[k]
    cols = jnp.concatenate([total, jnp.zeros((rows - 8, rows), F32)], axis=0).T
    mean = cols[:, 0:1] / d_model
    var = cols[:, 1:2] / d_model - mean * mean
    moments[0] = jnp.broadcast_to(mean, (rows, 128)).reshape(sides, side_rows, 128)
    moments[1] = jnp.broadcast_to(lax.rsqrt(var + 1e-6), (rows, 128)).reshape(sides, side_rows, 128)
    g_copy(yn).wait_recv()

    def normalize(side):
        for b in range(2):
            part = (xbuf[b, side].astype(F32) - moments[0, side][:, 0:1]) * moments[1, side][:, 0:1]
            h[side, :, b * width:(b + 1) * width] = (part * gbuf[b][0:1, :]).astype(BF16)

    def dq(c, k):
        src = sib if k == 0 else sibn
        return remote(pq.at[c, src], rq.at[c, k], dq_s.at[c, k], dq_r.at[c, k], sib_dev)

    def xq_copy(c):
        return remote(pq.at[c, xn], xq.at[c], xq_s.at[c], xq_r.at[c], xn_dev)

    def q_product(c, side):
        prod = jnp.dot(h[side], wq[c], preferred_element_type=F32)
        pq[c, pl.ds(2 * side, 2)] = prod.reshape(2, rows // 4, CQ)

    def q_send(c):
        dq(c, 1).wait_recv()
        dq(c, 1).wait_send()
        pq[c, xn] = pq[c, xn] + rq[c, 1]
        xq_copy(c).start()

    x_copy(yn, 0).wait_recv()
    normalize(far)

    @pl.loop(0, num_q)
    def _(c):
        wq_copy(c).wait()
        q_product(c, far)
        dq(c, 1).start()

        @pl.when(c >= 1)
        def _():
            q_send(c - 1)

    x_copy(yn, 1).wait_recv()
    normalize(near)
    q_send(num_q - 1)

    @pl.loop(0, num_q)
    def _(c):
        q_product(c, near)
        dq(c, 0).start()

    def d_copy(i, k):
        src = sib if k == 0 else sibn
        return remote(p.at[i, src], r.at[i, k], d_s.at[i, k], d_r.at[i, k], sib_dev)

    def x_send(i):
        return remote(p.at[i, xn], got_hbm.at[i], x_s.at[i], x_r.at[i], xn_dev)

    def perm_copy(i):
        return pltpu.make_async_copy(p.at[i, xn], perm_hbm.at[i - N1], out_sem.at[i])

    def send_copy(i):
        return pltpu.make_async_copy(p.at[i, xn], send_hbm.at[i - N2], out_sem.at[i])

    def own_copy(i):
        return pltpu.make_async_copy(p.at[i, xi], own_hbm.at[i], own_sem.at[i])

    def chip_sum(i):
        d_copy(i, 1).wait_recv()
        d_copy(i, 1).wait_send()
        p[i, xn] = p[i, xn] + r[i, 1]

        @pl.when(i < N1)
        def _():
            x_send(i).start()

        @pl.when((i >= N1) & (i < N2))
        def _():
            perm_copy(i).start()

        @pl.when(i >= N2)
        def _():
            send_copy(i).start()

        d_copy(i, 0).wait_recv()
        d_copy(i, 0).wait_send()
        p[i, xi] = p[i, xi] + r[i, 0]
        own_copy(i).start()

    def product(i):
        slot = i % SLOTS
        g_w, u_w = w_copies(i, slot)
        h_all = h[...].reshape(rows, h.shape[2])
        g_w.wait()
        p[i, :, :, :C] = jnp.dot(h_all, wg[slot], preferred_element_type=F32).reshape(4, rows // 4, C)
        u_w.wait()
        p[i, :, :, C:] = jnp.dot(h_all, wu[slot], preferred_element_type=F32).reshape(4, rows // 4, C)
        d_copy(i, 1).start()
        d_copy(i, 0).start()

        @pl.when(i + SLOTS < num_c)
        def _():
            for copy in w_copies(i + SLOTS, slot):
                copy.start()

    product(0)

    def step(i):
        product(i)
        chip_sum(i - 1)

    half = num_c // 2 + 1
    pl.loop(1, half)(step)

    @pl.loop(0, num_q)
    def _(c):
        dq(c, 0).wait_recv()
        dq(c, 0).wait_send()
        mine = pq[c, xi] + rq[c, 0]
        xq_copy(c).wait_recv()
        xq_copy(c).wait_send()
        value = (mine + xq[c]).astype(BF16)
        qs[:, :, pl.ds(pl.multiple_of(c * CQ, CQ), CQ)] = value.reshape(2, rows // 8, CQ)

    def yq_copy(k):
        return remote(qs.at[1 - k], qd.at[k], yq_s, yq_r, yn_dev)

    yq_copy(yi).start()
    qd[yi] = qs[yi]

    pl.loop(half, num_c)(step)
    chip_sum(num_c - 1)
    yq_copy(yn).wait_recv()
    q_out = pltpu.make_async_copy(qd, qkv_hbm, q_sem)
    q_out.start()

    for k in range(7):
        stat_copy(k, me).wait_send()
    g_copy(yi).wait_send()
    x_copy(yi, 0).wait_send()
    x_copy(yi, 1).wait_send()
    yq_copy(yi).wait_send()

    @pl.loop(0, num_c)
    def _(i):
        own_copy(i).wait()

    @pl.loop(N1, N2)
    def _(i):
        perm_copy(i).wait()

    @pl.loop(N2, num_c)
    def _(i):
        send_copy(i).wait()

    q_out.wait()

    @pl.loop(0, N1)
    def _(i):
        x_send(i).wait()


def front(x_loc, gain_loc, wqkv, wgate, wup, d_model):
    rows, width = x_loc.shape
    depth, q_cols = wqkv.shape
    num_q, num_c = q_cols // CQ, wgate.shape[1] // C
    quarter = rows // 4
    dma = pltpu.SemaphoreType.DMA
    any_spec = pl.BlockSpec(memory_space=pl.ANY)
    return pl.pallas_call(
        functools.partial(front_kernel, d_model),
        name="front",
        out_shape=(
            jax.ShapeDtypeStruct((2, rows // 8, q_cols), BF16),
            jax.ShapeDtypeStruct((N1, quarter, 2 * C), F32),
            jax.ShapeDtypeStruct((N2 - N1, quarter, 2 * C), F32),
            jax.ShapeDtypeStruct((num_c - N2, quarter, 2 * C), F32),
            jax.ShapeDtypeStruct((num_c, quarter, 2 * C), F32),
        ),
        in_specs=[any_spec] * 5,
        out_specs=(any_spec,) * 5,
        scratch_shapes=[
            pltpu.VMEM((8, 8, rows), F32),
            pltpu.VMEM((2, 2, rows // 2, width), BF16),
            pltpu.VMEM((width,), BF16),
            pltpu.VMEM((2, 8, width), F32),
            pltpu.VMEM((2, 2, rows // 2, 128), F32),
            pltpu.VMEM((2, rows // 2, depth), BF16),
            pltpu.VMEM((num_q, depth, CQ), BF16),
            pltpu.VMEM((SLOTS, depth, C), BF16),
            pltpu.VMEM((SLOTS, depth, C), BF16),
            pltpu.VMEM((num_q, 4, quarter, CQ), F32),
            pltpu.VMEM((num_q, 2, quarter, CQ), F32),
            pltpu.VMEM((num_q, quarter, CQ), F32),
            pltpu.VMEM((2, rows // 8, q_cols), BF16),
            pltpu.VMEM((2, rows // 8, q_cols), BF16),
            pltpu.VMEM((num_c, 4, quarter, 2 * C), F32),
            pltpu.VMEM((num_c, 2, quarter, 2 * C), F32),
            dma((2,)), dma((num_q,)), dma((SLOTS,)), dma((SLOTS,)), dma((7,)), dma((7,)), dma((3,)), dma((3,)),
            dma((num_q, 2)), dma((num_q, 2)), dma((num_q,)), dma((num_q,)), dma, dma,
            dma((num_c, 2)), dma((num_c, 2)), dma((N1,)), dma((N1,)), dma((num_c,)), dma((num_c,)), dma,
        ],
        compiler_params=pltpu.CompilerParams(collective_id=0, has_side_effects=True, vmem_limit_bytes=VMEM_LIMIT),
        cost_estimate=pl.CostEstimate(
            flops=2 * rows * depth * (q_cols + 2 * wgate.shape[1]),
            bytes_accessed=2 * depth * (q_cols + 2 * wgate.shape[1]),
            transcendentals=0,
        ),
    )(x_loc.reshape(2, rows // 2, width), gain_loc, wqkv, wgate, wup)


def attend_kernel(len_ref, qkv_ref, cos_ref, sin_ref, k_ref, v_ref, ko_ref, vo_ref, o_ref):
    ko_ref[...] = k_ref[...]
    vo_ref[...] = v_ref[...]
    for n in range(PER_STEP):
        pos = len_ref[pl.program_id(0) * PER_STEP + n]
        qkv = qkv_ref[n]
        heads, head_dim = qkv.shape[0] - 2, qkv.shape[1]
        wide = qkv.astype(F32)
        turned = (wide * cos_ref[n] + pltpu.roll(wide, head_dim // 2, 1) * sin_ref[n]).astype(BF16)
        query = turned[:heads]
        base = pl.multiple_of((pos // 16) * 16, 16)
        here = lax.broadcasted_iota(jnp.int32, (16, head_dim), 0) == pos - base
        for out, new in ((ko_ref, turned[heads:heads + 1]), (vo_ref, qkv[heads + 1:heads + 2])):
            tile = out[n, pl.ds(base, 16), :].astype(F32)
            out[n, pl.ds(base, 16), :] = jnp.where(here, new.astype(F32), tile).astype(BF16)
        scores = lax.dot_general(query, ko_ref[n], (((1,), (1,)), ((), ())), preferred_element_type=F32)
        scores = scores * head_dim ** -0.5
        at = lax.broadcasted_iota(jnp.int32, scores.shape, 1)
        scores = jnp.where(at <= pos, scores, -1e30)
        weight = jnp.exp(scores - jnp.max(scores, axis=1, keepdims=True))
        probs = (weight / jnp.sum(weight, axis=1, keepdims=True)).astype(BF16)
        o_ref[n] = jnp.dot(probs, vo_ref[n], preferred_element_type=F32).astype(BF16)


def attend(qkv, cos, sin, k_cache, v_cache, ctx_len):
    reqs, length, head_dim = k_cache.shape
    heads = qkv.shape[1] - 2
    cache_spec = pl.BlockSpec((PER_STEP, length, head_dim), lambda i, lens: (i, 0, 0))
    table_spec = pl.BlockSpec((PER_STEP, 1, head_dim), lambda i, lens: (i, 0, 0))
    return pl.pallas_call(
        attend_kernel,
        name="attend",
        grid_spec=pltpu.PrefetchScalarGridSpec(
            num_scalar_prefetch=1,
            grid=(reqs // PER_STEP,),
            in_specs=[
                pl.BlockSpec((PER_STEP, heads + 2, head_dim), lambda i, lens: (i, 0, 0)),
                table_spec, table_spec, cache_spec, cache_spec,
            ],
            out_specs=[cache_spec, cache_spec, pl.BlockSpec((PER_STEP, heads, head_dim), lambda i, lens: (i, 0, 0))],
        ),
        out_shape=(
            jax.ShapeDtypeStruct(k_cache.shape, BF16),
            jax.ShapeDtypeStruct(v_cache.shape, BF16),
            jax.ShapeDtypeStruct((reqs, heads, head_dim), BF16),
        ),
        compiler_params=pltpu.CompilerParams(dimension_semantics=("arbitrary",)),
        cost_estimate=pl.CostEstimate(
            flops=64 * reqs * heads * length * head_dim,
            bytes_accessed=8 * reqs * length * head_dim,
            transcendentals=reqs * heads * length,
        ),
    )(ctx_len, qkv, cos, sin, k_cache, v_cache)


def back_kernel(
    o_hbm, own_hbm, got_hbm, perm_hbm, send_hbm, wao_hbm, wmo_hbm, z_out,
    w, own, xr, act, z, zr,
    in_sem, out_sem, w_sem, own_sem, x_s, x_r, o_s, o_r, sib_s, sib_r, xn_s, xn_r, fwd_s, fwd_r, z_s, z_r,
):
    xi, yi, sib, xn, _, yn = places()
    sib_dev, xn_dev, yn_dev = {"x": sib}, {"x": xn}, {"yz": yn}
    width = z_out.shape[3]
    half_rows = act.shape[1] * act.shape[2]
    num_o, num_c = wao_hbm.shape[0] // C, wmo_hbm.shape[0] // C
    num_k = num_o + num_c
    o_cols = wao_hbm.shape[0]
    pieces = len(PIECES)
    starts = [FULL + sum(PIECES[:n]) for n in range(pieces + 1)]

    def w_copy(k):
        src = wao_hbm.at[pl.ds(k * C, C), :] if k < num_o else wmo_hbm.at[pl.ds((k - num_o) * C, C), :]
        return pltpu.make_async_copy(src, w.at[k], w_sem.at[k])

    def own_copy(i):
        return pltpu.make_async_copy(own_hbm.at[i], own.at[i], own_sem.at[i])

    def here_copy(i):
        src = got_hbm.at[i] if i < N1 else perm_hbm.at[i - N1]
        return pltpu.make_async_copy(src, xr.at[i], x_r.at[i])

    def x_send(i):
        return remote(send_hbm.at[i - N2], xr.at[i], x_s.at[i - N2], x_r.at[i], xn_dev)

    barrier = pltpu.get_barrier_semaphore()
    for dev in (sib_dev, xn_dev, yn_dev):
        pl.semaphore_signal(barrier, inc=1, device_id=dev, device_id_type=MESH)
    o_in = pltpu.make_async_copy(o_hbm.at[yi], act.at[yi, xi, :, 0:o_cols], in_sem)
    o_in.start()
    for i in range(N2):
        own_copy(i).start()
        here_copy(i).start()
    for i in range(N2, num_c):
        own_copy(i).start()
    pl.semaphore_wait(barrier, 3)

    def o_copy(half, row):
        return remote(o_hbm.at[half], act.at[row, xi, :, 0:o_cols], o_s, o_r, yn_dev)

    def block_of(e, owner):
        if e == 0:
            return act.at[:, owner, :, pl.ds(o_cols, FULL * C)]
        if e == 1:
            return act.at[:, owner, :, pl.ds(0, o_cols)]
        half, n = divmod(e - 2, pieces)
        return act.at[half, owner, :, pl.ds(o_cols + starts[n] * C, PIECES[n] * C)]

    def to_sib(e, owner):
        block = block_of(e, owner)
        return remote(block, block, sib_s.at[e], sib_r.at[e], sib_dev)

    def to_xn(e, owner):
        block = block_of(e, owner)
        return remote(block, block, xn_s.at[e], xn_r.at[e], xn_dev)

    def forward(e, owner):
        block = block_of(e, owner)
        return remote(block, block, fwd_s.at[e], fwd_r.at[e], sib_dev)

    def send_own(e):
        to_xn(e, xi).start()
        to_sib(e, xi).start()

    def pass_on(e):
        to_xn(e, xn).wait_recv()
        forward(e, xn).start()

    def arrived(e):
        to_sib(e, sib).wait_recv()
        forward(e, (sib + 2) % 4).wait_recv()

    def activate(i):
        own_copy(i).wait()
        value = activation(own[i] + xr[i])
        start = o_cols + i * C if isinstance(i, int) else pl.multiple_of(o_cols + i * C, C)
        act[:, xi, :, pl.ds(start, C)] = value.reshape(2, value.shape[0] // 2, C)

    def w_wait(k):
        pltpu.make_async_copy(wmo_hbm.at[pl.ds(0, C), :], w.at[k], w_sem.at[k]).wait()

    def multiply(first, count):
        @pl.loop(first, first + count)
        def _(k):
            w_wait(k)
            lhs = act[:, :, :, pl.ds(pl.multiple_of(k * C, C), C)].reshape(2 * half_rows, C)
            for b in range(2):
                prod = jnp.dot(lhs, w[k, :, b * width:(b + 1) * width], preferred_element_type=F32)
                z[b] = z[b] + prod.reshape(z.shape[1:])

    def multiply_one(half, n, b):
        @pl.loop(num_o + starts[n], num_o + starts[n + 1])
        def _(k):
            lhs = act[half, :, :, pl.ds(pl.multiple_of(k * C, C), C)].reshape(half_rows, C)
            cols = pl.ds(pl.multiple_of(b * width, width), width)
            prod = jnp.dot(lhs, w[k, :, cols], preferred_element_type=F32)
            z[b, half] = z[b, half] + prod.reshape(z.shape[2:])

    def multiply_half(half, n):
        @pl.loop(num_o + starts[n], num_o + starts[n + 1])
        def _(k):
            if half == 0:
                w_wait(k)
            lhs = act[half, :, :, pl.ds(pl.multiple_of(k * C, C), C)].reshape(half_rows, C)
            for b in range(2):
                prod = jnp.dot(lhs, w[k, :, b * width:(b + 1) * width], preferred_element_type=F32)
                z[b, half] = z[b, half] + prod.reshape(z.shape[2:])

    first = (num_c - N2 + 1) // 2
    for i in range(N2, N2 + first):
        x_send(i).start()
    o_copy(yn, yi).start()
    unread = list(range(num_k))

    def read_weights(count):
        for k in unread[:count]:
            w_copy(k).start()
        del unread[:count]

    read_weights(2)
    z[...] = jnp.zeros_like(z)

    def start_here(i):
        pltpu.make_async_copy(got_hbm.at[0], xr.at[i], x_r.at[i]).wait()
        activate(i)

    pl.loop(0, FULL)(start_here)
    o_in.wait()
    o_copy(yi, yn).wait_recv()
    send_own(1)
    send_own(0)
    for i in range(N2 + first, num_c):
        x_send(i).start()
    read_weights(2)
    pl.loop(FULL, N2)(start_here)
    ready = sum(end <= N2 for end in starts[1:])
    for n in range(ready):
        send_own(2 + n)
    read_weights(2)
    for i in range(N2, N2 + first):
        x_send(i).wait_recv()
        activate(i)
        read_weights(2)
    pass_on(1)
    read_weights(2)
    arrived(1)
    multiply(0, num_o)
    read_weights(2)

    for i in range(N2 + first, num_c):
        x_send(i).wait_recv()
        activate(i)
        read_weights(2)
    groups = 2 + 2 * pieces
    for e in range(2 + ready, groups):
        send_own(e)
    pass_on(0)
    read_weights(num_k)
    arrived(0)
    multiply(num_o, FULL)
    z_copies = [remote(z.at[yn, half], zr.at[half], z_s.at[half], z_r.at[half], yn_dev) for half in range(2)]
    pass_on(2)
    for e in range(2, groups):
        if e + 1 < groups:
            pass_on(e + 1)
        arrived(e)
        half, n = divmod(e - 2, pieces)
        if e + 1 < groups:
            multiply_half(half, n)
        else:
            multiply_one(half, n, yn)
        if n == pieces - 1:
            z_copies[half].start()
    multiply_one(1, pieces - 1, yi)

    o_copy(yn, yi).wait_send()
    for e in range(groups):
        to_xn(e, xi).wait_send()
        to_sib(e, xi).wait_send()
        forward(e, xn).wait_send()

    @pl.loop(N2, num_c)
    def _(i):
        x_send(i).wait_send()

    outs = [pltpu.make_async_copy(zr.at[half], z_out.at[:, half], out_sem.at[half]) for half in range(2)]
    for half in range(2):
        z_copies[half].wait()
        zr[half] = z[yi, half] + zr[half]
        outs[half].start()
    for half in range(2):
        outs[half].wait()


def back(x_loc, o_halves, own, got, perm, send, wao, wmo):
    rows, width = x_loc.shape
    num_o, num_c = wao.shape[0] // C, wmo.shape[0] // C
    num_k = num_o + num_c
    groups = 2 + 2 * len(PIECES)
    quarter = rows // 4
    dma = pltpu.SemaphoreType.DMA
    any_spec = pl.BlockSpec(memory_space=pl.ANY)
    z = pl.pallas_call(
        back_kernel,
        name="back",
        out_shape=jax.ShapeDtypeStruct((4, 2, rows // 8, width), F32),
        in_specs=[any_spec] * 7,
        out_specs=any_spec,
        scratch_shapes=[
            pltpu.VMEM((num_k, C, 2 * width), BF16),
            pltpu.VMEM((num_c, quarter, 2 * C), F32),
            pltpu.VMEM((num_c, quarter, 2 * C), F32),
            pltpu.VMEM((2, 4, rows // 8, num_k * C), BF16),
            pltpu.VMEM((2, 2, 4, rows // 8, width), F32),
            pltpu.VMEM((2, 4, rows // 8, width), F32),
            dma, dma((2,)), dma((num_k,)), dma((num_c,)), dma((num_c - N2,)), dma((num_c,)), dma, dma,
            dma((groups,)), dma((groups,)), dma((groups,)), dma((groups,)), dma((groups,)), dma((groups,)),
            dma((2,)), dma((2,)),
        ],
        compiler_params=pltpu.CompilerParams(collective_id=1, has_side_effects=True, vmem_limit_bytes=VMEM_LIMIT),
        cost_estimate=pl.CostEstimate(
            flops=4 * rows * num_k * C * width, bytes_accessed=4 * num_k * C * width, transcendentals=0
        ),
    )(o_halves, own, got, perm, send, wao, wmo)
    return (x_loc.astype(F32) + z.reshape(rows, width)).astype(BF16)


def solution(mesh):
    x_size, yz_size = mesh.shape["x"], mesh.shape["yz"]
    both_axes = ("x", "yz")
    row_spec = P("dp", both_axes)
    in_w_spec = P("x", "yz")
    out_w_spec = P("yz", "x")
    cache_spec = P(("dp", "x", "yz"), None, None)
    len_spec = P(("dp", "x", "yz"))
    across = [(i, (i + 2) % 4) for i in range(4)]

    def local_layer(x_loc, gain_loc, wqkv_loc, wgate_loc, wup_loc, wao_loc, wmo_loc, kc_loc, vc_loc, len_loc):
        d_model = x_loc.shape[1] * x_size * yz_size
        reqs, _, head_dim = kc_loc.shape
        half = head_dim // 2
        inv_freq = 10000.0 ** (-jnp.arange(half, dtype=F32) / half)
        angles = len_loc.astype(F32)[:, None] * inv_freq
        cos, sin = jnp.cos(angles), jnp.sin(angles)
        cos = jnp.concatenate([cos, cos], axis=1)[:, None, :]
        sin = jnp.concatenate([-sin, sin], axis=1)[:, None, :]

        qkv, got, perm, send, own = front(
            x_loc, gain_loc, wqkv_loc, wgate_loc, wup_loc, d_model
        )
        perm = lax.ppermute(perm, "x", across)
        qkv = jnp.concatenate([qkv[0], qkv[1]], axis=1).reshape(reqs, -1, head_dim)
        k_all, v_all, attn = attend(qkv, cos, sin, kc_loc, vc_loc, len_loc)
        o_halves = jnp.swapaxes(attn.reshape(reqs, 2, -1), 0, 1)
        y_loc = back(x_loc, o_halves, own, got, perm, send, wao_loc, wmo_loc)
        return y_loc, k_all, v_all

    in_specs = (row_spec, P(both_axes), in_w_spec, in_w_spec, in_w_spec, out_w_spec, out_w_spec, cache_spec, cache_spec, len_spec)
    out_specs = (row_spec, cache_spec, cache_spec)
    return jax.shard_map(local_layer, mesh=mesh, in_specs=in_specs, out_specs=out_specs, check_vma=False)
```

```python
import functools

import jax
import jax.numpy as jnp
from jax import lax
from jax.experimental import pallas as pl
from jax.experimental.pallas import tpu as pltpu
from jax.sharding import PartitionSpec as P

MESH = pl.DeviceIdType.MESH
F32 = jnp.float32
BF16 = jnp.bfloat16
VMEM_LIMIT = 66_900_000

C = 768
CQ = 640
PER_STEP = 2
SLOTS = 3
LOW, SHIFT, PERM = 4, 2, 8
FULL = 5
PIECES = (7, 4)


def remote(src, dst, send_sem, recv_sem, device):
    return pltpu.make_async_remote_copy(
        src_ref=src, dst_ref=dst, send_sem=send_sem, recv_sem=recv_sem, device_id=device, device_id_type=MESH
    )


def places():
    xi = lax.axis_index("x")
    yi = lax.axis_index("yz")
    sib = xi + 1 - 2 * (xi % 2)
    xn = (xi + 2) % 4
    return xi, yi, sib, xn, (sib + 2) % 4, 1 - yi


def activation(total):
    gate = total[:, :C].astype(BF16).astype(F32)
    up = total[:, C:].astype(BF16).astype(F32)
    return (jax.nn.silu(gate) * up).astype(BF16)


def front_kernel(
    d_model, x_hbm, g_hbm, wq_hbm, wg_hbm, wu_hbm,
    qkv_hbm, got_hbm, perm_hbm, send_hbm, own_hbm,
    stat, xbuf, gain, gbuf, moments, h, wq, wg, wu, pq, rq, xq, qs, qd, p, r,
    in_sem, wq_sem, wg_sem, wu_sem, st_s, st_r, xg_s, xg_r,
    dq_s, dq_r, xq_s, xq_r, yq_s, yq_r, d_s, d_r, x_s, x_r, out_sem, own_sem, q_sem,
):
    xi, yi, sib, xn, sibn, yn = places()
    me = yi * 4 + xi
    sides, side_rows, width = x_hbm.shape
    rows = sides * side_rows
    n1 = LOW + SHIFT * (xi % 2)
    n2 = n1 + PERM
    near = xi // 2
    far = 1 - near
    num_q = wq_hbm.shape[1] // CQ
    num_c = wg_hbm.shape[1] // C
    sib_dev, xn_dev, yn_dev = {"x": sib}, {"x": xn}, {"yz": yn}

    def wq_copy(c):
        return pltpu.make_async_copy(wq_hbm.at[:, pl.ds(c * CQ, CQ)], wq.at[c], wq_sem.at[c])

    def w_copies(i, slot):
        start = pl.multiple_of(i * C, C)
        return (
            pltpu.make_async_copy(wg_hbm.at[:, pl.ds(start, C)], wg.at[slot], wg_sem.at[slot]),
            pltpu.make_async_copy(wu_hbm.at[:, pl.ds(start, C)], wu.at[slot], wu_sem.at[slot]),
        )

    x_in = pltpu.make_async_copy(x_hbm, xbuf.at[yi], in_sem.at[0])
    g_in = pltpu.make_async_copy(g_hbm, gain, in_sem.at[1])
    x_in.start()
    g_in.start()
    barrier = pltpu.get_barrier_semaphore()
    offsets = [(dy, dx) for dy in range(2) for dx in range(4)][1:]
    for dy, dx in offsets:
        pl.semaphore_signal(barrier, inc=1, device_id={"yz": (yi + dy) % 2, "x": (xi + dx) % 4}, device_id_type=MESH)

    x_in.wait()
    x_f32 = xbuf[yi].reshape(rows, width).astype(F32)
    lane = lax.broadcasted_iota(jnp.int32, (rows, rows), 1)
    sums = jnp.where(
        lane == 0,
        jnp.sum(x_f32, axis=1, keepdims=True),
        jnp.where(lane == 1, jnp.sum(x_f32 * x_f32, axis=1, keepdims=True), 0.0),
    )
    stat[me] = sums.T[0:8, :]
    g_in.wait()
    gbuf[yi] = jnp.broadcast_to(gain[...].astype(F32)[None, :], (8, width))
    pl.semaphore_wait(barrier, 7)

    def stat_copy(k, slot):
        dy, dx = offsets[k]
        dev = {"yz": (yi + dy) % 2, "x": (xi + dx) % 4}
        return remote(stat.at[slot], stat.at[slot], st_s.at[k], st_r.at[k], dev)

    def x_copy(slot, n):
        block = xbuf.at[slot, (far, near)[n]]
        return remote(block, block, xg_s.at[1 + n], xg_r.at[1 + n], yn_dev)

    def g_copy(slot):
        return remote(gbuf.at[slot], gbuf.at[slot], xg_s.at[0], xg_r.at[0], yn_dev)

    for k in range(7):
        stat_copy(k, me).start()
    g_copy(yi).start()
    x_copy(yi, 0).start()
    x_copy(yi, 1).start()
    for c in range(num_q):
        wq_copy(c).start()
    for i in range(SLOTS):
        for copy in w_copies(i, i):
            copy.start()
    for k, (dy, dx) in enumerate(offsets):
        stat_copy(k, ((yi + 2 - dy) % 2) * 4 + (xi + 4 - dx) % 4).wait_recv()
    total = stat[0]
    for k in range(1, 8):
        total = total + stat[k]
    cols = jnp.concatenate([total, jnp.zeros((rows - 8, rows), F32)], axis=0).T
    mean = cols[:, 0:1] / d_model
    var = cols[:, 1:2] / d_model - mean * mean
    moments[0] = jnp.broadcast_to(mean, (rows, 128)).reshape(sides, side_rows, 128)
    moments[1] = jnp.broadcast_to(lax.rsqrt(var + 1e-6), (rows, 128)).reshape(sides, side_rows, 128)
    g_copy(yn).wait_recv()

    def normalize(side):
        for b in range(2):
            part = (xbuf[b, side].astype(F32) - moments[0, side][:, 0:1]) * moments[1, side][:, 0:1]
            h[side, :, b * width:(b + 1) * width] = (part * gbuf[b][0:1, :]).astype(BF16)

    def dq(c, k):
        src = sib if k == 0 else sibn
        return remote(pq.at[c, src], rq.at[c, k], dq_s.at[c, k], dq_r.at[c, k], sib_dev)

    def xq_copy(c):
        return remote(pq.at[c, xn], xq.at[c], xq_s.at[c], xq_r.at[c], xn_dev)

    def q_product(c, side):
        prod = jnp.dot(h[side], wq[c], preferred_element_type=F32)
        pq[c, pl.ds(2 * side, 2)] = prod.reshape(2, rows // 4, CQ)

    def q_send(c):
        dq(c, 1).wait_recv()
        dq(c, 1).wait_send()
        pq[c, xn] = pq[c, xn] + rq[c, 1]
        xq_copy(c).start()

    x_copy(yn, 0).wait_recv()
    normalize(far)

    @pl.loop(0, num_q)
    def _(c):
        wq_copy(c).wait()
        q_product(c, far)
        dq(c, 1).start()

        @pl.when(c >= 1)
        def _():
            q_send(c - 1)

    x_copy(yn, 1).wait_recv()
    normalize(near)
    q_send(num_q - 1)

    @pl.loop(0, num_q)
    def _(c):
        q_product(c, near)
        dq(c, 0).start()

    def d_copy(i, k):
        src = sib if k == 0 else sibn
        return remote(p.at[i, src], r.at[i, k], d_s.at[i, k], d_r.at[i, k], sib_dev)

    def x_send(i):
        return remote(p.at[i, xn], got_hbm.at[i], x_s.at[i], x_r.at[i], xn_dev)

    def perm_copy(i):
        return pltpu.make_async_copy(p.at[i, xn], perm_hbm.at[i - n1], out_sem.at[i])

    def send_copy(i):
        return pltpu.make_async_copy(p.at[i, xn], send_hbm.at[i - n2], out_sem.at[i])

    def own_copy(i):
        return pltpu.make_async_copy(p.at[i, xi], own_hbm.at[i], own_sem.at[i])

    def chip_sum(i):
        d_copy(i, 1).wait_recv()
        d_copy(i, 1).wait_send()
        p[i, xn] = p[i, xn] + r[i, 1]

        @pl.when(i < n1)
        def _():
            x_send(i).start()

        @pl.when((i >= n1) & (i < n2))
        def _():
            perm_copy(i).start()

        @pl.when(i >= n2)
        def _():
            send_copy(i).start()

        d_copy(i, 0).wait_recv()
        d_copy(i, 0).wait_send()
        p[i, xi] = p[i, xi] + r[i, 0]
        own_copy(i).start()

    def product(i):
        slot = i % SLOTS
        g_w, u_w = w_copies(i, slot)
        h_all = h[...].reshape(rows, h.shape[2])
        g_w.wait()
        p[i, :, :, :C] = jnp.dot(h_all, wg[slot], preferred_element_type=F32).reshape(4, rows // 4, C)
        u_w.wait()
        p[i, :, :, C:] = jnp.dot(h_all, wu[slot], preferred_element_type=F32).reshape(4, rows // 4, C)
        d_copy(i, 1).start()
        d_copy(i, 0).start()

        @pl.when(i + SLOTS < num_c)
        def _():
            for copy in w_copies(i + SLOTS, slot):
                copy.start()

    product(0)

    def step(i):
        product(i)
        chip_sum(i - 1)

    half = num_c // 2 + 1
    pl.loop(1, half)(step)

    @pl.loop(0, num_q)
    def _(c):
        dq(c, 0).wait_recv()
        dq(c, 0).wait_send()
        mine = pq[c, xi] + rq[c, 0]
        xq_copy(c).wait_recv()
        xq_copy(c).wait_send()
        value = (mine + xq[c]).astype(BF16)
        qs[:, :, pl.ds(pl.multiple_of(c * CQ, CQ), CQ)] = value.reshape(2, rows // 8, CQ)

    def yq_copy(k):
        return remote(qs.at[1 - k], qd.at[k], yq_s, yq_r, yn_dev)

    yq_copy(yi).start()
    qd[yi] = qs[yi]

    pl.loop(half, num_c)(step)
    chip_sum(num_c - 1)
    yq_copy(yn).wait_recv()
    q_out = pltpu.make_async_copy(qd, qkv_hbm, q_sem)
    q_out.start()

    for k in range(7):
        stat_copy(k, me).wait_send()
    g_copy(yi).wait_send()
    x_copy(yi, 0).wait_send()
    x_copy(yi, 1).wait_send()
    yq_copy(yi).wait_send()

    @pl.loop(0, num_c)
    def _(i):
        own_copy(i).wait()

    @pl.loop(n1, n2)
    def _(i):
        perm_copy(i).wait()

    @pl.loop(n2, num_c)
    def _(i):
        send_copy(i).wait()

    q_out.wait()

    @pl.loop(0, n1)
    def _(i):
        x_send(i).wait()


def front(x_loc, gain_loc, wqkv, wgate, wup, d_model):
    rows, width = x_loc.shape
    depth, q_cols = wqkv.shape
    num_q, num_c = q_cols // CQ, wgate.shape[1] // C
    quarter = rows // 4
    dma = pltpu.SemaphoreType.DMA
    any_spec = pl.BlockSpec(memory_space=pl.ANY)
    return pl.pallas_call(
        functools.partial(front_kernel, d_model),
        name="front",
        out_shape=(
            jax.ShapeDtypeStruct((2, rows // 8, q_cols), BF16),
            jax.ShapeDtypeStruct((LOW + SHIFT, quarter, 2 * C), F32),
            jax.ShapeDtypeStruct((PERM, quarter, 2 * C), F32),
            jax.ShapeDtypeStruct((num_c - LOW - PERM, quarter, 2 * C), F32),
            jax.ShapeDtypeStruct((num_c, quarter, 2 * C), F32),
        ),
        in_specs=[any_spec] * 5,
        out_specs=(any_spec,) * 5,
        scratch_shapes=[
            pltpu.VMEM((8, 8, rows), F32),
            pltpu.VMEM((2, 2, rows // 2, width), BF16),
            pltpu.VMEM((width,), BF16),
            pltpu.VMEM((2, 8, width), F32),
            pltpu.VMEM((2, 2, rows // 2, 128), F32),
            pltpu.VMEM((2, rows // 2, depth), BF16),
            pltpu.VMEM((num_q, depth, CQ), BF16),
            pltpu.VMEM((SLOTS, depth, C), BF16),
            pltpu.VMEM((SLOTS, depth, C), BF16),
            pltpu.VMEM((num_q, 4, quarter, CQ), F32),
            pltpu.VMEM((num_q, 2, quarter, CQ), F32),
            pltpu.VMEM((num_q, quarter, CQ), F32),
            pltpu.VMEM((2, rows // 8, q_cols), BF16),
            pltpu.VMEM((2, rows // 8, q_cols), BF16),
            pltpu.VMEM((num_c, 4, quarter, 2 * C), F32),
            pltpu.VMEM((num_c, 2, quarter, 2 * C), F32),
            dma((2,)), dma((num_q,)), dma((SLOTS,)), dma((SLOTS,)), dma((7,)), dma((7,)), dma((3,)), dma((3,)),
            dma((num_q, 2)), dma((num_q, 2)), dma((num_q,)), dma((num_q,)), dma, dma,
            dma((num_c, 2)), dma((num_c, 2)), dma((LOW + SHIFT,)), dma((LOW + SHIFT,)), dma((num_c,)), dma((num_c,)), dma,
        ],
        compiler_params=pltpu.CompilerParams(collective_id=0, has_side_effects=True, vmem_limit_bytes=VMEM_LIMIT),
        cost_estimate=pl.CostEstimate(
            flops=2 * rows * depth * (q_cols + 2 * wgate.shape[1]),
            bytes_accessed=2 * depth * (q_cols + 2 * wgate.shape[1]),
            transcendentals=0,
        ),
    )(x_loc.reshape(2, rows // 2, width), gain_loc, wqkv, wgate, wup)


def attend_kernel(len_ref, qkv_ref, cos_ref, sin_ref, k_ref, v_ref, ko_ref, vo_ref, o_ref):
    ko_ref[...] = k_ref[...]
    vo_ref[...] = v_ref[...]
    for n in range(PER_STEP):
        pos = len_ref[pl.program_id(0) * PER_STEP + n]
        qkv = qkv_ref[n]
        heads, head_dim = qkv.shape[0] - 2, qkv.shape[1]
        wide = qkv.astype(F32)
        turned = (wide * cos_ref[n] + pltpu.roll(wide, head_dim // 2, 1) * sin_ref[n]).astype(BF16)
        query = turned[:heads]
        base = pl.multiple_of((pos // 16) * 16, 16)
        here = lax.broadcasted_iota(jnp.int32, (16, head_dim), 0) == pos - base
        for out, new in ((ko_ref, turned[heads:heads + 1]), (vo_ref, qkv[heads + 1:heads + 2])):
            tile = out[n, pl.ds(base, 16), :].astype(F32)
            out[n, pl.ds(base, 16), :] = jnp.where(here, new.astype(F32), tile).astype(BF16)
        scores = lax.dot_general(query, ko_ref[n], (((1,), (1,)), ((), ())), preferred_element_type=F32)
        scores = scores * head_dim ** -0.5
        at = lax.broadcasted_iota(jnp.int32, scores.shape, 1)
        scores = jnp.where(at <= pos, scores, -1e30)
        weight = jnp.exp(scores - jnp.max(scores, axis=1, keepdims=True))
        probs = (weight / jnp.sum(weight, axis=1, keepdims=True)).astype(BF16)
        o_ref[n] = jnp.dot(probs, vo_ref[n], preferred_element_type=F32).astype(BF16)


def attend(qkv, cos, sin, k_cache, v_cache, ctx_len):
    reqs, length, head_dim = k_cache.shape
    heads = qkv.shape[1] - 2
    cache_spec = pl.BlockSpec((PER_STEP, length, head_dim), lambda i, lens: (i, 0, 0))
    table_spec = pl.BlockSpec((PER_STEP, 1, head_dim), lambda i, lens: (i, 0, 0))
    return pl.pallas_call(
        attend_kernel,
        name="attend",
        grid_spec=pltpu.PrefetchScalarGridSpec(
            num_scalar_prefetch=1,
            grid=(reqs // PER_STEP,),
            in_specs=[
                pl.BlockSpec((PER_STEP, heads + 2, head_dim), lambda i, lens: (i, 0, 0)),
                table_spec, table_spec, cache_spec, cache_spec,
            ],
            out_specs=[cache_spec, cache_spec, pl.BlockSpec((PER_STEP, heads, head_dim), lambda i, lens: (i, 0, 0))],
        ),
        out_shape=(
            jax.ShapeDtypeStruct(k_cache.shape, BF16),
            jax.ShapeDtypeStruct(v_cache.shape, BF16),
            jax.ShapeDtypeStruct((reqs, heads, head_dim), BF16),
        ),
        compiler_params=pltpu.CompilerParams(dimension_semantics=("arbitrary",)),
        cost_estimate=pl.CostEstimate(
            flops=64 * reqs * heads * length * head_dim,
            bytes_accessed=8 * reqs * length * head_dim,
            transcendentals=reqs * heads * length,
        ),
    )(ctx_len, qkv, cos, sin, k_cache, v_cache)


def back_kernel(
    o_hbm, own_hbm, got_hbm, perm_hbm, send_hbm, wao_hbm, wmo_hbm, z_out,
    w, own, xr, act, z, zr,
    in_sem, out_sem, w_sem, own_sem, x_s, x_r, o_s, o_r, sib_s, sib_r, xn_s, xn_r, fwd_s, fwd_r, z_s, z_r,
):
    xi, yi, sib, xn, _, yn = places()
    sib_dev, xn_dev, yn_dev = {"x": sib}, {"x": xn}, {"yz": yn}
    width = z_out.shape[3]
    half_rows = act.shape[1] * act.shape[2]
    num_o, num_c = wao_hbm.shape[0] // C, wmo_hbm.shape[0] // C
    num_k = num_o + num_c
    o_cols = wao_hbm.shape[0]
    n1 = LOW + SHIFT * (xi % 2)
    n2 = n1 + PERM
    pieces = len(PIECES)
    starts = [FULL + sum(PIECES[:n]) for n in range(pieces + 1)]

    def w_copy(k):
        src = wao_hbm.at[pl.ds(k * C, C), :] if k < num_o else wmo_hbm.at[pl.ds((k - num_o) * C, C), :]
        return pltpu.make_async_copy(src, w.at[k], w_sem.at[k])

    def own_copy(i):
        return pltpu.make_async_copy(own_hbm.at[i], own.at[i], own_sem.at[i])

    def here_copy(src, i):
        return pltpu.make_async_copy(src, xr.at[i], x_r.at[i])

    def x_send(i):
        return remote(send_hbm.at[i - n2], xr.at[i], x_s.at[i - n2], x_r.at[i], xn_dev)

    barrier = pltpu.get_barrier_semaphore()
    for dev in (sib_dev, xn_dev, yn_dev):
        pl.semaphore_signal(barrier, inc=1, device_id=dev, device_id_type=MESH)
    o_in = pltpu.make_async_copy(o_hbm.at[yi], act.at[yi, xi, :, 0:o_cols], in_sem)
    o_in.start()

    @pl.loop(0, num_c)
    def _(i):
        own_copy(i).start()

    @pl.loop(0, n1)
    def _(i):
        here_copy(got_hbm.at[i], i).start()

    @pl.loop(n1, n2)
    def _(i):
        here_copy(perm_hbm.at[i - n1], i).start()

    pl.semaphore_wait(barrier, 3)

    def o_copy(half, row):
        return remote(o_hbm.at[half], act.at[row, xi, :, 0:o_cols], o_s, o_r, yn_dev)

    def block_of(e, owner):
        if e == 0:
            return act.at[:, owner, :, pl.ds(o_cols, FULL * C)]
        if e == 1:
            return act.at[:, owner, :, pl.ds(0, o_cols)]
        half, n = divmod(e - 2, pieces)
        return act.at[half, owner, :, pl.ds(o_cols + starts[n] * C, PIECES[n] * C)]

    def to_sib(e, owner):
        block = block_of(e, owner)
        return remote(block, block, sib_s.at[e], sib_r.at[e], sib_dev)

    def to_xn(e, owner):
        block = block_of(e, owner)
        return remote(block, block, xn_s.at[e], xn_r.at[e], xn_dev)

    def forward(e, owner):
        block = block_of(e, owner)
        return remote(block, block, fwd_s.at[e], fwd_r.at[e], sib_dev)

    def send_own(e):
        to_xn(e, xi).start()
        to_sib(e, xi).start()

    def pass_on(e):
        to_xn(e, xn).wait_recv()
        forward(e, xn).start()

    def arrived(e):
        to_sib(e, sib).wait_recv()
        forward(e, (sib + 2) % 4).wait_recv()

    def activate(i):
        own_copy(i).wait()
        value = activation(own[i] + xr[i])
        start = o_cols + i * C if isinstance(i, int) else pl.multiple_of(o_cols + i * C, C)
        act[:, xi, :, pl.ds(start, C)] = value.reshape(2, value.shape[0] // 2, C)

    def w_wait(k):
        pltpu.make_async_copy(wmo_hbm.at[pl.ds(0, C), :], w.at[k], w_sem.at[k]).wait()

    def multiply(first, count):
        @pl.loop(first, first + count)
        def _(k):
            w_wait(k)
            lhs = act[:, :, :, pl.ds(pl.multiple_of(k * C, C), C)].reshape(2 * half_rows, C)
            for b in range(2):
                prod = jnp.dot(lhs, w[k, :, b * width:(b + 1) * width], preferred_element_type=F32)
                z[b] = z[b] + prod.reshape(z.shape[1:])

    def multiply_one(half, n, b):
        @pl.loop(num_o + starts[n], num_o + starts[n + 1])
        def _(k):
            lhs = act[half, :, :, pl.ds(pl.multiple_of(k * C, C), C)].reshape(half_rows, C)
            cols = pl.ds(pl.multiple_of(b * width, width), width)
            prod = jnp.dot(lhs, w[k, :, cols], preferred_element_type=F32)
            z[b, half] = z[b, half] + prod.reshape(z.shape[2:])

    def multiply_half(half, n):
        @pl.loop(num_o + starts[n], num_o + starts[n + 1])
        def _(k):
            if half == 0:
                w_wait(k)
            lhs = act[half, :, :, pl.ds(pl.multiple_of(k * C, C), C)].reshape(half_rows, C)
            for b in range(2):
                prod = jnp.dot(lhs, w[k, :, b * width:(b + 1) * width], preferred_element_type=F32)
                z[b, half] = z[b, half] + prod.reshape(z.shape[2:])

    @pl.loop(n2, num_c)
    def _(i):
        x_send(i).start()

    o_copy(yn, yi).start()
    for k in range(num_k):
        w_copy(k).start()
    z[...] = jnp.zeros_like(z)

    def start_here(i):
        here_copy(got_hbm.at[0], i).wait()
        activate(i)

    pl.loop(0, FULL)(start_here)
    o_in.wait()
    o_copy(yi, yn).wait_recv()
    send_own(1)
    send_own(0)
    pl.loop(FULL, n2)(start_here)
    ready = sum(end <= LOW + PERM for end in starts[1:])
    for n in range(ready):
        send_own(2 + n)

    @pl.loop(n2, num_c)
    def _(i):
        x_send(i).wait_recv()
        activate(i)

    groups = 2 + 2 * pieces
    for e in range(2 + ready, groups):
        send_own(e)
    pass_on(1)
    pass_on(0)
    arrived(1)
    multiply(0, num_o)
    arrived(0)
    multiply(num_o, FULL)
    z_copies = [remote(z.at[yn, half], zr.at[half], z_s.at[half], z_r.at[half], yn_dev) for half in range(2)]
    pass_on(2)
    for e in range(2, groups):
        if e + 1 < groups:
            pass_on(e + 1)
        arrived(e)
        half, n = divmod(e - 2, pieces)
        if e + 1 < groups:
            multiply_half(half, n)
        else:
            multiply_one(half, n, yn)
        if n == pieces - 1:
            z_copies[half].start()
    multiply_one(1, pieces - 1, yi)

    o_copy(yn, yi).wait_send()
    for e in range(groups):
        to_xn(e, xi).wait_send()
        to_sib(e, xi).wait_send()
        forward(e, xn).wait_send()

    @pl.loop(n2, num_c)
    def _(i):
        x_send(i).wait_send()

    outs = [pltpu.make_async_copy(zr.at[half], z_out.at[:, half], out_sem.at[half]) for half in range(2)]
    for half in range(2):
        z_copies[half].wait()
        zr[half] = z[yi, half] + zr[half]
        outs[half].start()
    for half in range(2):
        outs[half].wait()


def back(x_loc, o_halves, own, got, perm, send, wao, wmo):
    rows, width = x_loc.shape
    num_o, num_c = wao.shape[0] // C, wmo.shape[0] // C
    num_k = num_o + num_c
    groups = 2 + 2 * len(PIECES)
    quarter = rows // 4
    dma = pltpu.SemaphoreType.DMA
    any_spec = pl.BlockSpec(memory_space=pl.ANY)
    z = pl.pallas_call(
        back_kernel,
        name="back",
        out_shape=jax.ShapeDtypeStruct((4, 2, rows // 8, width), F32),
        in_specs=[any_spec] * 7,
        out_specs=any_spec,
        scratch_shapes=[
            pltpu.VMEM((num_k, C, 2 * width), BF16),
            pltpu.VMEM((num_c, quarter, 2 * C), F32),
            pltpu.VMEM((num_c, quarter, 2 * C), F32),
            pltpu.VMEM((2, 4, rows // 8, num_k * C), BF16),
            pltpu.VMEM((2, 2, 4, rows // 8, width), F32),
            pltpu.VMEM((2, 4, rows // 8, width), F32),
            dma, dma((2,)), dma((num_k,)), dma((num_c,)), dma((num_c - LOW - PERM,)), dma((num_c,)), dma, dma,
            dma((groups,)), dma((groups,)), dma((groups,)), dma((groups,)), dma((groups,)), dma((groups,)),
            dma((2,)), dma((2,)),
        ],
        compiler_params=pltpu.CompilerParams(collective_id=1, has_side_effects=True, vmem_limit_bytes=VMEM_LIMIT),
        cost_estimate=pl.CostEstimate(
            flops=4 * rows * num_k * C * width, bytes_accessed=4 * num_k * C * width, transcendentals=0
        ),
    )(o_halves, own, got, perm, send, wao, wmo)
    return (x_loc.astype(F32) + z.reshape(rows, width)).astype(BF16)


def solution(mesh):
    x_size, yz_size = mesh.shape["x"], mesh.shape["yz"]
    both_axes = ("x", "yz")
    row_spec = P("dp", both_axes)
    in_w_spec = P("x", "yz")
    out_w_spec = P("yz", "x")
    cache_spec = P(("dp", "x", "yz"), None, None)
    len_spec = P(("dp", "x", "yz"))
    across = [(i, (i + 2) % 4) for i in range(4)]

    def local_layer(x_loc, gain_loc, wqkv_loc, wgate_loc, wup_loc, wao_loc, wmo_loc, kc_loc, vc_loc, len_loc):
        d_model = x_loc.shape[1] * x_size * yz_size
        reqs, _, head_dim = kc_loc.shape
        half = head_dim // 2
        inv_freq = 10000.0 ** (-jnp.arange(half, dtype=F32) / half)
        angles = len_loc.astype(F32)[:, None] * inv_freq
        cos, sin = jnp.cos(angles), jnp.sin(angles)
        cos = jnp.concatenate([cos, cos], axis=1)[:, None, :]
        sin = jnp.concatenate([-sin, sin], axis=1)[:, None, :]

        qkv, got, perm, send, own = front(
            x_loc, gain_loc, wqkv_loc, wgate_loc, wup_loc, d_model
        )
        perm = lax.ppermute(perm, "x", across)
        qkv = jnp.concatenate([qkv[0], qkv[1]], axis=1).reshape(reqs, -1, head_dim)
        k_all, v_all, attn = attend(qkv, cos, sin, kc_loc, vc_loc, len_loc)
        o_halves = jnp.swapaxes(attn.reshape(reqs, 2, -1), 0, 1)
        y_loc = back(x_loc, o_halves, own, got, perm, send, wao_loc, wmo_loc)
        return y_loc, k_all, v_all

    in_specs = (row_spec, P(both_axes), in_w_spec, in_w_spec, in_w_spec, out_w_spec, out_w_spec, cache_spec, cache_spec, len_spec)
    out_specs = (row_spec, cache_spec, cache_spec)
    return jax.shard_map(local_layer, mesh=mesh, in_specs=in_specs, out_specs=out_specs, check_vma=False)
```

```python
import functools

import jax
import jax.numpy as jnp
from jax import lax
from jax.experimental import pallas as pl
from jax.experimental.pallas import tpu as pltpu
from jax.sharding import PartitionSpec as P

MESH = pl.DeviceIdType.MESH
F32 = jnp.float32
BF16 = jnp.bfloat16
VMEM_LIMIT = 66_900_000

C = 768
CQ = 640
PER_STEP = 2
SLOTS = 3
LOW, SHIFT, PERM = 5, 1, 8
FULL = 5
PIECES = (8, 3)


def remote(src, dst, send_sem, recv_sem, device):
    return pltpu.make_async_remote_copy(
        src_ref=src, dst_ref=dst, send_sem=send_sem, recv_sem=recv_sem, device_id=device, device_id_type=MESH
    )


def places():
    xi = lax.axis_index("x")
    yi = lax.axis_index("yz")
    sib = xi + 1 - 2 * (xi % 2)
    xn = (xi + 2) % 4
    return xi, yi, sib, xn, (sib + 2) % 4, 1 - yi


def activation(total):
    gate = total[:, :C].astype(BF16).astype(F32)
    up = total[:, C:].astype(BF16).astype(F32)
    return (jax.nn.silu(gate) * up).astype(BF16)


def front_kernel(
    d_model, x_hbm, g_hbm, wq_hbm, wg_hbm, wu_hbm,
    qkv_hbm, got_hbm, perm_hbm, send_hbm, own_hbm,
    stat, xbuf, gain, gbuf, moments, h, wq, wg, wu, pq, rq, xq, qs, qd, p, r,
    in_sem, wq_sem, wg_sem, wu_sem, st_s, st_r, xg_s, xg_r,
    dq_s, dq_r, xq_s, xq_r, yq_s, yq_r, d_s, d_r, x_s, x_r, out_sem, own_sem, q_sem,
):
    xi, yi, sib, xn, sibn, yn = places()
    me = yi * 4 + xi
    sides, side_rows, width = x_hbm.shape
    rows = sides * side_rows
    n1 = LOW + SHIFT * (xi % 2)
    n2 = n1 + PERM
    near = xi // 2
    far = 1 - near
    num_q = wq_hbm.shape[1] // CQ
    num_c = wg_hbm.shape[1] // C
    sib_dev, xn_dev, yn_dev = {"x": sib}, {"x": xn}, {"yz": yn}

    def wq_copy(c):
        return pltpu.make_async_copy(wq_hbm.at[:, pl.ds(c * CQ, CQ)], wq.at[c], wq_sem.at[c])

    def w_copies(i, slot):
        start = pl.multiple_of(i * C, C)
        return (
            pltpu.make_async_copy(wg_hbm.at[:, pl.ds(start, C)], wg.at[slot], wg_sem.at[slot]),
            pltpu.make_async_copy(wu_hbm.at[:, pl.ds(start, C)], wu.at[slot], wu_sem.at[slot]),
        )

    x_in = pltpu.make_async_copy(x_hbm, xbuf.at[yi], in_sem.at[0])
    g_in = pltpu.make_async_copy(g_hbm, gain, in_sem.at[1])
    x_in.start()
    g_in.start()
    barrier = pltpu.get_barrier_semaphore()
    offsets = [(dy, dx) for dy in range(2) for dx in range(4)][1:]
    for dy, dx in offsets:
        pl.semaphore_signal(barrier, inc=1, device_id={"yz": (yi + dy) % 2, "x": (xi + dx) % 4}, device_id_type=MESH)

    x_in.wait()
    x_f32 = xbuf[yi].reshape(rows, width).astype(F32)
    lane = lax.broadcasted_iota(jnp.int32, (rows, rows), 1)
    sums = jnp.where(
        lane == 0,
        jnp.sum(x_f32, axis=1, keepdims=True),
        jnp.where(lane == 1, jnp.sum(x_f32 * x_f32, axis=1, keepdims=True), 0.0),
    )
    stat[me] = sums.T[0:8, :]
    g_in.wait()
    gbuf[yi] = jnp.broadcast_to(gain[...].astype(F32)[None, :], (8, width))
    pl.semaphore_wait(barrier, 7)

    def stat_copy(k, slot):
        dy, dx = offsets[k]
        dev = {"yz": (yi + dy) % 2, "x": (xi + dx) % 4}
        return remote(stat.at[slot], stat.at[slot], st_s.at[k], st_r.at[k], dev)

    def x_copy(slot, n):
        block = xbuf.at[slot, (far, near)[n]]
        return remote(block, block, xg_s.at[1 + n], xg_r.at[1 + n], yn_dev)

    def g_copy(slot):
        return remote(gbuf.at[slot], gbuf.at[slot], xg_s.at[0], xg_r.at[0], yn_dev)

    for k in range(7):
        stat_copy(k, me).start()
    g_copy(yi).start()
    x_copy(yi, 0).start()
    x_copy(yi, 1).start()
    for c in range(num_q):
        wq_copy(c).start()
    for i in range(SLOTS):
        for copy in w_copies(i, i):
            copy.start()
    for k, (dy, dx) in enumerate(offsets):
        stat_copy(k, ((yi + 2 - dy) % 2) * 4 + (xi + 4 - dx) % 4).wait_recv()
    total = stat[0]
    for k in range(1, 8):
        total = total + stat[k]
    cols = jnp.concatenate([total, jnp.zeros((rows - 8, rows), F32)], axis=0).T
    mean = cols[:, 0:1] / d_model
    var = cols[:, 1:2] / d_model - mean * mean
    moments[0] = jnp.broadcast_to(mean, (rows, 128)).reshape(sides, side_rows, 128)
    moments[1] = jnp.broadcast_to(lax.rsqrt(var + 1e-6), (rows, 128)).reshape(sides, side_rows, 128)
    g_copy(yn).wait_recv()

    def normalize(side):
        for b in range(2):
            part = (xbuf[b, side].astype(F32) - moments[0, side][:, 0:1]) * moments[1, side][:, 0:1]
            h[side, :, b * width:(b + 1) * width] = (part * gbuf[b][0:1, :]).astype(BF16)

    def dq(c, k):
        src = sib if k == 0 else sibn
        return remote(pq.at[c, src], rq.at[c, k], dq_s.at[c, k], dq_r.at[c, k], sib_dev)

    def xq_copy(c):
        return remote(pq.at[c, xn], xq.at[c], xq_s.at[c], xq_r.at[c], xn_dev)

    def q_product(c, side):
        prod = jnp.dot(h[side], wq[c], preferred_element_type=F32)
        pq[c, pl.ds(2 * side, 2)] = prod.reshape(2, rows // 4, CQ)

    def q_send(c):
        dq(c, 1).wait_recv()
        dq(c, 1).wait_send()
        pq[c, xn] = pq[c, xn] + rq[c, 1]
        xq_copy(c).start()

    x_copy(yn, 0).wait_recv()
    normalize(far)

    @pl.loop(0, num_q)
    def _(c):
        wq_copy(c).wait()
        q_product(c, far)
        dq(c, 1).start()

        @pl.when(c >= 1)
        def _():
            q_send(c - 1)

    x_copy(yn, 1).wait_recv()
    normalize(near)
    q_send(num_q - 1)

    @pl.loop(0, num_q)
    def _(c):
        q_product(c, near)
        dq(c, 0).start()

    def d_copy(i, k):
        src = sib if k == 0 else sibn
        return remote(p.at[i, src], r.at[i, k], d_s.at[i, k], d_r.at[i, k], sib_dev)

    def x_send(i):
        return remote(p.at[i, xn], got_hbm.at[i], x_s.at[i], x_r.at[i], xn_dev)

    def perm_copy(i):
        return pltpu.make_async_copy(p.at[i, xn], perm_hbm.at[i - n1], out_sem.at[i])

    def send_copy(i):
        return pltpu.make_async_copy(p.at[i, xn], send_hbm.at[i - n2], out_sem.at[i])

    def own_copy(i):
        return pltpu.make_async_copy(p.at[i, xi], own_hbm.at[i], own_sem.at[i])

    def chip_sum(i):
        d_copy(i, 1).wait_recv()
        d_copy(i, 1).wait_send()
        p[i, xn] = p[i, xn] + r[i, 1]

        @pl.when(i < n1)
        def _():
            x_send(i).start()

        @pl.when((i >= n1) & (i < n2))
        def _():
            perm_copy(i).start()

        @pl.when(i >= n2)
        def _():
            send_copy(i).start()

        d_copy(i, 0).wait_recv()
        d_copy(i, 0).wait_send()
        p[i, xi] = p[i, xi] + r[i, 0]
        own_copy(i).start()

    def product(i):
        slot = i % SLOTS
        g_w, u_w = w_copies(i, slot)
        h_all = h[...].reshape(rows, h.shape[2])
        g_w.wait()
        p[i, :, :, :C] = jnp.dot(h_all, wg[slot], preferred_element_type=F32).reshape(4, rows // 4, C)
        u_w.wait()
        p[i, :, :, C:] = jnp.dot(h_all, wu[slot], preferred_element_type=F32).reshape(4, rows // 4, C)
        d_copy(i, 1).start()
        d_copy(i, 0).start()

        @pl.when(i + SLOTS < num_c)
        def _():
            for copy in w_copies(i + SLOTS, slot):
                copy.start()

    product(0)

    def step(i):
        product(i)
        chip_sum(i - 1)

    half = num_c // 2 + 1
    pl.loop(1, half)(step)

    @pl.loop(0, num_q)
    def _(c):
        dq(c, 0).wait_recv()
        dq(c, 0).wait_send()
        mine = pq[c, xi] + rq[c, 0]
        xq_copy(c).wait_recv()
        xq_copy(c).wait_send()
        value = (mine + xq[c]).astype(BF16)
        qs[:, :, pl.ds(pl.multiple_of(c * CQ, CQ), CQ)] = value.reshape(2, rows // 8, CQ)

    def yq_copy(k):
        return remote(qs.at[1 - k], qd.at[k], yq_s, yq_r, yn_dev)

    yq_copy(yi).start()
    qd[yi] = qs[yi]

    pl.loop(half, num_c)(step)
    chip_sum(num_c - 1)
    yq_copy(yn).wait_recv()
    q_out = pltpu.make_async_copy(qd, qkv_hbm, q_sem)
    q_out.start()

    for k in range(7):
        stat_copy(k, me).wait_send()
    g_copy(yi).wait_send()
    x_copy(yi, 0).wait_send()
    x_copy(yi, 1).wait_send()
    yq_copy(yi).wait_send()

    @pl.loop(0, num_c)
    def _(i):
        own_copy(i).wait()

    @pl.loop(n1, n2)
    def _(i):
        perm_copy(i).wait()

    @pl.loop(n2, num_c)
    def _(i):
        send_copy(i).wait()

    q_out.wait()

    @pl.loop(0, n1)
    def _(i):
        x_send(i).wait()


def front(x_loc, gain_loc, wqkv, wgate, wup, d_model):
    rows, width = x_loc.shape
    depth, q_cols = wqkv.shape
    num_q, num_c = q_cols // CQ, wgate.shape[1] // C
    quarter = rows // 4
    dma = pltpu.SemaphoreType.DMA
    any_spec = pl.BlockSpec(memory_space=pl.ANY)
    return pl.pallas_call(
        functools.partial(front_kernel, d_model),
        name="front",
        out_shape=(
            jax.ShapeDtypeStruct((2, rows // 8, q_cols), BF16),
            jax.ShapeDtypeStruct((LOW + SHIFT, quarter, 2 * C), F32),
            jax.ShapeDtypeStruct((PERM, quarter, 2 * C), F32),
            jax.ShapeDtypeStruct((num_c - LOW - PERM, quarter, 2 * C), F32),
            jax.ShapeDtypeStruct((num_c, quarter, 2 * C), F32),
        ),
        in_specs=[any_spec] * 5,
        out_specs=(any_spec,) * 5,
        scratch_shapes=[
            pltpu.VMEM((8, 8, rows), F32),
            pltpu.VMEM((2, 2, rows // 2, width), BF16),
            pltpu.VMEM((width,), BF16),
            pltpu.VMEM((2, 8, width), F32),
            pltpu.VMEM((2, 2, rows // 2, 128), F32),
            pltpu.VMEM((2, rows // 2, depth), BF16),
            pltpu.VMEM((num_q, depth, CQ), BF16),
            pltpu.VMEM((SLOTS, depth, C), BF16),
            pltpu.VMEM((SLOTS, depth, C), BF16),
            pltpu.VMEM((num_q, 4, quarter, CQ), F32),
            pltpu.VMEM((num_q, 2, quarter, CQ), F32),
            pltpu.VMEM((num_q, quarter, CQ), F32),
            pltpu.VMEM((2, rows // 8, q_cols), BF16),
            pltpu.VMEM((2, rows // 8, q_cols), BF16),
            pltpu.VMEM((num_c, 4, quarter, 2 * C), F32),
            pltpu.VMEM((num_c, 2, quarter, 2 * C), F32),
            dma((2,)), dma((num_q,)), dma((SLOTS,)), dma((SLOTS,)), dma((7,)), dma((7,)), dma((3,)), dma((3,)),
            dma((num_q, 2)), dma((num_q, 2)), dma((num_q,)), dma((num_q,)), dma, dma,
            dma((num_c, 2)), dma((num_c, 2)), dma((LOW + SHIFT,)), dma((LOW + SHIFT,)), dma((num_c,)), dma((num_c,)), dma,
        ],
        compiler_params=pltpu.CompilerParams(collective_id=0, has_side_effects=True, vmem_limit_bytes=VMEM_LIMIT),
        cost_estimate=pl.CostEstimate(
            flops=2 * rows * depth * (q_cols + 2 * wgate.shape[1]),
            bytes_accessed=2 * depth * (q_cols + 2 * wgate.shape[1]),
            transcendentals=0,
        ),
    )(x_loc.reshape(2, rows // 2, width), gain_loc, wqkv, wgate, wup)


def attend_kernel(len_ref, qkv_ref, cos_ref, sin_ref, k_ref, v_ref, ko_ref, vo_ref, o_ref):
    ko_ref[...] = k_ref[...]
    vo_ref[...] = v_ref[...]
    for n in range(PER_STEP):
        pos = len_ref[pl.program_id(0) * PER_STEP + n]
        qkv = qkv_ref[n]
        heads, head_dim = qkv.shape[0] - 2, qkv.shape[1]
        wide = qkv.astype(F32)
        turned = (wide * cos_ref[n] + pltpu.roll(wide, head_dim // 2, 1) * sin_ref[n]).astype(BF16)
        query = turned[:heads]
        base = pl.multiple_of((pos // 16) * 16, 16)
        here = lax.broadcasted_iota(jnp.int32, (16, head_dim), 0) == pos - base
        for out, new in ((ko_ref, turned[heads:heads + 1]), (vo_ref, qkv[heads + 1:heads + 2])):
            tile = out[n, pl.ds(base, 16), :].astype(F32)
            out[n, pl.ds(base, 16), :] = jnp.where(here, new.astype(F32), tile).astype(BF16)
        scores = lax.dot_general(query, ko_ref[n], (((1,), (1,)), ((), ())), preferred_element_type=F32)
        scores = scores * head_dim ** -0.5
        at = lax.broadcasted_iota(jnp.int32, scores.shape, 1)
        scores = jnp.where(at <= pos, scores, -1e30)
        weight = jnp.exp(scores - jnp.max(scores, axis=1, keepdims=True))
        probs = (weight / jnp.sum(weight, axis=1, keepdims=True)).astype(BF16)
        o_ref[n] = jnp.dot(probs, vo_ref[n], preferred_element_type=F32).astype(BF16)


def attend(qkv, cos, sin, k_cache, v_cache, ctx_len):
    reqs, length, head_dim = k_cache.shape
    heads = qkv.shape[1] - 2
    cache_spec = pl.BlockSpec((PER_STEP, length, head_dim), lambda i, lens: (i, 0, 0))
    table_spec = pl.BlockSpec((PER_STEP, 1, head_dim), lambda i, lens: (i, 0, 0))
    return pl.pallas_call(
        attend_kernel,
        name="attend",
        grid_spec=pltpu.PrefetchScalarGridSpec(
            num_scalar_prefetch=1,
            grid=(reqs // PER_STEP,),
            in_specs=[
                pl.BlockSpec((PER_STEP, heads + 2, head_dim), lambda i, lens: (i, 0, 0)),
                table_spec, table_spec, cache_spec, cache_spec,
            ],
            out_specs=[cache_spec, cache_spec, pl.BlockSpec((PER_STEP, heads, head_dim), lambda i, lens: (i, 0, 0))],
        ),
        out_shape=(
            jax.ShapeDtypeStruct(k_cache.shape, BF16),
            jax.ShapeDtypeStruct(v_cache.shape, BF16),
            jax.ShapeDtypeStruct((reqs, heads, head_dim), BF16),
        ),
        compiler_params=pltpu.CompilerParams(dimension_semantics=("arbitrary",)),
        cost_estimate=pl.CostEstimate(
            flops=64 * reqs * heads * length * head_dim,
            bytes_accessed=8 * reqs * length * head_dim,
            transcendentals=reqs * heads * length,
        ),
    )(ctx_len, qkv, cos, sin, k_cache, v_cache)


def back_kernel(
    o_hbm, own_hbm, got_hbm, perm_hbm, send_hbm, wao_hbm, wmo_hbm, z_out,
    w, own, xr, act, z, zr,
    in_sem, out_sem, w_sem, own_sem, x_s, x_r, o_s, o_r, sib_s, sib_r, xn_s, xn_r, fwd_s, fwd_r, z_s, z_r,
):
    xi, yi, sib, xn, _, yn = places()
    sib_dev, xn_dev, yn_dev = {"x": sib}, {"x": xn}, {"yz": yn}
    width = z_out.shape[3]
    half_rows = act.shape[1] * act.shape[2]
    num_o, num_c = wao_hbm.shape[0] // C, wmo_hbm.shape[0] // C
    num_k = num_o + num_c
    o_cols = wao_hbm.shape[0]
    n1 = LOW + SHIFT * (xi % 2)
    n2 = n1 + PERM
    pieces = len(PIECES)
    starts = [FULL + sum(PIECES[:n]) for n in range(pieces + 1)]

    def w_copy(k):
        src = wao_hbm.at[pl.ds(k * C, C), :] if k < num_o else wmo_hbm.at[pl.ds((k - num_o) * C, C), :]
        return pltpu.make_async_copy(src, w.at[k], w_sem.at[k])

    def own_copy(i):
        return pltpu.make_async_copy(own_hbm.at[i], own.at[i], own_sem.at[i])

    def here_copy(src, i):
        return pltpu.make_async_copy(src, xr.at[i], x_r.at[i])

    def x_send(i):
        return remote(send_hbm.at[i - n2], xr.at[i], x_s.at[i - n2], x_r.at[i], xn_dev)

    barrier = pltpu.get_barrier_semaphore()
    for dev in (sib_dev, xn_dev, yn_dev):
        pl.semaphore_signal(barrier, inc=1, device_id=dev, device_id_type=MESH)
    o_in = pltpu.make_async_copy(o_hbm.at[yi], act.at[yi, xi, :, 0:o_cols], in_sem)
    o_in.start()

    @pl.loop(0, num_c)
    def _(i):
        own_copy(i).start()

    @pl.loop(0, n1)
    def _(i):
        here_copy(got_hbm.at[i], i).start()

    @pl.loop(n1, n2)
    def _(i):
        here_copy(perm_hbm.at[i - n1], i).start()

    pl.semaphore_wait(barrier, 3)

    def o_copy(half, row):
        return remote(o_hbm.at[half], act.at[row, xi, :, 0:o_cols], o_s, o_r, yn_dev)

    def block_of(e, owner):
        if e == 0:
            return act.at[:, owner, :, pl.ds(o_cols, FULL * C)]
        if e == 1:
            return act.at[:, owner, :, pl.ds(0, o_cols)]
        half, n = divmod(e - 2, pieces)
        return act.at[half, owner, :, pl.ds(o_cols + starts[n] * C, PIECES[n] * C)]

    def to_sib(e, owner):
        block = block_of(e, owner)
        return remote(block, block, sib_s.at[e], sib_r.at[e], sib_dev)

    def to_xn(e, owner):
        block = block_of(e, owner)
        return remote(block, block, xn_s.at[e], xn_r.at[e], xn_dev)

    def forward(e, owner):
        block = block_of(e, owner)
        return remote(block, block, fwd_s.at[e], fwd_r.at[e], sib_dev)

    def send_own(e):
        to_xn(e, xi).start()
        to_sib(e, xi).start()

    def pass_on(e):
        to_xn(e, xn).wait_recv()
        forward(e, xn).start()

    def arrived(e):
        to_sib(e, sib).wait_recv()
        forward(e, (sib + 2) % 4).wait_recv()

    def activate(i):
        own_copy(i).wait()
        value = activation(own[i] + xr[i])
        start = o_cols + i * C if isinstance(i, int) else pl.multiple_of(o_cols + i * C, C)
        act[:, xi, :, pl.ds(start, C)] = value.reshape(2, value.shape[0] // 2, C)

    def w_wait(k):
        pltpu.make_async_copy(wmo_hbm.at[pl.ds(0, C), :], w.at[k], w_sem.at[k]).wait()

    def multiply(first, count):
        @pl.loop(first, first + count)
        def _(k):
            w_wait(k)
            lhs = act[:, :, :, pl.ds(pl.multiple_of(k * C, C), C)].reshape(2 * half_rows, C)
            for b in range(2):
                prod = jnp.dot(lhs, w[k, :, b * width:(b + 1) * width], preferred_element_type=F32)
                z[b] = z[b] + prod.reshape(z.shape[1:])

    def multiply_one(half, n, b):
        @pl.loop(num_o + starts[n], num_o + starts[n + 1])
        def _(k):
            lhs = act[half, :, :, pl.ds(pl.multiple_of(k * C, C), C)].reshape(half_rows, C)
            cols = pl.ds(pl.multiple_of(b * width, width), width)
            prod = jnp.dot(lhs, w[k, :, cols], preferred_element_type=F32)
            z[b, half] = z[b, half] + prod.reshape(z.shape[2:])

    def multiply_half(half, n):
        @pl.loop(num_o + starts[n], num_o + starts[n + 1])
        def _(k):
            if half == 0:
                w_wait(k)
            lhs = act[half, :, :, pl.ds(pl.multiple_of(k * C, C), C)].reshape(half_rows, C)
            for b in range(2):
                prod = jnp.dot(lhs, w[k, :, b * width:(b + 1) * width], preferred_element_type=F32)
                z[b, half] = z[b, half] + prod.reshape(z.shape[2:])

    middle = num_c - 1

    @pl.loop(n2, middle)
    def _(i):
        x_send(i).start()

    o_copy(yn, yi).start()
    for k in range(num_o):
        w_copy(k).start()
    z[...] = jnp.zeros_like(z)

    def start_here(i):
        here_copy(got_hbm.at[0], i).wait()
        activate(i)

    pl.loop(0, FULL)(start_here)
    o_in.wait()
    o_copy(yi, yn).wait_recv()
    send_own(1)
    send_own(0)
    x_send(middle).start()
    for k in range(num_o, num_k):
        w_copy(k).start()
    pl.loop(FULL, n2)(start_here)
    ready = sum(end <= LOW + PERM for end in starts[1:])
    for n in range(ready):
        send_own(2 + n)

    @pl.loop(n2, middle)
    def _(i):
        x_send(i).wait_recv()
        activate(i)

    pass_on(1)
    arrived(1)
    multiply(0, num_o)
    pass_on(0)
    x_send(middle).wait_recv()
    activate(middle)
    groups = 2 + 2 * pieces
    for e in range(2 + ready, groups):
        send_own(e)
    arrived(0)
    multiply(num_o, FULL)
    z_copies = [remote(z.at[yn, half], zr.at[half], z_s.at[half], z_r.at[half], yn_dev) for half in range(2)]
    pass_on(2)
    for e in range(2, groups):
        if e + 1 < groups:
            pass_on(e + 1)
        arrived(e)
        half, n = divmod(e - 2, pieces)
        if e + 1 < groups:
            multiply_half(half, n)
        else:
            multiply_one(half, n, yn)
        if n == pieces - 1:
            z_copies[half].start()
    multiply_one(1, pieces - 1, yi)

    o_copy(yn, yi).wait_send()
    for e in range(groups):
        to_xn(e, xi).wait_send()
        to_sib(e, xi).wait_send()
        forward(e, xn).wait_send()

    @pl.loop(n2, num_c)
    def _(i):
        x_send(i).wait_send()

    outs = [pltpu.make_async_copy(zr.at[half], z_out.at[:, half], out_sem.at[half]) for half in range(2)]
    for half in range(2):
        z_copies[half].wait()
        zr[half] = z[yi, half] + zr[half]
        outs[half].start()
    for half in range(2):
        outs[half].wait()


def back(x_loc, o_halves, own, got, perm, send, wao, wmo):
    rows, width = x_loc.shape
    num_o, num_c = wao.shape[0] // C, wmo.shape[0] // C
    num_k = num_o + num_c
    groups = 2 + 2 * len(PIECES)
    quarter = rows // 4
    dma = pltpu.SemaphoreType.DMA
    any_spec = pl.BlockSpec(memory_space=pl.ANY)
    z = pl.pallas_call(
        back_kernel,
        name="back",
        out_shape=jax.ShapeDtypeStruct((4, 2, rows // 8, width), F32),
        in_specs=[any_spec] * 7,
        out_specs=any_spec,
        scratch_shapes=[
            pltpu.VMEM((num_k, C, 2 * width), BF16),
            pltpu.VMEM((num_c, quarter, 2 * C), F32),
            pltpu.VMEM((num_c, quarter, 2 * C), F32),
            pltpu.VMEM((2, 4, rows // 8, num_k * C), BF16),
            pltpu.VMEM((2, 2, 4, rows // 8, width), F32),
            pltpu.VMEM((2, 4, rows // 8, width), F32),
            dma, dma((2,)), dma((num_k,)), dma((num_c,)), dma((num_c - LOW - PERM,)), dma((num_c,)), dma, dma,
            dma((groups,)), dma((groups,)), dma((groups,)), dma((groups,)), dma((groups,)), dma((groups,)),
            dma((2,)), dma((2,)),
        ],
        compiler_params=pltpu.CompilerParams(collective_id=1, has_side_effects=True, vmem_limit_bytes=VMEM_LIMIT),
        cost_estimate=pl.CostEstimate(
            flops=4 * rows * num_k * C * width, bytes_accessed=4 * num_k * C * width, transcendentals=0
        ),
    )(o_halves, own, got, perm, send, wao, wmo)
    return (x_loc.astype(F32) + z.reshape(rows, width)).astype(BF16)


def solution(mesh):
    x_size, yz_size = mesh.shape["x"], mesh.shape["yz"]
    both_axes = ("x", "yz")
    row_spec = P("dp", both_axes)
    in_w_spec = P("x", "yz")
    out_w_spec = P("yz", "x")
    cache_spec = P(("dp", "x", "yz"), None, None)
    len_spec = P(("dp", "x", "yz"))
    across = [(i, (i + 2) % 4) for i in range(4)]

    def local_layer(x_loc, gain_loc, wqkv_loc, wgate_loc, wup_loc, wao_loc, wmo_loc, kc_loc, vc_loc, len_loc):
        d_model = x_loc.shape[1] * x_size * yz_size
        reqs, _, head_dim = kc_loc.shape
        half = head_dim // 2
        inv_freq = 10000.0 ** (-jnp.arange(half, dtype=F32) / half)
        angles = len_loc.astype(F32)[:, None] * inv_freq
        cos, sin = jnp.cos(angles), jnp.sin(angles)
        cos = jnp.concatenate([cos, cos], axis=1)[:, None, :]
        sin = jnp.concatenate([-sin, sin], axis=1)[:, None, :]

        qkv, got, perm, send, own = front(
            x_loc, gain_loc, wqkv_loc, wgate_loc, wup_loc, d_model
        )
        perm = lax.ppermute(perm, "x", across)
        qkv = jnp.concatenate([qkv[0], qkv[1]], axis=1).reshape(reqs, -1, head_dim)
        k_all, v_all, attn = attend(qkv, cos, sin, kc_loc, vc_loc, len_loc)
        o_halves = jnp.swapaxes(attn.reshape(reqs, 2, -1), 0, 1)
        y_loc = back(x_loc, o_halves, own, got, perm, send, wao_loc, wmo_loc)
        return y_loc, k_all, v_all

    in_specs = (row_spec, P(both_axes), in_w_spec, in_w_spec, in_w_spec, out_w_spec, out_w_spec, cache_spec, cache_spec, len_spec)
    out_specs = (row_spec, cache_spec, cache_spec)
    return jax.shard_map(local_layer, mesh=mesh, in_specs=in_specs, out_specs=out_specs, check_vma=False)
```

```python
import functools

import jax
import jax.numpy as jnp
from jax import lax
from jax.experimental import pallas as pl
from jax.experimental.pallas import tpu as pltpu
from jax.sharding import PartitionSpec as P

MESH = pl.DeviceIdType.MESH
F32 = jnp.float32
BF16 = jnp.bfloat16
VMEM_LIMIT = 66_900_000

C = 768
CQ = 640
PER_STEP = 2
SLOTS = 3
LOW, SHIFT, PERM = 5, 0, 8
FULL = 5
PIECES = (8, 3)


def remote(src, dst, send_sem, recv_sem, device):
    return pltpu.make_async_remote_copy(
        src_ref=src, dst_ref=dst, send_sem=send_sem, recv_sem=recv_sem, device_id=device, device_id_type=MESH
    )


def places():
    xi = lax.axis_index("x")
    yi = lax.axis_index("yz")
    sib = xi + 1 - 2 * (xi % 2)
    xn = (xi + 2) % 4
    return xi, yi, sib, xn, (sib + 2) % 4, 1 - yi


def activation(total):
    gate = total[:, :C].astype(BF16).astype(F32)
    up = total[:, C:].astype(BF16).astype(F32)
    return (jax.nn.silu(gate) * up).astype(BF16)


def front_kernel(
    d_model, x_hbm, g_hbm, wq_hbm, wg_hbm, wu_hbm,
    qkv_hbm, got_hbm, perm_hbm, send_hbm, own_hbm,
    stat, xbuf, gain, gbuf, moments, h, wq, wg, wu, pq, rq, xq, qs, qd, p, r,
    in_sem, wq_sem, wg_sem, wu_sem, st_s, st_r, xg_s, xg_r,
    dq_s, dq_r, xq_s, xq_r, yq_s, yq_r, d_s, d_r, x_s, x_r, out_sem, own_sem, q_sem,
):
    xi, yi, sib, xn, sibn, yn = places()
    me = yi * 4 + xi
    sides, side_rows, width = x_hbm.shape
    rows = sides * side_rows
    n1 = LOW + SHIFT * (xi % 2)
    n2 = n1 + PERM
    near = xi // 2
    far = 1 - near
    num_q = wq_hbm.shape[1] // CQ
    num_c = wg_hbm.shape[1] // C
    sib_dev, xn_dev, yn_dev = {"x": sib}, {"x": xn}, {"yz": yn}

    def wq_copy(c):
        return pltpu.make_async_copy(wq_hbm.at[:, pl.ds(c * CQ, CQ)], wq.at[c], wq_sem.at[c])

    def w_copies(i, slot):
        start = pl.multiple_of(i * C, C)
        return (
            pltpu.make_async_copy(wg_hbm.at[:, pl.ds(start, C)], wg.at[slot], wg_sem.at[slot]),
            pltpu.make_async_copy(wu_hbm.at[:, pl.ds(start, C)], wu.at[slot], wu_sem.at[slot]),
        )

    x_in = pltpu.make_async_copy(x_hbm, xbuf.at[yi], in_sem.at[0])
    g_in = pltpu.make_async_copy(g_hbm, gain, in_sem.at[1])
    x_in.start()
    g_in.start()
    barrier = pltpu.get_barrier_semaphore()
    offsets = [(dy, dx) for dy in range(2) for dx in range(4)][1:]
    for dy, dx in offsets:
        pl.semaphore_signal(barrier, inc=1, device_id={"yz": (yi + dy) % 2, "x": (xi + dx) % 4}, device_id_type=MESH)

    x_in.wait()
    x_f32 = xbuf[yi].reshape(rows, width).astype(F32)
    lane = lax.broadcasted_iota(jnp.int32, (rows, rows), 1)
    sums = jnp.where(
        lane == 0,
        jnp.sum(x_f32, axis=1, keepdims=True),
        jnp.where(lane == 1, jnp.sum(x_f32 * x_f32, axis=1, keepdims=True), 0.0),
    )
    stat[me] = sums.T[0:8, :]
    g_in.wait()
    gbuf[yi] = jnp.broadcast_to(gain[...].astype(F32)[None, :], (8, width))
    pl.semaphore_wait(barrier, 7)

    def stat_copy(k, slot):
        dy, dx = offsets[k]
        dev = {"yz": (yi + dy) % 2, "x": (xi + dx) % 4}
        return remote(stat.at[slot], stat.at[slot], st_s.at[k], st_r.at[k], dev)

    def x_copy(slot, n):
        block = xbuf.at[slot, (far, near)[n]]
        return remote(block, block, xg_s.at[1 + n], xg_r.at[1 + n], yn_dev)

    def g_copy(slot):
        return remote(gbuf.at[slot], gbuf.at[slot], xg_s.at[0], xg_r.at[0], yn_dev)

    for k in range(7):
        stat_copy(k, me).start()
    g_copy(yi).start()
    x_copy(yi, 0).start()
    x_copy(yi, 1).start()
    for c in range(num_q):
        wq_copy(c).start()
    for i in range(SLOTS):
        for copy in w_copies(i, i):
            copy.start()
    for k, (dy, dx) in enumerate(offsets):
        stat_copy(k, ((yi + 2 - dy) % 2) * 4 + (xi + 4 - dx) % 4).wait_recv()
    total = stat[0]
    for k in range(1, 8):
        total = total + stat[k]
    cols = jnp.concatenate([total, jnp.zeros((rows - 8, rows), F32)], axis=0).T
    mean = cols[:, 0:1] / d_model
    var = cols[:, 1:2] / d_model - mean * mean
    moments[0] = jnp.broadcast_to(mean, (rows, 128)).reshape(sides, side_rows, 128)
    moments[1] = jnp.broadcast_to(lax.rsqrt(var + 1e-6), (rows, 128)).reshape(sides, side_rows, 128)
    g_copy(yn).wait_recv()

    def normalize(side):
        for b in range(2):
            part = (xbuf[b, side].astype(F32) - moments[0, side][:, 0:1]) * moments[1, side][:, 0:1]
            h[side, :, b * width:(b + 1) * width] = (part * gbuf[b][0:1, :]).astype(BF16)

    def dq(c, k):
        src = sib if k == 0 else sibn
        return remote(pq.at[c, src], rq.at[c, k], dq_s.at[c, k], dq_r.at[c, k], sib_dev)

    def xq_copy(c):
        return remote(pq.at[c, xn], xq.at[c], xq_s.at[c], xq_r.at[c], xn_dev)

    def q_product(c, side):
        prod = jnp.dot(h[side], wq[c], preferred_element_type=F32)
        pq[c, pl.ds(2 * side, 2)] = prod.reshape(2, rows // 4, CQ)

    def q_send(c):
        dq(c, 1).wait_recv()
        dq(c, 1).wait_send()
        pq[c, xn] = pq[c, xn] + rq[c, 1]
        xq_copy(c).start()

    x_copy(yn, 0).wait_recv()
    normalize(far)

    @pl.loop(0, num_q)
    def _(c):
        wq_copy(c).wait()
        q_product(c, far)
        dq(c, 1).start()

        @pl.when(c >= 1)
        def _():
            q_send(c - 1)

    x_copy(yn, 1).wait_recv()
    normalize(near)
    q_send(num_q - 1)

    @pl.loop(0, num_q)
    def _(c):
        q_product(c, near)
        dq(c, 0).start()

    def d_copy(i, k):
        src = sib if k == 0 else sibn
        return remote(p.at[i, src], r.at[i, k], d_s.at[i, k], d_r.at[i, k], sib_dev)

    def x_send(i):
        return remote(p.at[i, xn], got_hbm.at[i], x_s.at[i], x_r.at[i], xn_dev)

    def perm_copy(i):
        return pltpu.make_async_copy(p.at[i, xn], perm_hbm.at[i - n1], out_sem.at[i])

    def send_copy(i):
        return pltpu.make_async_copy(p.at[i, xn], send_hbm.at[i - n2], out_sem.at[i])

    def own_copy(i):
        return pltpu.make_async_copy(p.at[i, xi], own_hbm.at[i], own_sem.at[i])

    def chip_sum(i):
        d_copy(i, 1).wait_recv()
        d_copy(i, 1).wait_send()
        p[i, xn] = p[i, xn] + r[i, 1]

        @pl.when(i < n1)
        def _():
            x_send(i).start()

        @pl.when((i >= n1) & (i < n2))
        def _():
            perm_copy(i).start()

        @pl.when(i >= n2)
        def _():
            send_copy(i).start()

        d_copy(i, 0).wait_recv()
        d_copy(i, 0).wait_send()
        p[i, xi] = p[i, xi] + r[i, 0]
        own_copy(i).start()

    def product(i):
        slot = i % SLOTS
        g_w, u_w = w_copies(i, slot)
        h_all = h[...].reshape(rows, h.shape[2])
        g_w.wait()
        p[i, :, :, :C] = jnp.dot(h_all, wg[slot], preferred_element_type=F32).reshape(4, rows // 4, C)
        u_w.wait()
        p[i, :, :, C:] = jnp.dot(h_all, wu[slot], preferred_element_type=F32).reshape(4, rows // 4, C)
        d_copy(i, 1).start()
        d_copy(i, 0).start()

        @pl.when(i + SLOTS < num_c)
        def _():
            for copy in w_copies(i + SLOTS, slot):
                copy.start()

    product(0)

    def step(i):
        product(i)
        chip_sum(i - 1)

    half = num_c // 2 + 1
    pl.loop(1, half)(step)

    @pl.loop(0, num_q)
    def _(c):
        dq(c, 0).wait_recv()
        dq(c, 0).wait_send()
        mine = pq[c, xi] + rq[c, 0]
        xq_copy(c).wait_recv()
        xq_copy(c).wait_send()
        value = (mine + xq[c]).astype(BF16)
        qs[:, :, pl.ds(pl.multiple_of(c * CQ, CQ), CQ)] = value.reshape(2, rows // 8, CQ)

    def yq_copy(k):
        return remote(qs.at[1 - k], qd.at[k], yq_s, yq_r, yn_dev)

    yq_copy(yi).start()
    qd[yi] = qs[yi]

    pl.loop(half, num_c)(step)
    chip_sum(num_c - 1)
    yq_copy(yn).wait_recv()
    q_out = pltpu.make_async_copy(qd, qkv_hbm, q_sem)
    q_out.start()

    for k in range(7):
        stat_copy(k, me).wait_send()
    g_copy(yi).wait_send()
    x_copy(yi, 0).wait_send()
    x_copy(yi, 1).wait_send()
    yq_copy(yi).wait_send()

    @pl.loop(0, num_c)
    def _(i):
        own_copy(i).wait()

    @pl.loop(n1, n2)
    def _(i):
        perm_copy(i).wait()

    @pl.loop(n2, num_c)
    def _(i):
        send_copy(i).wait()

    q_out.wait()

    @pl.loop(0, n1)
    def _(i):
        x_send(i).wait()


def front(x_loc, gain_loc, wqkv, wgate, wup, d_model):
    rows, width = x_loc.shape
    depth, q_cols = wqkv.shape
    num_q, num_c = q_cols // CQ, wgate.shape[1] // C
    quarter = rows // 4
    dma = pltpu.SemaphoreType.DMA
    any_spec = pl.BlockSpec(memory_space=pl.ANY)
    return pl.pallas_call(
        functools.partial(front_kernel, d_model),
        name="front",
        out_shape=(
            jax.ShapeDtypeStruct((2, rows // 8, q_cols), BF16),
            jax.ShapeDtypeStruct((LOW + SHIFT, quarter, 2 * C), F32),
            jax.ShapeDtypeStruct((PERM, quarter, 2 * C), F32),
            jax.ShapeDtypeStruct((num_c - LOW - PERM, quarter, 2 * C), F32),
            jax.ShapeDtypeStruct((num_c, quarter, 2 * C), F32),
        ),
        in_specs=[any_spec] * 5,
        out_specs=(any_spec,) * 5,
        scratch_shapes=[
            pltpu.VMEM((8, 8, rows), F32),
            pltpu.VMEM((2, 2, rows // 2, width), BF16),
            pltpu.VMEM((width,), BF16),
            pltpu.VMEM((2, 8, width), F32),
            pltpu.VMEM((2, 2, rows // 2, 128), F32),
            pltpu.VMEM((2, rows // 2, depth), BF16),
            pltpu.VMEM((num_q, depth, CQ), BF16),
            pltpu.VMEM((SLOTS, depth, C), BF16),
            pltpu.VMEM((SLOTS, depth, C), BF16),
            pltpu.VMEM((num_q, 4, quarter, CQ), F32),
            pltpu.VMEM((num_q, 2, quarter, CQ), F32),
            pltpu.VMEM((num_q, quarter, CQ), F32),
            pltpu.VMEM((2, rows // 8, q_cols), BF16),
            pltpu.VMEM((2, rows // 8, q_cols), BF16),
            pltpu.VMEM((num_c, 4, quarter, 2 * C), F32),
            pltpu.VMEM((num_c, 2, quarter, 2 * C), F32),
            dma((2,)), dma((num_q,)), dma((SLOTS,)), dma((SLOTS,)), dma((7,)), dma((7,)), dma((3,)), dma((3,)),
            dma((num_q, 2)), dma((num_q, 2)), dma((num_q,)), dma((num_q,)), dma, dma,
            dma((num_c, 2)), dma((num_c, 2)), dma((LOW + SHIFT,)), dma((LOW + SHIFT,)), dma((num_c,)), dma((num_c,)), dma,
        ],
        compiler_params=pltpu.CompilerParams(collective_id=0, has_side_effects=True, vmem_limit_bytes=VMEM_LIMIT),
        cost_estimate=pl.CostEstimate(
            flops=2 * rows * depth * (q_cols + 2 * wgate.shape[1]),
            bytes_accessed=2 * depth * (q_cols + 2 * wgate.shape[1]),
            transcendentals=0,
        ),
    )(x_loc.reshape(2, rows // 2, width), gain_loc, wqkv, wgate, wup)


def attend_kernel(len_ref, qkv_ref, cos_ref, sin_ref, k_ref, v_ref, ko_ref, vo_ref, o_ref):
    ko_ref[...] = k_ref[...]
    vo_ref[...] = v_ref[...]
    for n in range(PER_STEP):
        pos = len_ref[pl.program_id(0) * PER_STEP + n]
        qkv = qkv_ref[n]
        heads, head_dim = qkv.shape[0] - 2, qkv.shape[1]
        wide = qkv.astype(F32)
        turned = (wide * cos_ref[n] + pltpu.roll(wide, head_dim // 2, 1) * sin_ref[n]).astype(BF16)
        query = turned[:heads]
        base = pl.multiple_of((pos // 16) * 16, 16)
        here = lax.broadcasted_iota(jnp.int32, (16, head_dim), 0) == pos - base
        for out, new in ((ko_ref, turned[heads:heads + 1]), (vo_ref, qkv[heads + 1:heads + 2])):
            tile = out[n, pl.ds(base, 16), :].astype(F32)
            out[n, pl.ds(base, 16), :] = jnp.where(here, new.astype(F32), tile).astype(BF16)
        scores = lax.dot_general(query, ko_ref[n], (((1,), (1,)), ((), ())), preferred_element_type=F32)
        scores = scores * head_dim ** -0.5
        at = lax.broadcasted_iota(jnp.int32, scores.shape, 1)
        scores = jnp.where(at <= pos, scores, -1e30)
        weight = jnp.exp(scores - jnp.max(scores, axis=1, keepdims=True))
        probs = (weight / jnp.sum(weight, axis=1, keepdims=True)).astype(BF16)
        o_ref[n] = jnp.dot(probs, vo_ref[n], preferred_element_type=F32).astype(BF16)


def attend(qkv, cos, sin, k_cache, v_cache, ctx_len):
    reqs, length, head_dim = k_cache.shape
    heads = qkv.shape[1] - 2
    cache_spec = pl.BlockSpec((PER_STEP, length, head_dim), lambda i, lens: (i, 0, 0))
    table_spec = pl.BlockSpec((PER_STEP, 1, head_dim), lambda i, lens: (i, 0, 0))
    return pl.pallas_call(
        attend_kernel,
        name="attend",
        grid_spec=pltpu.PrefetchScalarGridSpec(
            num_scalar_prefetch=1,
            grid=(reqs // PER_STEP,),
            in_specs=[
                pl.BlockSpec((PER_STEP, heads + 2, head_dim), lambda i, lens: (i, 0, 0)),
                table_spec, table_spec, cache_spec, cache_spec,
            ],
            out_specs=[cache_spec, cache_spec, pl.BlockSpec((PER_STEP, heads, head_dim), lambda i, lens: (i, 0, 0))],
        ),
        out_shape=(
            jax.ShapeDtypeStruct(k_cache.shape, BF16),
            jax.ShapeDtypeStruct(v_cache.shape, BF16),
            jax.ShapeDtypeStruct((reqs, heads, head_dim), BF16),
        ),
        compiler_params=pltpu.CompilerParams(dimension_semantics=("arbitrary",)),
        cost_estimate=pl.CostEstimate(
            flops=64 * reqs * heads * length * head_dim,
            bytes_accessed=8 * reqs * length * head_dim,
            transcendentals=reqs * heads * length,
        ),
    )(ctx_len, qkv, cos, sin, k_cache, v_cache)


def back_kernel(
    o_hbm, own_hbm, got_hbm, perm_hbm, send_hbm, wao_hbm, wmo_hbm, z_out,
    w, own, xr, act, z, zr,
    in_sem, out_sem, w_sem, own_sem, x_s, x_r, o_s, o_r, sib_s, sib_r, xn_s, xn_r, fwd_s, fwd_r, z_s, z_r,
):
    xi, yi, sib, xn, _, yn = places()
    sib_dev, xn_dev, yn_dev = {"x": sib}, {"x": xn}, {"yz": yn}
    width = z_out.shape[3]
    half_rows = act.shape[1] * act.shape[2]
    num_o, num_c = wao_hbm.shape[0] // C, wmo_hbm.shape[0] // C
    num_k = num_o + num_c
    o_cols = wao_hbm.shape[0]
    n1 = LOW + SHIFT * (xi % 2)
    n2 = n1 + PERM
    pieces = len(PIECES)
    starts = [FULL + sum(PIECES[:n]) for n in range(pieces + 1)]

    def w_copy(k):
        src = wao_hbm.at[pl.ds(k * C, C), :] if k < num_o else wmo_hbm.at[pl.ds((k - num_o) * C, C), :]
        return pltpu.make_async_copy(src, w.at[k], w_sem.at[k])

    def own_copy(i):
        return pltpu.make_async_copy(own_hbm.at[i], own.at[i], own_sem.at[i])

    def here_copy(src, i):
        return pltpu.make_async_copy(src, xr.at[i], x_r.at[i])

    def x_send(i):
        return remote(send_hbm.at[i - n2], xr.at[i], x_s.at[i - n2], x_r.at[i], xn_dev)

    barrier = pltpu.get_barrier_semaphore()
    for dev in (sib_dev, xn_dev, yn_dev):
        pl.semaphore_signal(barrier, inc=1, device_id=dev, device_id_type=MESH)
    o_in = pltpu.make_async_copy(o_hbm.at[yi], act.at[yi, xi, :, 0:o_cols], in_sem)
    o_in.start()

    @pl.loop(0, n1)
    def _(i):
        here_copy(got_hbm.at[i], i).start()

    @pl.loop(n1, n2)
    def _(i):
        here_copy(perm_hbm.at[i - n1], i).start()

    pl.semaphore_wait(barrier, 3)

    def o_copy(half, row):
        return remote(o_hbm.at[half], act.at[row, xi, :, 0:o_cols], o_s, o_r, yn_dev)

    def block_of(e, owner):
        if e == 0:
            return act.at[:, owner, :, pl.ds(o_cols, FULL * C)]
        if e == 1:
            return act.at[:, owner, :, pl.ds(0, o_cols)]
        half, n = divmod(e - 2, pieces)
        return act.at[half, owner, :, pl.ds(o_cols + starts[n] * C, PIECES[n] * C)]

    def to_sib(e, owner):
        block = block_of(e, owner)
        return remote(block, block, sib_s.at[e], sib_r.at[e], sib_dev)

    def to_xn(e, owner):
        block = block_of(e, owner)
        return remote(block, block, xn_s.at[e], xn_r.at[e], xn_dev)

    def forward(e, owner):
        block = block_of(e, owner)
        return remote(block, block, fwd_s.at[e], fwd_r.at[e], sib_dev)

    def send_own(e):
        to_xn(e, xi).start()
        to_sib(e, xi).start()

    def pass_on(e):
        to_xn(e, xn).wait_recv()
        forward(e, xn).start()

    def arrived(e):
        to_sib(e, sib).wait_recv()
        forward(e, (sib + 2) % 4).wait_recv()

    def activate(i):
        own_copy(i).wait()
        value = activation(own[i] + xr[i])
        start = o_cols + i * C if isinstance(i, int) else pl.multiple_of(o_cols + i * C, C)
        act[:, xi, :, pl.ds(start, C)] = value.reshape(2, value.shape[0] // 2, C)

    def w_wait(k):
        pltpu.make_async_copy(wmo_hbm.at[pl.ds(0, C), :], w.at[k], w_sem.at[k]).wait()

    def multiply(first, count):
        @pl.loop(first, first + count)
        def _(k):
            w_wait(k)
            lhs = act[:, :, :, pl.ds(pl.multiple_of(k * C, C), C)].reshape(2 * half_rows, C)
            for b in range(2):
                prod = jnp.dot(lhs, w[k, :, b * width:(b + 1) * width], preferred_element_type=F32)
                z[b] = z[b] + prod.reshape(z.shape[1:])

    def multiply_one(half, n, b):
        @pl.loop(num_o + starts[n], num_o + starts[n + 1])
        def _(k):
            lhs = act[half, :, :, pl.ds(pl.multiple_of(k * C, C), C)].reshape(half_rows, C)
            cols = pl.ds(pl.multiple_of(b * width, width), width)
            prod = jnp.dot(lhs, w[k, :, cols], preferred_element_type=F32)
            z[b, half] = z[b, half] + prod.reshape(z.shape[2:])

    def multiply_half(half, n):
        @pl.loop(num_o + starts[n], num_o + starts[n + 1])
        def _(k):
            if half == 0:
                w_wait(k)
            lhs = act[half, :, :, pl.ds(pl.multiple_of(k * C, C), C)].reshape(half_rows, C)
            for b in range(2):
                prod = jnp.dot(lhs, w[k, :, b * width:(b + 1) * width], preferred_element_type=F32)
                z[b, half] = z[b, half] + prod.reshape(z.shape[2:])

    middle = num_c - 1

    @pl.loop(n2, middle)
    def _(i):
        x_send(i).start()

    o_copy(yn, yi).start()

    @pl.loop(0, num_c)
    def _(i):
        own_copy(i).start()

    for k in range(num_o):
        w_copy(k).start()
    z[...] = jnp.zeros_like(z)

    def start_here(i):
        here_copy(got_hbm.at[0], i).wait()
        activate(i)

    pl.loop(0, FULL)(start_here)
    o_in.wait()
    o_copy(yi, yn).wait_recv()
    send_own(1)
    x_send(middle).start()
    send_own(0)
    for k in range(num_o, num_k):
        w_copy(k).start()
    pl.loop(FULL, n2)(start_here)
    ready = sum(end <= LOW + PERM for end in starts[1:])
    for n in range(ready):
        send_own(2 + n)

    @pl.loop(n2, middle)
    def _(i):
        x_send(i).wait_recv()
        activate(i)

    pass_on(1)
    arrived(1)
    multiply(0, num_o)
    x_send(middle).wait_recv()
    activate(middle)
    groups = 2 + 2 * pieces
    for e in range(2 + ready, groups):
        send_own(e)
    pass_on(0)
    arrived(0)
    multiply(num_o, FULL)
    z_copies = [remote(z.at[yn, half], zr.at[half], z_s.at[half], z_r.at[half], yn_dev) for half in range(2)]
    pass_on(2)
    for e in range(2, groups):
        if e + 1 < groups:
            pass_on(e + 1)
        arrived(e)
        half, n = divmod(e - 2, pieces)
        if e + 1 < groups:
            multiply_half(half, n)
        else:
            multiply_one(half, n, yn)
        if n == pieces - 1:
            z_copies[half].start()
    multiply_one(1, pieces - 1, yi)

    o_copy(yn, yi).wait_send()
    for e in range(groups):
        to_xn(e, xi).wait_send()
        to_sib(e, xi).wait_send()
        forward(e, xn).wait_send()

    @pl.loop(n2, num_c)
    def _(i):
        x_send(i).wait_send()

    outs = [pltpu.make_async_copy(zr.at[half], z_out.at[:, half], out_sem.at[half]) for half in range(2)]
    for half in range(2):
        z_copies[half].wait()
        zr[half] = z[yi, half] + zr[half]
        outs[half].start()
    for half in range(2):
        outs[half].wait()


def back(x_loc, o_halves, own, got, perm, send, wao, wmo):
    rows, width = x_loc.shape
    num_o, num_c = wao.shape[0] // C, wmo.shape[0] // C
    num_k = num_o + num_c
    groups = 2 + 2 * len(PIECES)
    quarter = rows // 4
    dma = pltpu.SemaphoreType.DMA
    any_spec = pl.BlockSpec(memory_space=pl.ANY)
    z = pl.pallas_call(
        back_kernel,
        name="back",
        out_shape=jax.ShapeDtypeStruct((4, 2, rows // 8, width), F32),
        in_specs=[any_spec] * 7,
        out_specs=any_spec,
        scratch_shapes=[
            pltpu.VMEM((num_k, C, 2 * width), BF16),
            pltpu.VMEM((num_c, quarter, 2 * C), F32),
            pltpu.VMEM((num_c, quarter, 2 * C), F32),
            pltpu.VMEM((2, 4, rows // 8, num_k * C), BF16),
            pltpu.VMEM((2, 2, 4, rows // 8, width), F32),
            pltpu.VMEM((2, 4, rows // 8, width), F32),
            dma, dma((2,)), dma((num_k,)), dma((num_c,)), dma((num_c - LOW - PERM,)), dma((num_c,)), dma, dma,
            dma((groups,)), dma((groups,)), dma((groups,)), dma((groups,)), dma((groups,)), dma((groups,)),
            dma((2,)), dma((2,)),
        ],
        compiler_params=pltpu.CompilerParams(collective_id=1, has_side_effects=True, vmem_limit_bytes=VMEM_LIMIT),
        cost_estimate=pl.CostEstimate(
            flops=4 * rows * num_k * C * width, bytes_accessed=4 * num_k * C * width, transcendentals=0
        ),
    )(o_halves, own, got, perm, send, wao, wmo)
    return (x_loc.astype(F32) + z.reshape(rows, width)).astype(BF16)


def solution(mesh):
    x_size, yz_size = mesh.shape["x"], mesh.shape["yz"]
    both_axes = ("x", "yz")
    row_spec = P("dp", both_axes)
    in_w_spec = P("x", "yz")
    out_w_spec = P("yz", "x")
    cache_spec = P(("dp", "x", "yz"), None, None)
    len_spec = P(("dp", "x", "yz"))
    across = [(i, (i + 2) % 4) for i in range(4)]

    def local_layer(x_loc, gain_loc, wqkv_loc, wgate_loc, wup_loc, wao_loc, wmo_loc, kc_loc, vc_loc, len_loc):
        d_model = x_loc.shape[1] * x_size * yz_size
        reqs, _, head_dim = kc_loc.shape
        half = head_dim // 2
        inv_freq = 10000.0 ** (-jnp.arange(half, dtype=F32) / half)
        angles = len_loc.astype(F32)[:, None] * inv_freq
        cos, sin = jnp.cos(angles), jnp.sin(angles)
        cos = jnp.concatenate([cos, cos], axis=1)[:, None, :]
        sin = jnp.concatenate([-sin, sin], axis=1)[:, None, :]

        qkv, got, perm, send, own = front(
            x_loc, gain_loc, wqkv_loc, wgate_loc, wup_loc, d_model
        )
        perm = lax.ppermute(perm, "x", across)
        qkv = jnp.concatenate([qkv[0], qkv[1]], axis=1).reshape(reqs, -1, head_dim)
        k_all, v_all, attn = attend(qkv, cos, sin, kc_loc, vc_loc, len_loc)
        o_halves = jnp.swapaxes(attn.reshape(reqs, 2, -1), 0, 1)
        y_loc = back(x_loc, o_halves, own, got, perm, send, wao_loc, wmo_loc)
        return y_loc, k_all, v_all

    in_specs = (row_spec, P(both_axes), in_w_spec, in_w_spec, in_w_spec, out_w_spec, out_w_spec, cache_spec, cache_spec, len_spec)
    out_specs = (row_spec, cache_spec, cache_spec)
    return jax.shard_map(local_layer, mesh=mesh, in_specs=in_specs, out_specs=out_specs, check_vma=False)
```

```python
import functools

import jax
import jax.numpy as jnp
from jax import lax
from jax.experimental import pallas as pl
from jax.experimental.pallas import tpu as pltpu
from jax.sharding import PartitionSpec as P

MESH = pl.DeviceIdType.MESH
F32 = jnp.float32
BF16 = jnp.bfloat16
VMEM_LIMIT = 66_900_000

C = 768
CQ = 640
PER_STEP = 2
SLOTS = 3
LOW, SHIFT, PERM = 5, 0, 8
FULL = 5
PIECES = (8, 3)


def remote(src, dst, send_sem, recv_sem, device):
    return pltpu.make_async_remote_copy(
        src_ref=src, dst_ref=dst, send_sem=send_sem, recv_sem=recv_sem, device_id=device, device_id_type=MESH
    )


def places():
    xi = lax.axis_index("x")
    yi = lax.axis_index("yz")
    sib = xi + 1 - 2 * (xi % 2)
    xn = (xi + 2) % 4
    return xi, yi, sib, xn, (sib + 2) % 4, 1 - yi


def activation(total):
    gate = total[:, :C].astype(BF16).astype(F32)
    up = total[:, C:].astype(BF16).astype(F32)
    return (jax.nn.silu(gate) * up).astype(BF16)


def front_kernel(
    d_model, x_hbm, g_hbm, wq_hbm, wg_hbm, wu_hbm,
    qkv_hbm, got_hbm, perm_hbm, send_hbm, own_hbm,
    stat, xbuf, gain, gbuf, moments, h, wq, wg, wu, pq, rq, xq, qs, qd, p, r,
    in_sem, wq_sem, wg_sem, wu_sem, st_s, st_r, xg_s, xg_r,
    dq_s, dq_r, xq_s, xq_r, yq_s, yq_r, d_s, d_r, x_s, x_r, out_sem, own_sem, q_sem,
):
    xi, yi, sib, xn, sibn, yn = places()
    me = yi * 4 + xi
    sides, side_rows, width = x_hbm.shape
    rows = sides * side_rows
    n1 = LOW + SHIFT * (xi % 2)
    n2 = n1 + PERM
    near = xi // 2
    far = 1 - near
    num_q = wq_hbm.shape[1] // CQ
    num_c = wg_hbm.shape[1] // C
    sib_dev, xn_dev, yn_dev = {"x": sib}, {"x": xn}, {"yz": yn}

    def wq_copy(c):
        return pltpu.make_async_copy(wq_hbm.at[:, pl.ds(c * CQ, CQ)], wq.at[c], wq_sem.at[c])

    def w_copies(i, slot):
        start = pl.multiple_of(i * C, C)
        return (
            pltpu.make_async_copy(wg_hbm.at[:, pl.ds(start, C)], wg.at[slot], wg_sem.at[slot]),
            pltpu.make_async_copy(wu_hbm.at[:, pl.ds(start, C)], wu.at[slot], wu_sem.at[slot]),
        )

    x_in = pltpu.make_async_copy(x_hbm, xbuf.at[yi], in_sem.at[0])
    g_in = pltpu.make_async_copy(g_hbm, gain, in_sem.at[1])
    x_in.start()
    g_in.start()
    barrier = pltpu.get_barrier_semaphore()
    offsets = [(dy, dx) for dy in range(2) for dx in range(4)][1:]
    for dy, dx in offsets:
        pl.semaphore_signal(barrier, inc=1, device_id={"yz": (yi + dy) % 2, "x": (xi + dx) % 4}, device_id_type=MESH)

    x_in.wait()
    x_f32 = xbuf[yi].reshape(rows, width).astype(F32)
    lane = lax.broadcasted_iota(jnp.int32, (rows, rows), 1)
    sums = jnp.where(
        lane == 0,
        jnp.sum(x_f32, axis=1, keepdims=True),
        jnp.where(lane == 1, jnp.sum(x_f32 * x_f32, axis=1, keepdims=True), 0.0),
    )
    stat[me] = sums.T[0:8, :]
    g_in.wait()
    gbuf[yi] = jnp.broadcast_to(gain[...].astype(F32)[None, :], (8, width))
    pl.semaphore_wait(barrier, 7)

    def stat_copy(k, slot):
        dy, dx = offsets[k]
        dev = {"yz": (yi + dy) % 2, "x": (xi + dx) % 4}
        return remote(stat.at[slot], stat.at[slot], st_s.at[k], st_r.at[k], dev)

    def x_copy(slot, n):
        block = xbuf.at[slot, (far, near)[n]]
        return remote(block, block, xg_s.at[1 + n], xg_r.at[1 + n], yn_dev)

    def g_copy(slot):
        return remote(gbuf.at[slot], gbuf.at[slot], xg_s.at[0], xg_r.at[0], yn_dev)

    for k in range(7):
        stat_copy(k, me).start()
    g_copy(yi).start()
    x_copy(yi, 0).start()
    x_copy(yi, 1).start()
    for c in range(num_q):
        wq_copy(c).start()
    for i in range(SLOTS):
        for copy in w_copies(i, i):
            copy.start()
    for k, (dy, dx) in enumerate(offsets):
        stat_copy(k, ((yi + 2 - dy) % 2) * 4 + (xi + 4 - dx) % 4).wait_recv()
    total = stat[0]
    for k in range(1, 8):
        total = total + stat[k]
    cols = jnp.concatenate([total, jnp.zeros((rows - 8, rows), F32)], axis=0).T
    mean = cols[:, 0:1] / d_model
    var = cols[:, 1:2] / d_model - mean * mean
    moments[0] = jnp.broadcast_to(mean, (rows, 128)).reshape(sides, side_rows, 128)
    moments[1] = jnp.broadcast_to(lax.rsqrt(var + 1e-6), (rows, 128)).reshape(sides, side_rows, 128)
    g_copy(yn).wait_recv()

    def normalize(side):
        for b in range(2):
            part = (xbuf[b, side].astype(F32) - moments[0, side][:, 0:1]) * moments[1, side][:, 0:1]
            h[side, :, b * width:(b + 1) * width] = (part * gbuf[b][0:1, :]).astype(BF16)

    def dq(c, k):
        src = sib if k == 0 else sibn
        return remote(pq.at[c, src], rq.at[c, k], dq_s.at[c, k], dq_r.at[c, k], sib_dev)

    def xq_copy(c):
        return remote(pq.at[c, xn], xq.at[c], xq_s.at[c], xq_r.at[c], xn_dev)

    def q_product(c, side):
        prod = jnp.dot(h[side], wq[c], preferred_element_type=F32)
        pq[c, pl.ds(2 * side, 2)] = prod.reshape(2, rows // 4, CQ)

    def q_send(c):
        dq(c, 1).wait_recv()
        dq(c, 1).wait_send()
        pq[c, xn] = pq[c, xn] + rq[c, 1]
        xq_copy(c).start()

    x_copy(yn, 0).wait_recv()
    normalize(far)

    @pl.loop(0, num_q)
    def _(c):
        wq_copy(c).wait()
        q_product(c, far)
        dq(c, 1).start()

        @pl.when(c >= 1)
        def _():
            q_send(c - 1)

    x_copy(yn, 1).wait_recv()
    normalize(near)
    q_send(num_q - 1)

    @pl.loop(0, num_q)
    def _(c):
        q_product(c, near)
        dq(c, 0).start()

    def d_copy(i, k):
        src = sib if k == 0 else sibn
        return remote(p.at[i, src], r.at[i, k], d_s.at[i, k], d_r.at[i, k], sib_dev)

    def x_send(i):
        return remote(p.at[i, xn], got_hbm.at[i], x_s.at[i], x_r.at[i], xn_dev)

    def perm_copy(i):
        return pltpu.make_async_copy(p.at[i, xn], perm_hbm.at[i - n1], out_sem.at[i])

    def send_copy(i):
        return pltpu.make_async_copy(p.at[i, xn], send_hbm.at[i - n2], out_sem.at[i])

    def own_copy(i):
        return pltpu.make_async_copy(p.at[i, xi], own_hbm.at[i], own_sem.at[i])

    def chip_sum(i):
        d_copy(i, 1).wait_recv()
        d_copy(i, 1).wait_send()
        p[i, xn] = p[i, xn] + r[i, 1]

        @pl.when(i < n1)
        def _():
            x_send(i).start()

        @pl.when((i >= n1) & (i < n2))
        def _():
            perm_copy(i).start()

        @pl.when(i >= n2)
        def _():
            send_copy(i).start()

        d_copy(i, 0).wait_recv()
        d_copy(i, 0).wait_send()
        p[i, xi] = p[i, xi] + r[i, 0]
        own_copy(i).start()

    def product(i):
        slot = i % SLOTS
        g_w, u_w = w_copies(i, slot)
        h_all = h[...].reshape(rows, h.shape[2])
        g_w.wait()
        p[i, :, :, :C] = jnp.dot(h_all, wg[slot], preferred_element_type=F32).reshape(4, rows // 4, C)
        u_w.wait()
        p[i, :, :, C:] = jnp.dot(h_all, wu[slot], preferred_element_type=F32).reshape(4, rows // 4, C)
        d_copy(i, 1).start()
        d_copy(i, 0).start()

        @pl.when(i + SLOTS < num_c)
        def _():
            for copy in w_copies(i + SLOTS, slot):
                copy.start()

    product(0)

    def step(i):
        product(i)
        chip_sum(i - 1)

    half = num_c // 2 + 1
    pl.loop(1, half)(step)

    @pl.loop(0, num_q)
    def _(c):
        dq(c, 0).wait_recv()
        dq(c, 0).wait_send()
        mine = pq[c, xi] + rq[c, 0]
        xq_copy(c).wait_recv()
        xq_copy(c).wait_send()
        value = (mine + xq[c]).astype(BF16)
        qs[:, :, pl.ds(pl.multiple_of(c * CQ, CQ), CQ)] = value.reshape(2, rows // 8, CQ)

    def yq_copy(k):
        return remote(qs.at[1 - k], qd.at[k], yq_s, yq_r, yn_dev)

    yq_copy(yi).start()
    qd[yi] = qs[yi]

    pl.loop(half, num_c)(step)
    chip_sum(num_c - 1)
    yq_copy(yn).wait_recv()
    q_out = pltpu.make_async_copy(qd, qkv_hbm, q_sem)
    q_out.start()

    for k in range(7):
        stat_copy(k, me).wait_send()
    g_copy(yi).wait_send()
    x_copy(yi, 0).wait_send()
    x_copy(yi, 1).wait_send()
    yq_copy(yi).wait_send()

    @pl.loop(0, num_c)
    def _(i):
        own_copy(i).wait()

    @pl.loop(n1, n2)
    def _(i):
        perm_copy(i).wait()

    @pl.loop(n2, num_c)
    def _(i):
        send_copy(i).wait()

    q_out.wait()

    @pl.loop(0, n1)
    def _(i):
        x_send(i).wait()


def front(x_loc, gain_loc, wqkv, wgate, wup, d_model):
    rows, width = x_loc.shape
    depth, q_cols = wqkv.shape
    num_q, num_c = q_cols // CQ, wgate.shape[1] // C
    quarter = rows // 4
    dma = pltpu.SemaphoreType.DMA
    any_spec = pl.BlockSpec(memory_space=pl.ANY)
    return pl.pallas_call(
        functools.partial(front_kernel, d_model),
        name="front",
        out_shape=(
            jax.ShapeDtypeStruct((2, rows // 8, q_cols), BF16),
            jax.ShapeDtypeStruct((LOW + SHIFT, quarter, 2 * C), F32),
            jax.ShapeDtypeStruct((PERM, quarter, 2 * C), F32),
            jax.ShapeDtypeStruct((num_c - LOW - PERM, quarter, 2 * C), F32),
            jax.ShapeDtypeStruct((num_c, quarter, 2 * C), F32),
        ),
        in_specs=[any_spec] * 5,
        out_specs=(any_spec,) * 5,
        scratch_shapes=[
            pltpu.VMEM((8, 8, rows), F32),
            pltpu.VMEM((2, 2, rows // 2, width), BF16),
            pltpu.VMEM((width,), BF16),
            pltpu.VMEM((2, 8, width), F32),
            pltpu.VMEM((2, 2, rows // 2, 128), F32),
            pltpu.VMEM((2, rows // 2, depth), BF16),
            pltpu.VMEM((num_q, depth, CQ), BF16),
            pltpu.VMEM((SLOTS, depth, C), BF16),
            pltpu.VMEM((SLOTS, depth, C), BF16),
            pltpu.VMEM((num_q, 4, quarter, CQ), F32),
            pltpu.VMEM((num_q, 2, quarter, CQ), F32),
            pltpu.VMEM((num_q, quarter, CQ), F32),
            pltpu.VMEM((2, rows // 8, q_cols), BF16),
            pltpu.VMEM((2, rows // 8, q_cols), BF16),
            pltpu.VMEM((num_c, 4, quarter, 2 * C), F32),
            pltpu.VMEM((num_c, 2, quarter, 2 * C), F32),
            dma((2,)), dma((num_q,)), dma((SLOTS,)), dma((SLOTS,)), dma((7,)), dma((7,)), dma((3,)), dma((3,)),
            dma((num_q, 2)), dma((num_q, 2)), dma((num_q,)), dma((num_q,)), dma, dma,
            dma((num_c, 2)), dma((num_c, 2)), dma((LOW + SHIFT,)), dma((LOW + SHIFT,)), dma((num_c,)), dma((num_c,)), dma,
        ],
        compiler_params=pltpu.CompilerParams(collective_id=0, has_side_effects=True, vmem_limit_bytes=VMEM_LIMIT),
        cost_estimate=pl.CostEstimate(
            flops=2 * rows * depth * (q_cols + 2 * wgate.shape[1]),
            bytes_accessed=2 * depth * (q_cols + 2 * wgate.shape[1]),
            transcendentals=0,
        ),
    )(x_loc.reshape(2, rows // 2, width), gain_loc, wqkv, wgate, wup)


def attend_kernel(len_ref, qkv_ref, cos_ref, sin_ref, k_ref, v_ref, ko_ref, vo_ref, o_ref):
    ko_ref[...] = k_ref[...]
    vo_ref[...] = v_ref[...]
    for n in range(PER_STEP):
        pos = len_ref[pl.program_id(0) * PER_STEP + n]
        qkv = qkv_ref[n]
        heads, head_dim = qkv.shape[0] - 2, qkv.shape[1]
        wide = qkv.astype(F32)
        turned = (wide * cos_ref[n] + pltpu.roll(wide, head_dim // 2, 1) * sin_ref[n]).astype(BF16)
        query = turned[:heads]
        base = pl.multiple_of((pos // 16) * 16, 16)
        here = lax.broadcasted_iota(jnp.int32, (16, head_dim), 0) == pos - base
        for out, new in ((ko_ref, turned[heads:heads + 1]), (vo_ref, qkv[heads + 1:heads + 2])):
            tile = out[n, pl.ds(base, 16), :].astype(F32)
            out[n, pl.ds(base, 16), :] = jnp.where(here, new.astype(F32), tile).astype(BF16)
        scores = lax.dot_general(query, ko_ref[n], (((1,), (1,)), ((), ())), preferred_element_type=F32)
        scores = scores * head_dim ** -0.5
        at = lax.broadcasted_iota(jnp.int32, scores.shape, 1)
        scores = jnp.where(at <= pos, scores, -1e30)
        weight = jnp.exp(scores - jnp.max(scores, axis=1, keepdims=True))
        probs = (weight / jnp.sum(weight, axis=1, keepdims=True)).astype(BF16)
        o_ref[n] = jnp.dot(probs, vo_ref[n], preferred_element_type=F32).astype(BF16)


def attend(qkv, cos, sin, k_cache, v_cache, ctx_len):
    reqs, length, head_dim = k_cache.shape
    heads = qkv.shape[1] - 2
    cache_spec = pl.BlockSpec((PER_STEP, length, head_dim), lambda i, lens: (i, 0, 0))
    table_spec = pl.BlockSpec((PER_STEP, 1, head_dim), lambda i, lens: (i, 0, 0))
    return pl.pallas_call(
        attend_kernel,
        name="attend",
        grid_spec=pltpu.PrefetchScalarGridSpec(
            num_scalar_prefetch=1,
            grid=(reqs // PER_STEP,),
            in_specs=[
                pl.BlockSpec((PER_STEP, heads + 2, head_dim), lambda i, lens: (i, 0, 0)),
                table_spec, table_spec, cache_spec, cache_spec,
            ],
            out_specs=[cache_spec, cache_spec, pl.BlockSpec((PER_STEP, heads, head_dim), lambda i, lens: (i, 0, 0))],
        ),
        out_shape=(
            jax.ShapeDtypeStruct(k_cache.shape, BF16),
            jax.ShapeDtypeStruct(v_cache.shape, BF16),
            jax.ShapeDtypeStruct((reqs, heads, head_dim), BF16),
        ),
        compiler_params=pltpu.CompilerParams(dimension_semantics=("arbitrary",)),
        cost_estimate=pl.CostEstimate(
            flops=64 * reqs * heads * length * head_dim,
            bytes_accessed=8 * reqs * length * head_dim,
            transcendentals=reqs * heads * length,
        ),
    )(ctx_len, qkv, cos, sin, k_cache, v_cache)


def back_kernel(
    o_hbm, own_hbm, got_hbm, perm_hbm, send_hbm, wao_hbm, wmo_hbm, z_out,
    w, own, xr, act, z, zr,
    in_sem, out_sem, w_sem, own_sem, x_s, x_r, o_s, o_r, sib_s, sib_r, xn_s, xn_r, fwd_s, fwd_r, z_s, z_r,
):
    xi, yi, sib, xn, _, yn = places()
    sib_dev, xn_dev, yn_dev = {"x": sib}, {"x": xn}, {"yz": yn}
    width = z_out.shape[3]
    half_rows = act.shape[1] * act.shape[2]
    num_o, num_c = wao_hbm.shape[0] // C, wmo_hbm.shape[0] // C
    num_k = num_o + num_c
    o_cols = wao_hbm.shape[0]
    n1 = LOW + SHIFT * (xi % 2)
    n2 = n1 + PERM
    pieces = len(PIECES)
    starts = [FULL + sum(PIECES[:n]) for n in range(pieces + 1)]

    def w_copy(k):
        src = wao_hbm.at[pl.ds(k * C, C), :] if k < num_o else wmo_hbm.at[pl.ds((k - num_o) * C, C), :]
        return pltpu.make_async_copy(src, w.at[k], w_sem.at[k])

    def own_copy(i):
        return pltpu.make_async_copy(own_hbm.at[i], own.at[i], own_sem.at[i])

    def here_copy(src, i):
        return pltpu.make_async_copy(src, xr.at[i], x_r.at[i])

    late = num_c - LOW - PERM
    x_send = remote(send_hbm, xr.at[pl.ds(n2, late)], x_s, x_r.at[n2], xn_dev)

    barrier = pltpu.get_barrier_semaphore()
    for dev in (sib_dev, xn_dev, yn_dev):
        pl.semaphore_signal(barrier, inc=1, device_id=dev, device_id_type=MESH)
    o_in = pltpu.make_async_copy(o_hbm.at[yi], act.at[yi, xi, :, 0:o_cols], in_sem)
    o_in.start()

    @pl.loop(0, n1)
    def _(i):
        here_copy(got_hbm.at[i], i).start()

    @pl.loop(n1, n2)
    def _(i):
        here_copy(perm_hbm.at[i - n1], i).start()

    pl.semaphore_wait(barrier, 3)

    def o_copy(half, row):
        return remote(o_hbm.at[half], act.at[row, xi, :, 0:o_cols], o_s, o_r, yn_dev)

    def block_of(e, owner):
        if e == 0:
            return act.at[:, owner, :, pl.ds(0, o_cols + FULL * C)]
        half, n = divmod(e - 1, pieces)
        return act.at[half, owner, :, pl.ds(o_cols + starts[n] * C, PIECES[n] * C)]

    def to_sib(e, owner):
        block = block_of(e, owner)
        return remote(block, block, sib_s.at[e], sib_r.at[e], sib_dev)

    def to_xn(e, owner):
        block = block_of(e, owner)
        return remote(block, block, xn_s.at[e], xn_r.at[e], xn_dev)

    def forward(e, owner):
        block = block_of(e, owner)
        return remote(block, block, fwd_s.at[e], fwd_r.at[e], sib_dev)

    def send_own(e):
        to_xn(e, xi).start()
        to_sib(e, xi).start()

    def pass_on(e):
        to_xn(e, xn).wait_recv()
        forward(e, xn).start()

    def arrived(e):
        to_sib(e, sib).wait_recv()
        forward(e, (sib + 2) % 4).wait_recv()

    def activate(i):
        own_copy(i).wait()
        value = activation(own[i] + xr[i])
        start = o_cols + i * C if isinstance(i, int) else pl.multiple_of(o_cols + i * C, C)
        act[:, xi, :, pl.ds(start, C)] = value.reshape(2, value.shape[0] // 2, C)

    def w_wait(k):
        pltpu.make_async_copy(wmo_hbm.at[pl.ds(0, C), :], w.at[k], w_sem.at[k]).wait()

    def multiply(first, count):
        @pl.loop(first, first + count)
        def _(k):
            w_wait(k)
            lhs = act[:, :, :, pl.ds(pl.multiple_of(k * C, C), C)].reshape(2 * half_rows, C)
            for b in range(2):
                prod = jnp.dot(lhs, w[k, :, b * width:(b + 1) * width], preferred_element_type=F32)
                z[b] = z[b] + prod.reshape(z.shape[1:])

    def multiply_one(half, n, b):
        @pl.loop(num_o + starts[n], num_o + starts[n + 1])
        def _(k):
            lhs = act[half, :, :, pl.ds(pl.multiple_of(k * C, C), C)].reshape(half_rows, C)
            cols = pl.ds(pl.multiple_of(b * width, width), width)
            prod = jnp.dot(lhs, w[k, :, cols], preferred_element_type=F32)
            z[b, half] = z[b, half] + prod.reshape(z.shape[2:])

    def multiply_half(half, n):
        @pl.loop(num_o + starts[n], num_o + starts[n + 1])
        def _(k):
            if half == 0:
                w_wait(k)
            lhs = act[half, :, :, pl.ds(pl.multiple_of(k * C, C), C)].reshape(half_rows, C)
            for b in range(2):
                prod = jnp.dot(lhs, w[k, :, b * width:(b + 1) * width], preferred_element_type=F32)
                z[b, half] = z[b, half] + prod.reshape(z.shape[2:])

    x_send.start()
    o_copy(yn, yi).start()

    @pl.loop(0, num_c)
    def _(i):
        own_copy(i).start()

    for k in range(num_o):
        w_copy(k).start()
    z[...] = jnp.zeros_like(z)

    def start_here(i):
        here_copy(got_hbm.at[0], i).wait()
        activate(i)

    pl.loop(0, FULL)(start_here)
    o_in.wait()
    o_copy(yi, yn).wait_recv()
    send_own(0)
    for k in range(num_o, num_k):
        w_copy(k).start()
    pl.loop(FULL, n2)(start_here)
    ready = sum(end <= LOW + PERM for end in starts[1:])
    for n in range(ready):
        send_own(1 + n)

    x_send.wait_recv()
    pl.loop(n2, num_c)(activate)
    groups = 1 + 2 * pieces
    for e in range(1 + ready, groups):
        send_own(e)
    pass_on(0)
    arrived(0)
    multiply(0, num_o + FULL)
    z_copies = [remote(z.at[yn, half], zr.at[half], z_s.at[half], z_r.at[half], yn_dev) for half in range(2)]
    pass_on(1)
    for e in range(1, groups):
        if e + 1 < groups:
            pass_on(e + 1)
        arrived(e)
        half, n = divmod(e - 1, pieces)
        if e + 1 < groups:
            multiply_half(half, n)
        else:
            multiply_one(half, n, yn)
        if n == pieces - 1:
            z_copies[half].start()
    multiply_one(1, pieces - 1, yi)

    o_copy(yn, yi).wait_send()
    for e in range(groups):
        to_xn(e, xi).wait_send()
        to_sib(e, xi).wait_send()
        forward(e, xn).wait_send()

    x_send.wait_send()

    outs = [pltpu.make_async_copy(zr.at[half], z_out.at[:, half], out_sem.at[half]) for half in range(2)]
    for half in range(2):
        z_copies[half].wait()
        zr[half] = z[yi, half] + zr[half]
        outs[half].start()
    for half in range(2):
        outs[half].wait()


def back(x_loc, o_halves, own, got, perm, send, wao, wmo):
    rows, width = x_loc.shape
    num_o, num_c = wao.shape[0] // C, wmo.shape[0] // C
    num_k = num_o + num_c
    groups = 1 + 2 * len(PIECES)
    quarter = rows // 4
    dma = pltpu.SemaphoreType.DMA
    any_spec = pl.BlockSpec(memory_space=pl.ANY)
    z = pl.pallas_call(
        back_kernel,
        name="back",
        out_shape=jax.ShapeDtypeStruct((4, 2, rows // 8, width), F32),
        in_specs=[any_spec] * 7,
        out_specs=any_spec,
        scratch_shapes=[
            pltpu.VMEM((num_k, C, 2 * width), BF16),
            pltpu.VMEM((num_c, quarter, 2 * C), F32),
            pltpu.VMEM((num_c, quarter, 2 * C), F32),
            pltpu.VMEM((2, 4, rows // 8, num_k * C), BF16),
            pltpu.VMEM((2, 2, 4, rows // 8, width), F32),
            pltpu.VMEM((2, 4, rows // 8, width), F32),
            dma, dma((2,)), dma((num_k,)), dma((num_c,)), dma, dma((num_c,)), dma, dma,
            dma((groups,)), dma((groups,)), dma((groups,)), dma((groups,)), dma((groups,)), dma((groups,)),
            dma((2,)), dma((2,)),
        ],
        compiler_params=pltpu.CompilerParams(collective_id=1, has_side_effects=True, vmem_limit_bytes=VMEM_LIMIT),
        cost_estimate=pl.CostEstimate(
            flops=4 * rows * num_k * C * width, bytes_accessed=4 * num_k * C * width, transcendentals=0
        ),
    )(o_halves, own, got, perm, send, wao, wmo)
    return (x_loc.astype(F32) + z.reshape(rows, width)).astype(BF16)


def solution(mesh):
    x_size, yz_size = mesh.shape["x"], mesh.shape["yz"]
    both_axes = ("x", "yz")
    row_spec = P("dp", both_axes)
    in_w_spec = P("x", "yz")
    out_w_spec = P("yz", "x")
    cache_spec = P(("dp", "x", "yz"), None, None)
    len_spec = P(("dp", "x", "yz"))
    across = [(i, (i + 2) % 4) for i in range(4)]

    def local_layer(x_loc, gain_loc, wqkv_loc, wgate_loc, wup_loc, wao_loc, wmo_loc, kc_loc, vc_loc, len_loc):
        d_model = x_loc.shape[1] * x_size * yz_size
        reqs, _, head_dim = kc_loc.shape
        half = head_dim // 2
        inv_freq = 10000.0 ** (-jnp.arange(half, dtype=F32) / half)
        angles = len_loc.astype(F32)[:, None] * inv_freq
        cos, sin = jnp.cos(angles), jnp.sin(angles)
        cos = jnp.concatenate([cos, cos], axis=1)[:, None, :]
        sin = jnp.concatenate([-sin, sin], axis=1)[:, None, :]

        qkv, got, perm, send, own = front(
            x_loc, gain_loc, wqkv_loc, wgate_loc, wup_loc, d_model
        )
        perm = lax.ppermute(perm, "x", across)
        qkv = jnp.concatenate([qkv[0], qkv[1]], axis=1).reshape(reqs, -1, head_dim)
        k_all, v_all, attn = attend(qkv, cos, sin, kc_loc, vc_loc, len_loc)
        o_halves = jnp.swapaxes(attn.reshape(reqs, 2, -1), 0, 1)
        y_loc = back(x_loc, o_halves, own, got, perm, send, wao_loc, wmo_loc)
        return y_loc, k_all, v_all

    in_specs = (row_spec, P(both_axes), in_w_spec, in_w_spec, in_w_spec, out_w_spec, out_w_spec, cache_spec, cache_spec, len_spec)
    out_specs = (row_spec, cache_spec, cache_spec)
    return jax.shard_map(local_layer, mesh=mesh, in_specs=in_specs, out_specs=out_specs, check_vma=False)
```

```python
import functools

import jax
import jax.numpy as jnp
from jax import lax
from jax.experimental import pallas as pl
from jax.experimental.pallas import tpu as pltpu
from jax.sharding import PartitionSpec as P

MESH = pl.DeviceIdType.MESH
F32 = jnp.float32
BF16 = jnp.bfloat16
VMEM_LIMIT = 66_900_000

C = 768
CQ = 640
PER_STEP = 2
SLOTS = 3
N1 = 5
N2 = 13
PIECES = (8, 3)


def remote(src, dst, send_sem, recv_sem, device):
    return pltpu.make_async_remote_copy(
        src_ref=src, dst_ref=dst, send_sem=send_sem, recv_sem=recv_sem, device_id=device, device_id_type=MESH
    )


def places():
    xi = lax.axis_index("x")
    yi = lax.axis_index("yz")
    sib = xi + 1 - 2 * (xi % 2)
    xn = (xi + 2) % 4
    return xi, yi, sib, xn, (sib + 2) % 4, 1 - yi


def activation(total):
    gate = total[:, :C].astype(BF16).astype(F32)
    up = total[:, C:].astype(BF16).astype(F32)
    return (jax.nn.silu(gate) * up).astype(BF16)


def front_kernel(
    d_model, x_hbm, g_hbm, wq_hbm, wg_hbm, wu_hbm,
    qkv_hbm, a_hbm, perm_hbm, send_hbm, own_hbm,
    stat, xbuf, gain, gbuf, moments, h, wq, wg, wu, pq, rq, xq, qs, qd, p, r, xr, a,
    in_sem, wq_sem, wg_sem, wu_sem, st_s, st_r, xg_s, xg_r,
    dq_s, dq_r, xq_s, xq_r, yq_s, yq_r, d_s, d_r, x_s, x_r, out_sem, own_sem, q_sem, a_sem,
):
    xi, yi, sib, xn, sibn, yn = places()
    me = yi * 4 + xi
    sides, side_rows, width = x_hbm.shape
    rows = sides * side_rows
    near = xi // 2
    far = 1 - near
    num_q = wq_hbm.shape[1] // CQ
    num_c = wg_hbm.shape[1] // C
    sib_dev, xn_dev, yn_dev = {"x": sib}, {"x": xn}, {"yz": yn}

    def wq_copy(c):
        return pltpu.make_async_copy(wq_hbm.at[:, pl.ds(c * CQ, CQ)], wq.at[c], wq_sem.at[c])

    def w_copies(i, slot):
        start = pl.multiple_of(i * C, C)
        return (
            pltpu.make_async_copy(wg_hbm.at[:, pl.ds(start, C)], wg.at[slot], wg_sem.at[slot]),
            pltpu.make_async_copy(wu_hbm.at[:, pl.ds(start, C)], wu.at[slot], wu_sem.at[slot]),
        )

    x_in = pltpu.make_async_copy(x_hbm, xbuf.at[yi], in_sem.at[0])
    g_in = pltpu.make_async_copy(g_hbm, gain, in_sem.at[1])
    x_in.start()
    g_in.start()
    barrier = pltpu.get_barrier_semaphore()
    offsets = [(dy, dx) for dy in range(2) for dx in range(4)][1:]
    for dy, dx in offsets:
        pl.semaphore_signal(barrier, inc=1, device_id={"yz": (yi + dy) % 2, "x": (xi + dx) % 4}, device_id_type=MESH)

    x_in.wait()
    x_f32 = xbuf[yi].reshape(rows, width).astype(F32)
    lane = lax.broadcasted_iota(jnp.int32, (rows, rows), 1)
    sums = jnp.where(
        lane == 0,
        jnp.sum(x_f32, axis=1, keepdims=True),
        jnp.where(lane == 1, jnp.sum(x_f32 * x_f32, axis=1, keepdims=True), 0.0),
    )
    stat[me] = sums.T[0:8, :]
    g_in.wait()
    gbuf[yi] = jnp.broadcast_to(gain[...].astype(F32)[None, :], (8, width))
    pl.semaphore_wait(barrier, 7)

    def stat_copy(k, slot):
        dy, dx = offsets[k]
        dev = {"yz": (yi + dy) % 2, "x": (xi + dx) % 4}
        return remote(stat.at[slot], stat.at[slot], st_s.at[k], st_r.at[k], dev)

    def x_copies(slot):
        return [
            remote(xbuf.at[slot, side], xbuf.at[slot, side], xg_s.at[1 + n], xg_r.at[1 + n], yn_dev)
            for n, side in enumerate((far, near))
        ]

    def g_copy(slot):
        return remote(gbuf.at[slot], gbuf.at[slot], xg_s.at[0], xg_r.at[0], yn_dev)

    for k in range(7):
        stat_copy(k, me).start()
    g_copy(yi).start()
    for copy in x_copies(yi):
        copy.start()
    for c in range(num_q):
        wq_copy(c).start()
    for i in range(SLOTS):
        for copy in w_copies(i, i):
            copy.start()
    for k, (dy, dx) in enumerate(offsets):
        stat_copy(k, ((yi + 2 - dy) % 2) * 4 + (xi + 4 - dx) % 4).wait_recv()
    total = stat[0]
    for k in range(1, 8):
        total = total + stat[k]
    cols = jnp.concatenate([total, jnp.zeros((rows - 8, rows), F32)], axis=0).T
    mean = cols[:, 0:1] / d_model
    var = cols[:, 1:2] / d_model - mean * mean
    moments[0] = jnp.broadcast_to(mean, (rows, 128)).reshape(sides, side_rows, 128)
    moments[1] = jnp.broadcast_to(lax.rsqrt(var + 1e-6), (rows, 128)).reshape(sides, side_rows, 128)
    g_copy(yn).wait_recv()

    def normalize(side):
        for b in range(2):
            part = (xbuf[b, side].astype(F32) - moments[0, side][:, 0:1]) * moments[1, side][:, 0:1]
            h[side, :, b * width:(b + 1) * width] = (part * gbuf[b][0:1, :]).astype(BF16)

    def dq(c, k):
        src = sib if k == 0 else sibn
        return remote(pq.at[c, src], rq.at[c, k], dq_s.at[c, k], dq_r.at[c, k], sib_dev)

    def xq_copy(c):
        return remote(pq.at[c, xn], xq.at[c], xq_s.at[c], xq_r.at[c], xn_dev)

    def q_product(c, side):
        prod = jnp.dot(h[side], wq[c], preferred_element_type=F32)
        pq[c, pl.ds(2 * side, 2)] = prod.reshape(2, rows // 4, CQ)

    def q_send(c):
        dq(c, 1).wait_recv()
        dq(c, 1).wait_send()
        pq[c, xn] = pq[c, xn] + rq[c, 1]
        xq_copy(c).start()

    x_copies(yn)[0].wait_recv()
    normalize(far)

    @pl.loop(0, num_q)
    def _(c):
        wq_copy(c).wait()
        q_product(c, far)
        dq(c, 1).start()

        @pl.when(c >= 1)
        def _():
            q_send(c - 1)

    x_copies(yn)[1].wait_recv()
    normalize(near)
    q_send(num_q - 1)

    @pl.loop(0, num_q)
    def _(c):
        q_product(c, near)
        dq(c, 0).start()

    def d_copy(i, k):
        src = sib if k == 0 else sibn
        return remote(p.at[i, src], r.at[i, k], d_s.at[i, k], d_r.at[i, k], sib_dev)

    def x_send(i):
        return remote(p.at[i, xn], xr.at[i], x_s.at[i], x_r.at[i], xn_dev)

    def perm_copy(i):
        return pltpu.make_async_copy(p.at[i, xn], perm_hbm.at[i - N1], out_sem.at[i])

    def send_copy(i):
        return pltpu.make_async_copy(p.at[i, xn], send_hbm.at[i - N2], out_sem.at[i])

    def own_copy(i):
        return pltpu.make_async_copy(p.at[i, xi], own_hbm.at[i - N1], own_sem.at[i])

    def chip_sum(i):
        d_copy(i, 1).wait_recv()
        d_copy(i, 1).wait_send()
        p[i, xn] = p[i, xn] + r[i, 1]

        @pl.when(i < N1)
        def _():
            x_send(i).start()

        @pl.when((i >= N1) & (i < N2))
        def _():
            perm_copy(i).start()

        @pl.when(i >= N2)
        def _():
            send_copy(i).start()

        d_copy(i, 0).wait_recv()
        d_copy(i, 0).wait_send()
        p[i, xi] = p[i, xi] + r[i, 0]

        @pl.when(i >= N1)
        def _():
            own_copy(i).start()

    def product(i):
        slot = i % SLOTS
        g_w, u_w = w_copies(i, slot)
        h_all = h[...].reshape(rows, h.shape[2])
        g_w.wait()
        p[i, :, :, :C] = jnp.dot(h_all, wg[slot], preferred_element_type=F32).reshape(4, rows // 4, C)
        u_w.wait()
        p[i, :, :, C:] = jnp.dot(h_all, wu[slot], preferred_element_type=F32).reshape(4, rows // 4, C)
        d_copy(i, 1).start()
        d_copy(i, 0).start()

        @pl.when(i + SLOTS < num_c)
        def _():
            for copy in w_copies(i + SLOTS, slot):
                copy.start()

    product(0)

    def step(i):
        product(i)
        chip_sum(i - 1)

    half = num_c // 2 + 1
    pl.loop(1, half)(step)

    @pl.loop(0, num_q)
    def _(c):
        dq(c, 0).wait_recv()
        dq(c, 0).wait_send()
        mine = pq[c, xi] + rq[c, 0]
        xq_copy(c).wait_recv()
        xq_copy(c).wait_send()
        value = (mine + xq[c]).astype(BF16)
        qs[:, :, pl.ds(pl.multiple_of(c * CQ, CQ), CQ)] = value.reshape(2, rows // 8, CQ)

    def yq_copy(k):
        return remote(qs.at[1 - k], qd.at[k], yq_s, yq_r, yn_dev)

    yq_copy(yi).start()
    qd[yi] = qs[yi]

    pl.loop(half, num_c)(step)
    chip_sum(num_c - 1)
    yq_copy(yn).wait_recv()
    q_out = pltpu.make_async_copy(qd, qkv_hbm, q_sem)
    q_out.start()

    @pl.loop(0, N1)
    def _(i):
        x_send(i).wait_recv()
        x_send(i).wait_send()
        act = activation(p[i, xi] + xr[i])
        a[:, :, pl.ds(pl.multiple_of(i * C, C), C)] = act.reshape(2, rows // 8, C)

    a_out = pltpu.make_async_copy(a, a_hbm, a_sem)
    a_out.start()
    for k in range(7):
        stat_copy(k, me).wait_send()
    g_copy(yi).wait_send()
    for copy in x_copies(yi):
        copy.wait_send()
    yq_copy(yi).wait_send()

    @pl.loop(N1, N2)
    def _(i):
        perm_copy(i).wait()
        own_copy(i).wait()

    @pl.loop(N2, num_c)
    def _(i):
        send_copy(i).wait()
        own_copy(i).wait()

    q_out.wait()
    a_out.wait()


def front(x_loc, gain_loc, wqkv, wgate, wup, d_model):
    rows, width = x_loc.shape
    depth, q_cols = wqkv.shape
    num_q, num_c = q_cols // CQ, wgate.shape[1] // C
    quarter = rows // 4
    dma = pltpu.SemaphoreType.DMA
    any_spec = pl.BlockSpec(memory_space=pl.ANY)
    return pl.pallas_call(
        functools.partial(front_kernel, d_model),
        name="front",
        out_shape=(
            jax.ShapeDtypeStruct((2, rows // 8, q_cols), BF16),
            jax.ShapeDtypeStruct((2, rows // 8, N1 * C), BF16),
            jax.ShapeDtypeStruct((N2 - N1, quarter, 2 * C), F32),
            jax.ShapeDtypeStruct((num_c - N2, quarter, 2 * C), F32),
            jax.ShapeDtypeStruct((num_c - N1, quarter, 2 * C), F32),
        ),
        in_specs=[any_spec] * 5,
        out_specs=(any_spec,) * 5,
        scratch_shapes=[
            pltpu.VMEM((8, 8, rows), F32),
            pltpu.VMEM((2, 2, rows // 2, width), BF16),
            pltpu.VMEM((width,), BF16),
            pltpu.VMEM((2, 8, width), F32),
            pltpu.VMEM((2, 2, rows // 2, 128), F32),
            pltpu.VMEM((2, rows // 2, depth), BF16),
            pltpu.VMEM((num_q, depth, CQ), BF16),
            pltpu.VMEM((SLOTS, depth, C), BF16),
            pltpu.VMEM((SLOTS, depth, C), BF16),
            pltpu.VMEM((num_q, 4, quarter, CQ), F32),
            pltpu.VMEM((num_q, 2, quarter, CQ), F32),
            pltpu.VMEM((num_q, quarter, CQ), F32),
            pltpu.VMEM((2, rows // 8, q_cols), BF16),
            pltpu.VMEM((2, rows // 8, q_cols), BF16),
            pltpu.VMEM((num_c, 4, quarter, 2 * C), F32),
            pltpu.VMEM((num_c, 2, quarter, 2 * C), F32),
            pltpu.VMEM((N1, quarter, 2 * C), F32),
            pltpu.VMEM((2, rows // 8, N1 * C), BF16),
            dma((2,)), dma((num_q,)), dma((SLOTS,)), dma((SLOTS,)), dma((7,)), dma((7,)), dma((3,)), dma((3,)),
            dma((num_q, 2)), dma((num_q, 2)), dma((num_q,)), dma((num_q,)), dma, dma,
            dma((num_c, 2)), dma((num_c, 2)), dma((N1,)), dma((N1,)), dma((num_c,)), dma((num_c,)), dma, dma,
        ],
        compiler_params=pltpu.CompilerParams(collective_id=0, has_side_effects=True, vmem_limit_bytes=VMEM_LIMIT),
        cost_estimate=pl.CostEstimate(
            flops=2 * rows * depth * (q_cols + 2 * wgate.shape[1]),
            bytes_accessed=2 * depth * (q_cols + 2 * wgate.shape[1]),
            transcendentals=0,
        ),
    )(x_loc.reshape(2, rows // 2, width), gain_loc, wqkv, wgate, wup)


def attend_kernel(len_ref, qkv_ref, cos_ref, sin_ref, k_ref, v_ref, ko_ref, vo_ref, o_ref):
    ko_ref[...] = k_ref[...]
    vo_ref[...] = v_ref[...]
    for n in range(PER_STEP):
        pos = len_ref[pl.program_id(0) * PER_STEP + n]
        qkv = qkv_ref[n]
        heads, head_dim = qkv.shape[0] - 2, qkv.shape[1]
        wide = qkv.astype(F32)
        turned = (wide * cos_ref[n] + pltpu.roll(wide, head_dim // 2, 1) * sin_ref[n]).astype(BF16)
        query = turned[:heads]
        base = pl.multiple_of((pos // 16) * 16, 16)
        here = lax.broadcasted_iota(jnp.int32, (16, head_dim), 0) == pos - base
        for out, new in ((ko_ref, turned[heads:heads + 1]), (vo_ref, qkv[heads + 1:heads + 2])):
            tile = out[n, pl.ds(base, 16), :].astype(F32)
            out[n, pl.ds(base, 16), :] = jnp.where(here, new.astype(F32), tile).astype(BF16)
        scores = lax.dot_general(query, ko_ref[n], (((1,), (1,)), ((), ())), preferred_element_type=F32)
        scores = scores * head_dim ** -0.5
        at = lax.broadcasted_iota(jnp.int32, scores.shape, 1)
        scores = jnp.where(at <= pos, scores, -1e30)
        weight = jnp.exp(scores - jnp.max(scores, axis=1, keepdims=True))
        probs = (weight / jnp.sum(weight, axis=1, keepdims=True)).astype(BF16)
        o_ref[n] = jnp.dot(probs, vo_ref[n], preferred_element_type=F32).astype(BF16)


def attend(qkv, cos, sin, k_cache, v_cache, ctx_len):
    reqs, length, head_dim = k_cache.shape
    heads = qkv.shape[1] - 2
    cache_spec = pl.BlockSpec((PER_STEP, length, head_dim), lambda i, lens: (i, 0, 0))
    table_spec = pl.BlockSpec((PER_STEP, 1, head_dim), lambda i, lens: (i, 0, 0))
    return pl.pallas_call(
        attend_kernel,
        name="attend",
        grid_spec=pltpu.PrefetchScalarGridSpec(
            num_scalar_prefetch=1,
            grid=(reqs // PER_STEP,),
            in_specs=[
                pl.BlockSpec((PER_STEP, heads + 2, head_dim), lambda i, lens: (i, 0, 0)),
                table_spec, table_spec, cache_spec, cache_spec,
            ],
            out_specs=[cache_spec, cache_spec, pl.BlockSpec((PER_STEP, heads, head_dim), lambda i, lens: (i, 0, 0))],
        ),
        out_shape=(
            jax.ShapeDtypeStruct(k_cache.shape, BF16),
            jax.ShapeDtypeStruct(v_cache.shape, BF16),
            jax.ShapeDtypeStruct((reqs, heads, head_dim), BF16),
        ),
        compiler_params=pltpu.CompilerParams(dimension_semantics=("arbitrary",)),
        cost_estimate=pl.CostEstimate(
            flops=64 * reqs * heads * length * head_dim,
            bytes_accessed=8 * reqs * length * head_dim,
            transcendentals=reqs * heads * length,
        ),
    )(ctx_len, qkv, cos, sin, k_cache, v_cache)


def back_kernel(
    o_hbm, a1_hbm, own_hbm, perm_hbm, send_hbm, wao_hbm, wmo_hbm, z_hbm,
    w, own, xr, act, z, zr,
    in_sem, out_sem, w_sem, own_sem, x_s, x_r, o_s, o_r, sib_s, sib_r, xn_s, xn_r, fwd_s, fwd_r, z_s, z_r,
):
    xi, yi, sib, xn, _, yn = places()
    sib_dev, xn_dev, yn_dev = {"x": sib}, {"x": xn}, {"yz": yn}
    width = z_hbm.shape[3]
    half_rows = act.shape[1] * act.shape[2]
    num_o, num_c = wao_hbm.shape[0] // C, wmo_hbm.shape[0] // C
    num_k = num_o + num_c
    o_cols = wao_hbm.shape[0]
    late = num_c - N1
    here = N2 - N1
    pieces = len(PIECES)
    starts = [sum(PIECES[:n]) for n in range(pieces + 1)]

    def w_copy(k):
        src = wao_hbm.at[pl.ds(k * C, C), :] if k < num_o else wmo_hbm.at[pl.ds((k - num_o) * C, C), :]
        return pltpu.make_async_copy(src, w.at[k], w_sem.at[k])

    def own_copy(i):
        return pltpu.make_async_copy(own_hbm.at[i], own.at[i], own_sem.at[i])

    def perm_copy(i):
        return pltpu.make_async_copy(perm_hbm.at[i], xr.at[i], x_r.at[i])

    def x_send(i):
        return remote(send_hbm.at[i - here], xr.at[i], x_s.at[i - here], x_r.at[i], xn_dev)

    barrier = pltpu.get_barrier_semaphore()
    for dev in (sib_dev, xn_dev, yn_dev):
        pl.semaphore_signal(barrier, inc=1, device_id=dev, device_id_type=MESH)
    o_in = pltpu.make_async_copy(o_hbm.at[yi], act.at[yi, xi, :, 0:o_cols], in_sem.at[0])
    a1_in = pltpu.make_async_copy(a1_hbm, act.at[:, xi, :, pl.ds(o_cols, N1 * C)], in_sem.at[1])
    o_in.start()
    a1_in.start()
    for i in range(late):
        own_copy(i).start()
    for i in range(here):
        perm_copy(i).start()
    pl.semaphore_wait(barrier, 3)

    def o_copy(half, row):
        return remote(o_hbm.at[half], act.at[row, xi, :, 0:o_cols], o_s, o_r, yn_dev)

    def block_of(e, owner):
        if e == 0:
            return act.at[:, owner, :, pl.ds(o_cols, N1 * C)]
        if e == 1:
            return act.at[:, owner, :, pl.ds(0, o_cols)]
        half, n = divmod(e - 2, pieces)
        return act.at[half, owner, :, pl.ds(o_cols + (N1 + starts[n]) * C, PIECES[n] * C)]

    def to_sib(e, owner):
        block = block_of(e, owner)
        return remote(block, block, sib_s.at[e], sib_r.at[e], sib_dev)

    def to_xn(e, owner):
        block = block_of(e, owner)
        return remote(block, block, xn_s.at[e], xn_r.at[e], xn_dev)

    def forward(e, owner):
        block = block_of(e, owner)
        return remote(block, block, fwd_s.at[e], fwd_r.at[e], sib_dev)

    def send_own(e):
        to_xn(e, xi).start()
        to_sib(e, xi).start()

    def pass_on(e):
        to_xn(e, xn).wait_recv()
        forward(e, xn).start()

    def arrived(e):
        to_sib(e, sib).wait_recv()
        forward(e, (sib + 2) % 4).wait_recv()

    def activate(i):
        own_copy(i).wait()
        value = activation(own[i] + xr[i])
        start = pl.multiple_of(o_cols + (N1 + i) * C, C)
        act[:, xi, :, pl.ds(start, C)] = value.reshape(2, value.shape[0] // 2, C)

    def w_wait(k):
        pltpu.make_async_copy(wmo_hbm.at[pl.ds(0, C), :], w.at[k], w_sem.at[k]).wait()

    def multiply(first, count):
        @pl.loop(first, first + count)
        def _(k):
            w_wait(k)
            lhs = act[:, :, :, pl.ds(pl.multiple_of(k * C, C), C)].reshape(2 * half_rows, C)
            for b in range(2):
                prod = jnp.dot(lhs, w[k, :, b * width:(b + 1) * width], preferred_element_type=F32)
                z[b] = z[b] + prod.reshape(z.shape[1:])

    def multiply_half(half, n):
        @pl.loop(num_o + N1 + starts[n], num_o + N1 + starts[n + 1])
        def _(k):
            if half == 0:
                w_wait(k)
            lhs = act[half, :, :, pl.ds(pl.multiple_of(k * C, C), C)].reshape(half_rows, C)
            for b in range(2):
                prod = jnp.dot(lhs, w[k, :, b * width:(b + 1) * width], preferred_element_type=F32)
                z[b, half] = z[b, half] + prod.reshape(z.shape[2:])

    first = (late - here + 1) // 2
    for i in range(here, here + first):
        x_send(i).start()
    o_copy(yn, yi).start()
    for k in range(num_k):
        w_copy(k).start()
    z[...] = jnp.zeros_like(z)

    @pl.loop(0, here)
    def _(i):
        perm_copy(i).wait()
        activate(i)

    a1_in.wait()
    o_in.wait()
    o_copy(yi, yn).wait_recv()
    send_own(1)
    send_own(0)
    for i in range(here + first, late):
        x_send(i).start()
    ready = sum(end <= here for end in starts[1:])
    for n in range(ready):
        send_own(2 + n)

    @pl.loop(here, here + first)
    def _(i):
        x_send(i).wait_recv()
        activate(i)

    pass_on(1)
    pass_on(0)
    arrived(1)
    multiply(0, num_o)
    arrived(0)
    multiply(num_o, N1)

    @pl.loop(here + first, late)
    def _(i):
        x_send(i).wait_recv()
        activate(i)

    groups = 2 + 2 * pieces
    for e in range(2 + ready, groups):
        send_own(e)
    z_copies = [remote(z.at[yn, half], zr.at[half], z_s.at[half], z_r.at[half], yn_dev) for half in range(2)]
    pass_on(2)
    for e in range(2, groups):
        if e + 1 < groups:
            pass_on(e + 1)
        arrived(e)
        half, n = divmod(e - 2, pieces)
        multiply_half(half, n)
        if n == pieces - 1:
            z_copies[half].start()

    o_copy(yn, yi).wait_send()
    for e in range(groups):
        to_xn(e, xi).wait_send()
        to_sib(e, xi).wait_send()
        forward(e, xn).wait_send()

    @pl.loop(here, late)
    def _(i):
        x_send(i).wait_send()

    outs = [pltpu.make_async_copy(zr.at[half], z_hbm.at[:, half], out_sem.at[half]) for half in range(2)]
    for half in range(2):
        z_copies[half].wait()
        zr[half] = z[yi, half] + zr[half]
        outs[half].start()
    for half in range(2):
        outs[half].wait()


def back(x_loc, o_halves, a1, own, perm, send, wao, wmo):
    rows, width = x_loc.shape
    num_o, num_c = wao.shape[0] // C, wmo.shape[0] // C
    num_k, late = num_o + num_c, num_c - N1
    groups = 2 + 2 * len(PIECES)
    quarter = rows // 4
    dma = pltpu.SemaphoreType.DMA
    any_spec = pl.BlockSpec(memory_space=pl.ANY)
    z = pl.pallas_call(
        back_kernel,
        name="back",
        out_shape=jax.ShapeDtypeStruct((4, 2, rows // 8, width), F32),
        in_specs=[any_spec] * 7,
        out_specs=any_spec,
        scratch_shapes=[
            pltpu.VMEM((num_k, C, 2 * width), BF16),
            pltpu.VMEM((late, quarter, 2 * C), F32),
            pltpu.VMEM((late, quarter, 2 * C), F32),
            pltpu.VMEM((2, 4, rows // 8, num_k * C), BF16),
            pltpu.VMEM((2, 2, 4, rows // 8, width), F32),
            pltpu.VMEM((2, 4, rows // 8, width), F32),
            dma((2,)), dma((2,)), dma((num_k,)), dma((late,)), dma((num_c - N2,)), dma((late,)), dma, dma,
            dma((groups,)), dma((groups,)), dma((groups,)), dma((groups,)), dma((groups,)), dma((groups,)),
            dma((2,)), dma((2,)),
        ],
        compiler_params=pltpu.CompilerParams(collective_id=1, has_side_effects=True, vmem_limit_bytes=VMEM_LIMIT),
        cost_estimate=pl.CostEstimate(
            flops=4 * rows * num_k * C * width, bytes_accessed=4 * num_k * C * width, transcendentals=0
        ),
    )(o_halves, a1, own, perm, send, wao, wmo)
    return (x_loc.astype(F32) + z.reshape(rows, width)).astype(BF16)


def solution(mesh):
    x_size, yz_size = mesh.shape["x"], mesh.shape["yz"]
    both_axes = ("x", "yz")
    row_spec = P("dp", both_axes)
    in_w_spec = P("x", "yz")
    out_w_spec = P("yz", "x")
    cache_spec = P(("dp", "x", "yz"), None, None)
    len_spec = P(("dp", "x", "yz"))
    across = [(i, (i + 2) % 4) for i in range(4)]

    def local_layer(x_loc, gain_loc, wqkv_loc, wgate_loc, wup_loc, wao_loc, wmo_loc, kc_loc, vc_loc, len_loc):
        d_model = x_loc.shape[1] * x_size * yz_size
        reqs, _, head_dim = kc_loc.shape
        half = head_dim // 2
        inv_freq = 10000.0 ** (-jnp.arange(half, dtype=F32) / half)
        angles = len_loc.astype(F32)[:, None] * inv_freq
        cos, sin = jnp.cos(angles), jnp.sin(angles)
        cos = jnp.concatenate([cos, cos], axis=1)[:, None, :]
        sin = jnp.concatenate([-sin, sin], axis=1)[:, None, :]

        qkv, a1, perm, send, own = front(
            x_loc, gain_loc, wqkv_loc, wgate_loc, wup_loc, d_model
        )
        perm = lax.ppermute(perm, "x", across)
        qkv = jnp.concatenate([qkv[0], qkv[1]], axis=1).reshape(reqs, -1, head_dim)
        k_all, v_all, attn = attend(qkv, cos, sin, kc_loc, vc_loc, len_loc)
        o_halves = jnp.swapaxes(attn.reshape(reqs, 2, -1), 0, 1)
        y_loc = back(x_loc, o_halves, a1, own, perm, send, wao_loc, wmo_loc)
        return y_loc, k_all, v_all

    in_specs = (row_spec, P(both_axes), in_w_spec, in_w_spec, in_w_spec, out_w_spec, out_w_spec, cache_spec, cache_spec, len_spec)
    out_specs = (row_spec, cache_spec, cache_spec)
    return jax.shard_map(local_layer, mesh=mesh, in_specs=in_specs, out_specs=out_specs, check_vma=False)
```
